32 devices in a mesh: dp: 8 (over y, x, core), mp: 4 (over z).
Axes of the slice: x: 2, y: 2, z: 4, core: 2. Of those that a mesh axis runs over, the one named last changes fastest.
Arguments:
- hidden_in: bfloat16 [4096, 2048], P('dp'), may hold values from -6 to 6
- cotangent: bfloat16 [4096, 2048], P('dp'), may hold values from -6 to 6
- segments: int32 [8, 512], P('dp'), may hold values from 0 to 5, never falling along the last dimension, each value on 1 to 256 neighbouring positions
- live_counts: int32 [8], P('dp'), may hold values from 128 to 512, as said below
- w_query: bfloat16 [2048, 2048], P('dp', 'mp'), may hold values from -0.125 to 0.125
- w_key: bfloat16 [2048, 2048], P('dp', 'mp'), may hold values from -0.125 to 0.125
- w_value: bfloat16 [2048, 2048], P('dp', 'mp'), may hold values from -0.125 to 0.125
- w_output: bfloat16 [2048, 2048], P('mp', 'dp'), may hold values from -0.125 to 0.125
- w_gate: bfloat16 [2048, 8192], P('dp', 'mp'), may hold values from -0.125 to 0.125
- w_up: bfloat16 [2048, 8192], P('dp', 'mp'), may hold values from -0.125 to 0.125
- w_down: bfloat16 [8192, 2048], P('mp', 'dp'), may hold values from -0.0625 to 0.0625
- query_gain: float32 [2048], P('mp'), may hold values from 0.5 to 1.5
- key_gain: float32 [2048], P('mp'), may hold values from 0.5 to 1.5
- attn_gain: float32 [2048], replicated, may hold values from 0.5 to 1.5
- ffn_gain: float32 [2048], replicated, may hold values from 0.5 to 1.5
Outputs:
- hidden_out: bfloat16 [4096, 2048], P('dp')
- grad_in: float32 [4096, 2048], P('dp')
- grad_query: float32 [2048, 2048], P('dp', 'mp')
- grad_key: float32 [2048, 2048], P('dp', 'mp')
- grad_value: float32 [2048, 2048], P('dp', 'mp')
- grad_output_w: float32 [2048, 2048], P('mp', 'dp')
- grad_gate: float32 [2048, 8192], P('dp', 'mp')
- grad_up: float32 [2048, 8192], P('dp', 'mp')
- grad_down: float32 [8192, 2048], P('mp', 'dp')
- grad_query_gain: float32 [2048], P('mp')
- grad_key_gain: float32 [2048], P('mp')
- grad_attn_gain: float32 [2048], replicated
- grad_ffn_gain: float32 [2048], replicated
The draws below stay inside these ranges and needn't reach their ends.
Inputs may be any that keep to these rules, and one draw needn't show every extreme that they name: Within the rows of one index of dp, segments never fall; each of the 6 documents has 1 to 256 rows and one has exactly 256. `live_counts`: rows of a block at or after its live count are padding; some index of dp has 512 live rows and some has 128.
All inputs are finite; a program needn't handle non-finite values.
Results may differ from the reference program's by a relative error of at most 0.017.
Values may be sent and summed in bfloat16 or wider, within the bound.
A program may use at most 256 MiB of HBM per device.

```python
import math
import jax
import jax.numpy as jnp
import numpy as np
from jax import lax

D = 2048
HD = 128
FF = 8192
TOK_DEV = 512
DOCS = 6
DOC_MOST = 256
LIVE_LEAST = 128
TOKENS = 4096
N_DP = 8


def draw_live_counts(key, part):
    values = jax.random.randint(key, (N_DP,), LIVE_LEAST, TOK_DEV + 1, dtype=jnp.int32)
    order = jax.random.permutation(jax.random.fold_in(key, 7), N_DP)
    values = values.at[order[0]].set(TOK_DEV)
    values = values.at[order[1]].set(LIVE_LEAST)
    return values.astype(jnp.int32)


def block_levels(own_key, shape, shards, least, high):
    gain, own = 1.0, jax.random.fold_in(own_key, 6)
    for axis_at, blocks in shards:
        draws = jnp.exp(jax.random.uniform(jax.random.fold_in(own, axis_at), (blocks,), jnp.float32, least / len(shards), high / len(shards)))
        gain = gain * jnp.repeat(draws, shape[axis_at] // blocks).reshape([-1 if axis == axis_at else 1 for axis in range(len(shape))])
    return gain


def split_up(amount, total, bound, slope):
    weights = [(1 << 20) // math.isqrt(rank ** slope) + 1 for rank in range(2, amount + 1)]
    surplus, holding = total - bound - (amount - 1), [1] * (amount - 1)
    while surplus > 0:
        candidates = [i for i in range(amount - 1) if holding[i] < bound]
        whole, remaining = sum([weights[i] for i in candidates]), surplus
        for i in candidates:
            more = min(bound - holding[i], max(1, remaining * weights[i] // whole), surplus)
            holding[i] = holding[i] + more
            surplus = surplus - more
    return np.array([bound] + holding)


def uneven_parts(key, count, total, most, slope):
    if count == 2:
        one = jax.random.randint(key, (), max(1, total - most), min(most, total - 1) + 1)
        return jnp.stack([one, total - one])
    tallies = jnp.asarray(split_up(count, total, most, slope), jnp.int32)
    pairs = (count - 1) // 2
    source_of, taker = tallies[1:1 + 2 * pairs:2], tallies[2:2 + 2 * pairs:2]
    room = jnp.minimum(source_of - 1, most - taker)
    passed = jax.random.randint(jax.random.fold_in(key, 1), (pairs,), 0, 1 << 20) % (room + 1)
    tallies = tallies.at[1:1 + 2 * pairs:2].set(source_of - passed).at[2:2 + 2 * pairs:2].set(taker + passed)
    return tallies[jax.random.permutation(jax.random.fold_in(key, 2), count)]


def bell_draw(rng, dims, scale, reach, split=(), kind=jnp.bfloat16):
    factor_of = block_levels(rng, dims, split, -0.22, 0.18) if split else 1.0
    values = jax.random.normal(rng, dims, jnp.float32) * scale * factor_of
    return jnp.minimum(jnp.maximum(values, -reach), reach).astype(kind)


def setup_inputs(seed: int = 0) -> dict:
    streams_of = jax.random.split(jax.random.key(seed), 16)
    return {
        "hidden_in": bell_draw(streams_of[0], (TOKENS, D), 1.0, 6.0, ((0, 8),)),
        "cotangent": bell_draw(streams_of[1], (TOKENS, D), 1.0, 6.0, ((0, 8),)),
        "segments": jax.vmap(lambda own: jnp.searchsorted(jnp.cumsum(uneven_parts(own, DOCS, TOK_DEV, DOC_MOST, 1)), jnp.arange(TOK_DEV), side="right"))(jax.random.split(streams_of[2], N_DP)).reshape((N_DP, TOK_DEV)).astype(jnp.int32),
        "live_counts": draw_live_counts(jax.random.fold_in(streams_of[15], 71), 0),
        "w_query": bell_draw(streams_of[4], (D, D), D ** -0.5, 0.125, ((0, 8), (1, 4))),
        "w_key": bell_draw(streams_of[5], (D, D), D ** -0.5, 0.125, ((0, 8), (1, 4))),
        "w_value": bell_draw(streams_of[6], (D, D), D ** -0.5, 0.125, ((0, 8), (1, 4))),
        "w_output": bell_draw(streams_of[7], (D, D), D ** -0.5, 0.125, ((0, 4), (1, 8))),
        "w_gate": bell_draw(streams_of[8], (D, FF), D ** -0.5, 0.125, ((0, 8), (1, 4))),
        "w_up": bell_draw(streams_of[9], (D, FF), D ** -0.5, 0.125, ((0, 8), (1, 4))),
        "w_down": bell_draw(streams_of[10], (FF, D), FF ** -0.5, 0.0625, ((0, 4), (1, 8))),
        "query_gain": jnp.clip(1.0 + 0.1 * jax.random.normal(streams_of[11], (D,), jnp.float32), 0.5, 1.5),
        "key_gain": jnp.clip(1.0 + 0.1 * jax.random.normal(streams_of[12], (D,), jnp.float32), 0.5, 1.5),
        "attn_gain": jnp.clip(1.0 + 0.1 * jax.random.normal(streams_of[13], (D,), jnp.float32), 0.5, 1.5),
        "ffn_gain": jnp.clip(1.0 + 0.1 * jax.random.normal(streams_of[14], (D,), jnp.float32), 0.5, 1.5),
    }


EPS = 1e-06
THETA = 500000.0

def kept(values):
    return lax.optimization_barrier(values)

def doc_positions(seg_row):
    row_count = seg_row.shape[0]
    row_index = jnp.arange(row_count, dtype=jnp.int32)
    change = jnp.concatenate([jnp.ones((1,), dtype=bool), seg_row[1:] != seg_row[:-1]])
    doc_start = lax.cummax(jnp.where(change, row_index, jnp.zeros_like(row_index)), axis=0)
    return (row_index - doc_start).astype(jnp.float32)

def rotary_tables(positions, head_size):
    half_size = head_size // 2
    inv_freq = THETA ** (-(jnp.arange(half_size, dtype=jnp.float32) * (2.0 / head_size)))
    angles = positions[:, None] * inv_freq[None, :]
    return (jnp.cos(angles)[:, None, :], jnp.sin(angles)[:, None, :])

def rotate(values, cos_tab, sin_tab):
    half_size = values.shape[2] // 2
    first_half = values[:, :, :half_size]
    second_half = values[:, :, half_size:]
    return jnp.concatenate([first_half * cos_tab - second_half * sin_tab, second_half * cos_tab + first_half * sin_tab], axis=2)

def rotate_back(grads, cos_tab, sin_tab):
    half_size = grads.shape[2] // 2
    first_half = grads[:, :, :half_size]
    second_half = grads[:, :, half_size:]
    return jnp.concatenate([first_half * cos_tab + second_half * sin_tab, second_half * cos_tab - first_half * sin_tab], axis=2)

def block_mask(seg_row, offset, block_rows):
    row_index = jnp.arange(seg_row.shape[0])
    rows = row_index[offset:offset + block_rows]
    same = seg_row[offset:offset + block_rows, None] == seg_row[None, :]
    return same & (rows[:, None] >= row_index[None, :])

def block_scores(q_blk, k_bf, allowed, score_scale):
    scores = jnp.einsum('qhe,khe->hqk', q_blk.astype(jnp.float32), k_bf.astype(jnp.float32)) * score_scale
    return jnp.where(allowed[None], scores, jnp.float32(-1e+30))

def attend_forward(q_bf, k_bf, v_bf, seg_row, score_scale):
    row_count = q_bf.shape[0]
    block_rows = min(512, row_count)
    outputs = []
    lse_parts = []
    for offset in range(0, row_count, block_rows):
        allowed = block_mask(seg_row, offset, block_rows)
        scores = block_scores(q_bf[offset:offset + block_rows], k_bf, allowed, score_scale)
        row_max = lax.optimization_barrier(jnp.max(scores, axis=2, keepdims=True))
        lse = row_max + jnp.log(lax.optimization_barrier(jnp.sum(jnp.exp(scores - row_max), axis=2, keepdims=True)))
        probs = kept(jnp.exp(scores - lse).astype(jnp.bfloat16))
        outputs.append(jnp.einsum('hqk,khe->qhe', probs.astype(jnp.float32), v_bf.astype(jnp.float32)))
        lse_parts.append(lse)
    return (kept(jnp.concatenate(outputs, axis=0).astype(jnp.bfloat16)), lse_parts)

def attend_backward(q_bf, k_bf, v_bf, o_bf, do_bf, lse_parts, seg_row, score_scale):
    row_count = q_bf.shape[0]
    block_rows = min(512, row_count)
    dq_parts = []
    dk_acc = jnp.zeros(k_bf.shape, jnp.float32)
    dv_acc = jnp.zeros(v_bf.shape, jnp.float32)
    for part_index, offset in enumerate(range(0, row_count, block_rows)):
        allowed = block_mask(seg_row, offset, block_rows)
        q_blk = q_bf[offset:offset + block_rows]
        do_blk = do_bf[offset:offset + block_rows]
        o_blk = o_bf[offset:offset + block_rows]
        scores = block_scores(q_blk, k_bf, allowed, score_scale)
        probs = jnp.exp(scores - lse_parts[part_index])
        probs_bf = kept(probs.astype(jnp.bfloat16))
        dprob = jnp.einsum('qhe,khe->hqk', do_blk.astype(jnp.float32), v_bf.astype(jnp.float32))
        delta = jnp.transpose(lax.optimization_barrier(jnp.sum(do_blk.astype(jnp.float32) * o_blk.astype(jnp.float32), axis=2)))[:, :, None]
        dscore = kept((probs * (dprob - delta)).astype(jnp.bfloat16)).astype(jnp.float32)
        dq_parts.append(jnp.einsum('hqk,khe->qhe', dscore, k_bf.astype(jnp.float32)) * score_scale)
        dk_acc = dk_acc + jnp.einsum('hqk,qhe->khe', dscore, q_blk.astype(jnp.float32)) * score_scale
        dv_acc = dv_acc + jnp.einsum('hqk,qhe->khe', probs_bf.astype(jnp.float32), do_blk.astype(jnp.float32))
    return (jnp.concatenate(dq_parts, axis=0), dk_acc, dv_acc.astype(jnp.bfloat16))

def norm_back(raw, inv_scale, gained):
    return inv_scale * gained - raw * inv_scale ** 3 * lax.optimization_barrier(jnp.mean(gained * raw, axis=1, keepdims=True))

def layer_rows(x_rows, cot_rows, seg_row, live_n, weights, gains):
    w_query, w_key, w_value, w_output, w_gate, w_up, w_down = weights
    query_gain, key_gain, attn_gain, ffn_gain = gains
    row_count, width = x_rows.shape
    head_size = HD
    heads = width // head_size
    score_scale = 1.0 / math.sqrt(head_size)
    live_mask = (jnp.arange(row_count, dtype=jnp.int32) < live_n).astype(jnp.float32)[:, None]
    cos_tab, sin_tab = rotary_tables(doc_positions(seg_row), head_size)
    q_proj = jnp.dot(x_rows, w_query, preferred_element_type=jnp.float32)
    k_proj = jnp.dot(x_rows, w_key, preferred_element_type=jnp.float32)
    v_bf = jnp.dot(x_rows, w_value, preferred_element_type=jnp.float32).astype(jnp.bfloat16)
    inv_q = lax.rsqrt(lax.optimization_barrier(jnp.mean(q_proj * q_proj, axis=1, keepdims=True)) + EPS)
    inv_k = lax.rsqrt(lax.optimization_barrier(jnp.mean(k_proj * k_proj, axis=1, keepdims=True)) + EPS)
    q_rot = kept(rotate((q_proj * inv_q * query_gain).reshape(row_count, heads, head_size), cos_tab, sin_tab).astype(jnp.bfloat16))
    k_rot = kept(rotate((k_proj * inv_k * key_gain).reshape(row_count, heads, head_size), cos_tab, sin_tab).astype(jnp.bfloat16))
    v_heads = kept(v_bf).reshape(row_count, heads, head_size)
    o_bf, lse_parts = attend_forward(q_rot, k_rot, v_heads, seg_row, score_scale)
    o_flat = o_bf.reshape(row_count, width)
    attn_raw = jnp.dot(o_flat, w_output, preferred_element_type=jnp.float32)
    inv_a = lax.rsqrt(lax.optimization_barrier(jnp.mean(attn_raw * attn_raw, axis=1, keepdims=True)) + EPS)
    h_mid = x_rows.astype(jnp.float32) + attn_raw * inv_a * attn_gain
    h_bf = h_mid.astype(jnp.bfloat16)
    gate_pre = jnp.dot(h_bf, w_gate, preferred_element_type=jnp.float32)
    up_pre = jnp.dot(h_bf, w_up, preferred_element_type=jnp.float32)
    act_bf = (jax.nn.silu(gate_pre) * up_pre).astype(jnp.bfloat16)
    ffn_raw = jnp.dot(act_bf, w_down, preferred_element_type=jnp.float32)
    inv_f = lax.rsqrt(lax.optimization_barrier(jnp.mean(ffn_raw * ffn_raw, axis=1, keepdims=True)) + EPS)
    out_rows = (live_mask * (h_mid + ffn_raw * inv_f * ffn_gain)).astype(jnp.bfloat16)
    dy = live_mask * cot_rows.astype(jnp.float32)
    g_ffn_gain = lax.optimization_barrier(jnp.sum(dy * ffn_raw * inv_f, axis=0))
    d_ffn = norm_back(ffn_raw, inv_f, ffn_gain * dy).astype(jnp.bfloat16)
    d_act = jnp.dot(d_ffn, w_down.T, preferred_element_type=jnp.float32)
    sig = jax.nn.sigmoid(gate_pre)
    d_up = (d_act * gate_pre * sig).astype(jnp.bfloat16)
    d_gate = (d_act * up_pre * sig * (1.0 + gate_pre * (1.0 - sig))).astype(jnp.bfloat16)
    dh = dy + (jnp.dot(d_gate, w_gate.T, preferred_element_type=jnp.float32) + jnp.dot(d_up, w_up.T, preferred_element_type=jnp.float32))
    g_down = jnp.dot(act_bf.T, d_ffn, preferred_element_type=jnp.float32)
    g_gate = jnp.dot(h_bf.T, d_gate, preferred_element_type=jnp.float32)
    g_up = jnp.dot(h_bf.T, d_up, preferred_element_type=jnp.float32)
    g_attn_gain = lax.optimization_barrier(jnp.sum(dh * attn_raw * inv_a, axis=0))
    d_attn = norm_back(attn_raw, inv_a, attn_gain * dh).astype(jnp.bfloat16)
    d_heads = kept(jnp.dot(d_attn, w_output.T, preferred_element_type=jnp.float32).astype(jnp.bfloat16))
    g_output = jnp.dot(o_flat.T, d_attn, preferred_element_type=jnp.float32)
    dq_rot, dk_rot, d_val = attend_backward(q_rot, k_rot, v_heads, o_bf, d_heads.reshape(row_count, heads, head_size), lse_parts, seg_row, score_scale)
    dq_norm = rotate_back(dq_rot, cos_tab, sin_tab).reshape(row_count, width)
    dk_norm = rotate_back(dk_rot, cos_tab, sin_tab).reshape(row_count, width)
    g_query_gain = lax.optimization_barrier(jnp.sum(dq_norm * q_proj * inv_q, axis=0))
    g_key_gain = lax.optimization_barrier(jnp.sum(dk_norm * k_proj * inv_k, axis=0))
    dq_bf = norm_back(q_proj, inv_q, query_gain * dq_norm).astype(jnp.bfloat16)
    dk_bf = norm_back(k_proj, inv_k, key_gain * dk_norm).astype(jnp.bfloat16)
    dv_bf = d_val.reshape(row_count, width)
    dx_rows = dh + (jnp.dot(dq_bf, w_query.T, preferred_element_type=jnp.float32) + jnp.dot(dk_bf, w_key.T, preferred_element_type=jnp.float32) + jnp.dot(dv_bf, w_value.T, preferred_element_type=jnp.float32))
    g_query = jnp.dot(x_rows.T, dq_bf, preferred_element_type=jnp.float32)
    g_key = jnp.dot(x_rows.T, dk_bf, preferred_element_type=jnp.float32)
    g_value = jnp.dot(x_rows.T, dv_bf, preferred_element_type=jnp.float32)
    grads = (g_query, g_key, g_value, g_output, g_gate, g_up, g_down, g_query_gain, g_key_gain, g_attn_gain, g_ffn_gain)
    return ((out_rows, dx_rows), grads)

def reference(hidden_in, cotangent, segments, live_counts, w_query, w_key, w_value, w_output, w_gate, w_up, w_down, query_gain, key_gain, attn_gain, ffn_gain):
    n_blocks, row_count = segments.shape
    width = hidden_in.shape[1]
    weights = (w_query, w_key, w_value, w_output, w_gate, w_up, w_down)
    gains = (query_gain, key_gain, attn_gain, ffn_gain)
    init = tuple((jnp.zeros(item.shape, jnp.float32) for item in weights + gains))

    def one_block(carry, inputs):
        x_rows, cot_rows, seg_row, live_n = inputs
        outputs, grads = layer_rows(x_rows, cot_rows, seg_row, live_n, weights, gains)
        return (tuple((total + term for total, term in zip(carry, grads))), outputs)
    totals, stacked = lax.scan(one_block, init, (hidden_in.reshape(n_blocks, row_count, width), cotangent.reshape(n_blocks, row_count, width), segments, live_counts))
    hidden_out = stacked[0].reshape(n_blocks * row_count, width)
    grad_in = stacked[1].reshape(n_blocks * row_count, width)
    return (hidden_out, grad_in, totals[0], totals[1], totals[2], totals[3], totals[4], totals[5], totals[6], totals[7], totals[8], totals[9], totals[10])
```

```python
import math

import jax
import jax.numpy as jnp
from jax import lax
from jax.sharding import PartitionSpec as P

HD = 128


EPS = 1e-06
THETA = 500000.0


def doc_positions(seg_row):
    row_count = seg_row.shape[0]
    row_index = jnp.arange(row_count, dtype=jnp.int32)
    change = jnp.concatenate([jnp.ones((1,), dtype=bool), seg_row[1:] != seg_row[:-1]])
    doc_start = lax.cummax(jnp.where(change, row_index, jnp.zeros_like(row_index)), axis=0)
    return (row_index - doc_start).astype(jnp.float32)


def rotary_tables(positions, head_size):
    half_size = head_size // 2
    inv_freq = THETA ** (-(jnp.arange(half_size, dtype=jnp.float32) * (2.0 / head_size)))
    angles = positions[:, None] * inv_freq[None, :]
    return (jnp.cos(angles)[:, None, :], jnp.sin(angles)[:, None, :])


def rotate(values, cos_tab, sin_tab):
    half_size = values.shape[2] // 2
    first_half = values[:, :, :half_size]
    second_half = values[:, :, half_size:]
    return jnp.concatenate(
        [
            first_half * cos_tab - second_half * sin_tab,
            second_half * cos_tab + first_half * sin_tab,
        ],
        axis=2,
    )


def rotate_back(grads, cos_tab, sin_tab):
    half_size = grads.shape[2] // 2
    first_half = grads[:, :, :half_size]
    second_half = grads[:, :, half_size:]
    return jnp.concatenate(
        [
            first_half * cos_tab + second_half * sin_tab,
            second_half * cos_tab - first_half * sin_tab,
        ],
        axis=2,
    )


def block_mask(seg_row, offset, block_rows):
    row_index = jnp.arange(seg_row.shape[0])
    same = seg_row[offset : offset + block_rows, None] == seg_row[None, :]
    return same & (row_index[:, None] >= row_index[None, :])


def block_scores(q_blk, k_bf, allowed, score_scale):
    scores = (
        jnp.einsum("qhe,khe->hqk", q_blk, k_bf, preferred_element_type=jnp.float32) * score_scale
    )
    return jnp.where(allowed[None], scores, jnp.float32(-1e30))


def attend_forward(q_bf, k_bf, v_bf, seg_row, score_scale):
    row_count = q_bf.shape[0]
    block_rows = min(512, row_count)
    allowed = block_mask(seg_row, 0, block_rows)
    scores = block_scores(q_bf, k_bf, allowed, score_scale)
    row_max = jnp.max(scores, axis=2, keepdims=True)
    lse = row_max + jnp.log(jnp.sum(jnp.exp(scores - row_max), axis=2, keepdims=True))
    probs = jnp.exp(scores - lse).astype(jnp.bfloat16)
    outputs = jnp.einsum("hqk,khe->qhe", probs, v_bf, preferred_element_type=jnp.float32)
    lse_parts = [lse]
    return (outputs.astype(jnp.bfloat16), lse_parts)


def attend_backward(q_bf, k_bf, v_bf, o_bf, do_bf, lse_parts, seg_row, score_scale):
    row_count = q_bf.shape[0]
    block_rows = min(512, row_count)
    dq_parts = []
    dk_acc = jnp.zeros(k_bf.shape, jnp.float32)
    dv_acc = jnp.zeros(v_bf.shape, jnp.float32)
    for part_index, offset in enumerate(range(0, row_count, block_rows)):
        allowed = block_mask(seg_row, offset, block_rows)
        scores = block_scores(q_bf, k_bf, allowed, score_scale)
        probs = jnp.exp(scores - lse_parts[part_index])
        probs_bf = probs.astype(jnp.bfloat16)
        dprob = jnp.einsum("qhe,khe->hqk", do_bf, v_bf, preferred_element_type=jnp.float32)
        delta = jnp.transpose(
            jnp.sum(do_bf.astype(jnp.float32) * o_bf.astype(jnp.float32), axis=2)
        )[:, :, None]
        dscore = (probs * (dprob - delta)).astype(jnp.bfloat16)
        dq_parts.append(
            jnp.einsum("hqk,khe->qhe", dscore, k_bf, preferred_element_type=jnp.float32)
            * score_scale
        )
        dk_acc = (
            jnp.einsum("hqk,qhe->khe", dscore, q_bf, preferred_element_type=jnp.float32)
            * score_scale
        )
        dv_acc = jnp.einsum("hqk,qhe->khe", probs_bf, do_bf, preferred_element_type=jnp.float32)
    return (dq_parts[0], dk_acc, dv_acc.astype(jnp.bfloat16))


def scatter_grad(grad, axis_name, scatter_dimension, tiled):
    total = lax.psum_scatter(
        grad.astype(jnp.bfloat16), axis_name, scatter_dimension=scatter_dimension, tiled=tiled
    )
    return total.astype(jnp.float32)


def sum_parts(part, axis_name):
    own = lax.psum_scatter(
        part.astype(jnp.bfloat16), axis_name, scatter_dimension=0, tiled=True
    )
    return lax.all_gather(own, axis_name, axis=0, tiled=True).astype(jnp.float32)


def norm_back(raw, inv_scale, gained, row_sums, width):
    return inv_scale * gained - raw * inv_scale**3 * (row_sums[:, None] / width)


def on_device(
    hidden_in,
    cotangent,
    segments,
    live_counts,
    w_query,
    w_key,
    w_value,
    w_output,
    w_gate,
    w_up,
    w_down,
    query_gain,
    key_gain,
    attn_gain,
    ffn_gain,
):
    gathered = (
        lax.all_gather(w_query, "dp", axis=0, tiled=True),
        lax.all_gather(w_key, "dp", axis=0, tiled=True),
        lax.all_gather(w_value, "dp", axis=0, tiled=True),
        lax.all_gather(w_output, "dp", axis=1, tiled=True),
        lax.all_gather(w_gate, "dp", axis=0, tiled=True),
        lax.all_gather(w_up, "dp", axis=0, tiled=True),
        lax.all_gather(w_down, "dp", axis=1, tiled=True),
    )
    wq_full, wk_full, wv_full, wo_full, wg_full, wu_full, wd_full = gathered
    seg_row = segments[0]
    live_n = live_counts[0]
    row_count, width = hidden_in.shape
    local_width = wq_full.shape[1]
    heads_here = local_width // HD
    score_scale = 1.0 / math.sqrt(HD)
    live_mask = (jnp.arange(row_count, dtype=jnp.int32) < live_n).astype(jnp.float32)[:, None]
    cos_tab, sin_tab = rotary_tables(doc_positions(seg_row), HD)
    q_proj = jnp.dot(hidden_in, wq_full, preferred_element_type=jnp.float32)
    k_proj = jnp.dot(hidden_in, wk_full, preferred_element_type=jnp.float32)
    v_bf = jnp.dot(hidden_in, wv_full, preferred_element_type=jnp.float32).astype(jnp.bfloat16)
    sq_query, sq_key = lax.psum(
        (jnp.sum(q_proj * q_proj, axis=1), jnp.sum(k_proj * k_proj, axis=1)), "mp"
    )
    inv_q = lax.rsqrt(sq_query[:, None] / width + EPS)
    inv_k = lax.rsqrt(sq_key[:, None] / width + EPS)
    q_rot = rotate(
        (q_proj * inv_q * query_gain).reshape(row_count, heads_here, HD), cos_tab, sin_tab
    ).astype(jnp.bfloat16)
    k_rot = rotate(
        (k_proj * inv_k * key_gain).reshape(row_count, heads_here, HD), cos_tab, sin_tab
    ).astype(jnp.bfloat16)
    v_heads = v_bf.reshape(row_count, heads_here, HD)
    o_bf, lse_parts = attend_forward(q_rot, k_rot, v_heads, seg_row, score_scale)
    o_flat = o_bf.reshape(row_count, local_width)
    attn_raw = sum_parts(jnp.dot(o_flat, wo_full, preferred_element_type=jnp.float32), "mp")
    inv_a = lax.rsqrt(jnp.mean(attn_raw * attn_raw, axis=1, keepdims=True) + EPS)
    h_mid = hidden_in.astype(jnp.float32) + attn_raw * inv_a * attn_gain
    h_bf = h_mid.astype(jnp.bfloat16)
    gate_pre = jnp.dot(h_bf, wg_full, preferred_element_type=jnp.float32)
    up_pre = jnp.dot(h_bf, wu_full, preferred_element_type=jnp.float32)
    act_bf = (jax.nn.silu(gate_pre) * up_pre).astype(jnp.bfloat16)
    ffn_raw = sum_parts(jnp.dot(act_bf, wd_full, preferred_element_type=jnp.float32), "mp")
    inv_f = lax.rsqrt(jnp.mean(ffn_raw * ffn_raw, axis=1, keepdims=True) + EPS)
    hidden_out = (live_mask * (h_mid + ffn_raw * inv_f * ffn_gain)).astype(jnp.bfloat16)
    wq_back, wk_back, wv_back, wo_back, wg_back, wu_back, wd_back = gathered
    dy = live_mask * cotangent.astype(jnp.float32)
    g_ffn_gain = jnp.sum(dy * ffn_raw * inv_f, axis=0)
    gained_f = ffn_gain * dy
    d_ffn = norm_back(ffn_raw, inv_f, gained_f, jnp.sum(gained_f * ffn_raw, axis=1), width).astype(
        jnp.bfloat16
    )
    d_act = jnp.dot(d_ffn, wd_back.T, preferred_element_type=jnp.float32)
    sig = jax.nn.sigmoid(gate_pre)
    d_up = (d_act * gate_pre * sig).astype(jnp.bfloat16)
    d_gate = (d_act * up_pre * sig * (1.0 + gate_pre * (1.0 - sig))).astype(jnp.bfloat16)
    ffn_part = jnp.dot(d_gate, wg_back.T, preferred_element_type=jnp.float32) + jnp.dot(
        d_up, wu_back.T, preferred_element_type=jnp.float32
    )
    dh = dy + sum_parts(ffn_part, "mp")
    g_down = jnp.dot(act_bf.T, d_ffn, preferred_element_type=jnp.float32)
    g_gate = jnp.dot(h_bf.T, d_gate, preferred_element_type=jnp.float32)
    g_up = jnp.dot(h_bf.T, d_up, preferred_element_type=jnp.float32)
    g_attn_gain = jnp.sum(dh * attn_raw * inv_a, axis=0)
    gained_a = attn_gain * dh
    d_attn = norm_back(
        attn_raw, inv_a, gained_a, jnp.sum(gained_a * attn_raw, axis=1), width
    ).astype(jnp.bfloat16)
    d_heads = jnp.dot(d_attn, wo_back.T, preferred_element_type=jnp.float32).astype(jnp.bfloat16)
    g_output = jnp.dot(o_flat.T, d_attn, preferred_element_type=jnp.float32)
    dq_rot, dk_rot, d_val = attend_backward(
        q_rot,
        k_rot,
        v_heads,
        o_bf,
        d_heads.reshape(row_count, heads_here, HD),
        lse_parts,
        seg_row,
        score_scale,
    )
    dq_norm = rotate_back(dq_rot, cos_tab, sin_tab).reshape(row_count, local_width)
    dk_norm = rotate_back(dk_rot, cos_tab, sin_tab).reshape(row_count, local_width)
    g_query_gain = jnp.sum(dq_norm * q_proj * inv_q, axis=0)
    g_key_gain = jnp.sum(dk_norm * k_proj * inv_k, axis=0)
    gained_q = query_gain * dq_norm
    gained_k = key_gain * dk_norm
    sums_query, sums_key = lax.psum(
        (jnp.sum(gained_q * q_proj, axis=1), jnp.sum(gained_k * k_proj, axis=1)), "mp"
    )
    dq_bf = norm_back(q_proj, inv_q, gained_q, sums_query, width).astype(jnp.bfloat16)
    dk_bf = norm_back(k_proj, inv_k, gained_k, sums_key, width).astype(jnp.bfloat16)
    dv_bf = d_val.reshape(row_count, local_width)
    input_part = (
        jnp.dot(dq_bf, wq_back.T, preferred_element_type=jnp.float32)
        + jnp.dot(dk_bf, wk_back.T, preferred_element_type=jnp.float32)
        + jnp.dot(dv_bf, wv_back.T, preferred_element_type=jnp.float32)
    )
    grad_in = dh + sum_parts(input_part, "mp")
    g_query = jnp.dot(hidden_in.T, dq_bf, preferred_element_type=jnp.float32)
    g_key = jnp.dot(hidden_in.T, dk_bf, preferred_element_type=jnp.float32)
    g_value = jnp.dot(hidden_in.T, dv_bf, preferred_element_type=jnp.float32)
    owned = (
        scatter_grad(g_query, "dp", scatter_dimension=0, tiled=True),
        scatter_grad(g_key, "dp", scatter_dimension=0, tiled=True),
        scatter_grad(g_value, "dp", scatter_dimension=0, tiled=True),
        scatter_grad(g_output, "dp", scatter_dimension=1, tiled=True),
        scatter_grad(g_gate, "dp", scatter_dimension=0, tiled=True),
        scatter_grad(g_up, "dp", scatter_dimension=0, tiled=True),
        scatter_grad(g_down, "dp", scatter_dimension=1, tiled=True),
    )
    gain_totals = lax.psum((g_query_gain, g_key_gain, g_attn_gain, g_ffn_gain), "dp")
    return (
        hidden_out,
        grad_in,
        owned[0],
        owned[1],
        owned[2],
        owned[3],
        owned[4],
        owned[5],
        owned[6],
        gain_totals[0],
        gain_totals[1],
        gain_totals[2],
        gain_totals[3],
    )


def solution(mesh):
    return jax.shard_map(
        on_device,
        mesh=mesh,
        in_specs=(
            P("dp", None),
            P("dp", None),
            P("dp", None),
            P("dp"),
            P("dp", "mp"),
            P("dp", "mp"),
            P("dp", "mp"),
            P("mp", "dp"),
            P("dp", "mp"),
            P("dp", "mp"),
            P("mp", "dp"),
            P("mp"),
            P("mp"),
            P(),
            P(),
        ),
        out_specs=(
            P("dp", None),
            P("dp", None),
            P("dp", "mp"),
            P("dp", "mp"),
            P("dp", "mp"),
            P("mp", "dp"),
            P("dp", "mp"),
            P("dp", "mp"),
            P("mp", "dp"),
            P("mp"),
            P("mp"),
            P(),
            P(),
        ),
        check_vma=False,
    )
```

```python
import functools, math
import jax, jax.numpy as jnp
from jax import lax
from jax.experimental import pallas as pl
from jax.experimental.pallas import tpu as pltpu
from jax.sharding import PartitionSpec as P

HD = 128
EPS = 1e-06
THETA = 500000.0
UNIT = 256
BF = jnp.bfloat16
F32 = jnp.float32
NT = (((1,), (1,)), ((), ()))


def dot(a, b):
    return jnp.dot(a, b, preferred_element_type=F32)


def dot_nt(a, b):
    return lax.dot_general(a, b, NT, preferred_element_type=F32)


def dot_tn(a, b):
    return lax.dot_general(a, b, (((0,), (0,)), ((), ())), preferred_element_type=F32)


class Place:
    def __init__(self, n_mp):
        self.dp = lax.axis_index("dp")
        self.z = lax.axis_index("mp")
        self.n_mp = n_mp
        self.c = lax.rem(self.dp, 2)
        self.x = lax.rem(self.dp // 2, 2)
        self.y = self.dp // 4
        self.sib = self.dp + 1 - 2 * self.c
        self.xn = self.dp + 2 - 4 * self.x
        self.yn = self.dp + 4 - 8 * self.y
        self.dg = self.xn + 4 - 8 * self.y
        flip = 1 - 2 * self.c
        self.order = (
            self.dp, self.sib, self.xn, self.xn + flip,
            self.yn, self.yn + flip, self.dg, self.dg + flip,
        )

    def at(self, dp):
        return {"dp": dp}

    def barrier(self):
        sem = pltpu.get_barrier_semaphore()
        for dp in (self.sib, self.xn, self.yn):
            pl.semaphore_signal(sem, inc=1, device_id={"dp": dp}, device_id_type=pl.DeviceIdType.MESH)
        for step in range(1, self.n_mp):
            pl.semaphore_signal(
                sem, inc=1, device_id={"mp": lax.rem(self.z + step, self.n_mp)},
                device_id_type=pl.DeviceIdType.MESH,
            )
        pl.semaphore_wait(sem, 3 + self.n_mp - 1)


def remote(src, dst, send, recv, device):
    return pltpu.make_async_remote_copy(
        src_ref=src, dst_ref=dst, send_sem=send, recv_sem=recv,
        device_id=device, device_id_type=pl.DeviceIdType.MESH,
    )


class Gather:
    def __init__(self, place, src, full, by_rows, send, recv, local):
        self.place, self.src, self.full, self.by_rows = place, src, full, by_rows
        self.send, self.recv, self.local = send, recv, local
        self.rows, self.cols = src.shape
        self.half = self.rows // 2

    def spot(self, owner, part=None):
        first, count = (0, self.rows) if part is None else (part * self.half, self.half)
        if self.by_rows:
            start = pl.multiple_of(owner * self.rows + first, self.half)
            return self.full.at[pl.ds(start, count), :]
        start = pl.multiple_of(owner * self.cols, self.cols)
        return self.full.at[pl.ds(first, count), pl.ds(start, self.cols)]

    def mine(self, part=None):
        if part is None:
            return self.src
        return self.src.at[pl.ds(part * self.half, self.half), :]

    def copies(self):
        p = self.place
        return {
            0: (self.mine(0), p.dp, 0, p.xn, p.xn),
            1: (self.mine(1), p.dp, 1, p.xn, p.xn),
            2: (self.mine(0), p.dp, 0, p.yn, p.yn),
            3: (self.mine(1), p.dp, 1, p.yn, p.yn),
            4: (self.spot(p.yn, 1), p.yn, 1, p.xn, p.dg),
            5: (self.spot(p.xn, 0), p.xn, 0, p.yn, p.dg),
            6: (self.mine(), p.dp, None, p.sib, p.order[1]),
            7: (self.spot(p.xn), p.xn, None, p.sib, p.order[3]),
            8: (self.spot(p.yn), p.yn, None, p.sib, p.order[5]),
            9: (self.spot(p.dg), p.dg, None, p.sib, p.order[7]),
        }

    def start(self, *kinds):
        table = self.copies()
        for kind in kinds:
            src, owner, part, target, _ = table[kind]
            remote(src, self.spot(owner, part), self.send.at[kind], self.recv.at[kind], {"dp": target}).start()

    def arrived(self, *kinds):
        table = self.copies()
        for kind in kinds:
            src, _, part, target, owner = table[kind]
            spot = self.spot(owner, part)
            remote(spot, spot, self.send.at[kind], self.recv.at[kind], {"dp": target}).wait_recv()

    def own_copy(self):
        return pltpu.make_async_copy(self.src, self.spot(self.place.dp), self.local)

    def begin_a(self):
        self.start(0, 3)

    def begin_b(self):
        self.start(1, 2, 6)
        self.own_copy().start()

    def relay(self):
        self.arrived(0)
        self.start(5)
        self.arrived(3)
        self.start(4)

    def pass_on(self):
        self.arrived(1)
        self.start(7)
        self.arrived(2)
        self.start(8)

    def last(self):
        self.arrived(5, 4)
        self.start(9)

    def ready(self):
        self.own_copy().wait()
        self.arrived(6, 7, 8, 9)

    def drain(self):
        table = self.copies()
        for kind in range(10):
            src, owner, part, target, _ = table[kind]
            remote(src, self.spot(owner, part), self.send.at[kind], self.recv.at[kind], {"dp": target}).wait_send()


class RowSum:
    def __init__(self, place, part, took, total, sems, columns):
        self.place, self.part, self.took, self.total, self.sems = place, part, took, total, sems
        self.columns = columns
        self.width = part.shape[1] // len(columns)
        self.count = len(columns) // 2

    def spot(self, ref, flow, k):
        block = self.columns[2 * k + flow]
        return ref.at[:, pl.ds(pl.multiple_of(block * self.width, self.width), self.width)]

    def where(self, flow):
        p = self.place
        at = p.z if flow == 0 else p.n_mp - 1 - p.z
        step = 1 if flow == 0 else -1
        return at, {"mp": p.z + step}, {"mp": p.z - step}

    def forth(self, flow, k):
        return remote(
            self.spot(self.part, flow, k), self.took.at[flow, k],
            self.sems.at[0, flow, k], self.sems.at[1, flow, k], self.where(flow)[1],
        )

    def back(self, flow, k):
        spot = self.spot(self.total, flow, k)
        return remote(spot, spot, self.sems.at[2, flow, k], self.sems.at[3, flow, k], self.where(flow)[2])

    def begin(self, flow, k):
        @pl.when(self.where(flow)[0] == 0)
        def _():
            self.forth(flow, k).start()

    def gather_steps(self, tick):
        for pos in range(1, self.place.n_mp):
            k = tick - (pos - 1)
            if 0 <= k < self.count:
                for flow in range(2):
                    @pl.when(self.where(flow)[0] == pos)
                    def _():
                        self.gather_step(flow, k)

    def return_steps(self, tick):
        for pos in range(self.place.n_mp - 2, -1, -1):
            k = tick - (self.place.n_mp - 2 - pos)
            if 0 <= k < self.count:
                for flow in range(2):
                    @pl.when(self.where(flow)[0] == pos)
                    def _():
                        self.return_step(flow, k)

    @property
    def ticks(self):
        return self.count + self.place.n_mp - 2

    def gather_step(self, flow, k):
        at = self.where(flow)[0]
        last = self.place.n_mp - 1

        @pl.when(at > 0)
        def _():
            self.forth(flow, k).wait_recv()

        @pl.when((at > 0) & (at < last))
        def _():
            spot = self.spot(self.part, flow, k)
            spot[...] = (spot[...].astype(F32) + self.took[flow, k].astype(F32)).astype(BF)
            self.forth(flow, k).start()

        @pl.when(at == last)
        def _():
            mine = self.spot(self.part, flow, k)
            self.spot(self.total, flow, k)[...] = (mine[...].astype(F32) + self.took[flow, k].astype(F32)).astype(BF)
            self.back(flow, k).start()

    def return_step(self, flow, k):
        at = self.where(flow)[0]
        last = self.place.n_mp - 1

        @pl.when(at < last)
        def _():
            self.back(flow, k).wait_recv()

        @pl.when((at > 0) & (at < last))
        def _():
            self.back(flow, k).start()

    def drain(self):
        last = self.place.n_mp - 1
        for flow in range(2):
            for k in range(self.count):
                @pl.when(self.where(flow)[0] < last)
                def _():
                    self.forth(flow, k).wait_send()

                @pl.when(self.where(flow)[0] > 0)
                def _():
                    self.back(flow, k).wait_send()


def as_row(col):
    n = col.shape[0]
    r = lax.broadcasted_iota(jnp.int32, (n, n), 0)
    s = lax.broadcasted_iota(jnp.int32, (n, n), 1)
    return jnp.sum(jnp.where(r == s, col, 0.0), axis=0, keepdims=True)


def as_col(row):
    n = row.shape[1]
    r = lax.broadcasted_iota(jnp.int32, (n, n), 0)
    s = lax.broadcasted_iota(jnp.int32, (n, n), 1)
    return jnp.sum(jnp.where(r == s, row, 0.0), axis=1, keepdims=True)


class SmallSum:
    def __init__(self, place, slots, sems):
        self.place, self.slots, self.sems = place, slots, sems

    def copy(self, step):
        p = self.place
        return remote(
            self.slots.at[0], self.slots.at[step], self.sems.at[0, step], self.sems.at[1, step],
            {"mp": lax.rem(p.z + step, p.n_mp)},
        )

    def begin(self):
        for step in range(1, self.place.n_mp):
            self.copy(step).start()

    def end(self):
        for step in range(1, self.place.n_mp):
            self.copy(step).wait_recv()
        total = self.slots[0]
        for step in range(1, self.place.n_mp):
            total = total + self.slots[step]
        return total

    def drain(self):
        for step in range(1, self.place.n_mp):
            self.copy(step).wait_send()


def turn(values, cos_tab, sin_tab):
    return values * cos_tab + pltpu.roll(values, HD // 2, 1) * sin_tab


def forward_kernel(
    n_mp,
    x_in, wq_in, wk_in, wv_in, wo_in, wg_in, wu_in, wd_in,
    cos_ref, sin_ref, seg_col, seg_row, q_gain, k_gain, a_gain,
    wq_out, wk_out, wv_out, wo_out, wg_out, wu_out, wd_out,
    qp_out, kp_out, qr_out, kr_out, v_out, o_out, stat_out, raw_a_out, h_out,
    gate_out, up_out, act_out, raw_f_out,
    wq, wk, wv, wo, wg, wu, wd,
    x, qp, kp, qr, kr, v, o, stat, raw_a, h, gate, up, act, raw_f, part, took, sums,
    g_send, g_recv, g_local, sum_a, sum_f, small, out_sem, x_sem,
):
    place = Place(n_mp)
    rows, width = x.shape
    local = qp.shape[1]
    heads = local // HD
    scale = 1.0 / math.sqrt(HD)
    place.barrier()
    ins = (wq_in, wk_in, wv_in, wo_in, wg_in, wu_in, wd_in)
    fulls = (wq, wk, wv, wo, wg, wu, wd)
    outs = (wq_out, wk_out, wv_out, wo_out, wg_out, wu_out, wd_out)
    gq, gk, gv, go, gg, gu, gd = [
        Gather(place, ins[i], fulls[i], i not in (3, 6), g_send.at[i], g_recv.at[i], g_local.at[i])
        for i in range(7)
    ]
    gathers = (gq, gk, gv, go, gg, gu, gd)
    started = []

    def save(index, src, dst):
        copy = pltpu.make_async_copy(src, dst, out_sem.at[index])
        copy.start()
        started.append(copy)

    get_x = pltpu.make_async_copy(x_in, x, x_sem)
    get_x.start()
    gq.begin_a()
    gq.begin_b()
    gk.begin_a()
    gk.begin_b()
    gq.relay()
    gv.begin_a()
    gq.pass_on()
    gv.begin_b()
    gk.relay()
    go.begin_a()
    gk.pass_on()
    go.begin_b()
    gq.last()
    get_x.wait()
    gq.ready()
    save(0, wq, wq_out)
    half = rows // 2
    norm_sum = SmallSum(place, sums, small)

    def project(full, dst):
        squares = []
        for r in range(2):
            value = dot(x[r * half:(r + 1) * half, :], full[...])
            dst[r * half:(r + 1) * half, :] = value.astype(dst.dtype)
            squares.append(jnp.sum(value * value, axis=1, keepdims=True))
        return jnp.concatenate(squares, axis=0)

    sums[0] = jnp.zeros(sums.shape[1:], F32)
    sums[0, 0:1, :] = as_row(project(wq, qp))
    gv.relay()
    gk.last()
    gk.ready()
    save(1, wk, wk_out)
    sums[0, 1:2, :] = as_row(project(wk, kp))
    norm_sum.begin()
    gv.pass_on()
    go.relay()
    gg.begin_a()
    go.pass_on()
    gg.begin_b()
    gv.last()
    gv.ready()
    save(2, wv, wv_out)
    project(wv, v)
    totals = norm_sum.end()
    inv_q = lax.rsqrt(as_col(totals[0:1, :]) / width + EPS)
    inv_k = lax.rsqrt(as_col(totals[1:2, :]) / width + EPS)
    stat[:, heads:heads + 1] = inv_q
    stat[:, heads + 1:heads + 2] = inv_k
    save(7, qp, qp_out)
    save(8, kp, kp_out)
    save(9, v, v_out)
    block = rows // 4
    for hd in range(heads):
        cols = slice(hd * HD, (hd + 1) * HD)
        qr[:, cols] = turn(qp[:, cols] * inv_q * q_gain[:, cols], cos_ref[...], sin_ref[...]).astype(BF)
        kr[:, cols] = turn(kp[:, cols] * inv_k * k_gain[:, cols], cos_ref[...], sin_ref[...]).astype(BF)
    save(10, qr, qr_out)
    save(11, kr, kr_out)
    for rb in range(4):
        near = slice(rb * block, (rb + 1) * block)
        keys = (rb + 1) * block
        t_at = lax.broadcasted_iota(jnp.int32, (block, keys), 0) + rb * block
        s_at = lax.broadcasted_iota(jnp.int32, (block, keys), 1)
        allowed = (seg_col[near, :] == seg_row[:, 0:keys]) & (s_at <= t_at)
        for hd in range(heads):
            cols = slice(hd * HD, (hd + 1) * HD)
            scores = jnp.where(allowed, dot_nt(qr[near, cols], kr[0:keys, cols]) * scale, -1e30)
            top = jnp.max(scores, axis=1, keepdims=True)
            weights = jnp.exp(scores - top)
            norm = jnp.sum(weights, axis=1, keepdims=True)
            stat[near, hd:hd + 1] = top + jnp.log(norm)
            o[near, cols] = dot((weights / norm).astype(BF), v[0:keys, cols]).astype(BF)
    save(12, o, o_out)
    save(13, stat, stat_out)
    go.last()
    go.ready()
    save(3, wo, wo_out)
    step_of = lambda block: pl.ds(pl.multiple_of(block * (width // 8), width // 8), width // 8)
    sum_attn = RowSum(place, part, took, raw_a, sum_a, place.order)
    for at in range(8):
        cols = step_of(place.order[at])
        part[:, cols] = dot(o[...], wo[:, cols]).astype(BF)
        sum_attn.begin(at % 2, at // 2)
    gu.begin_a()
    for tick in range(sum_attn.ticks):
        sum_attn.gather_steps(tick)
        if tick == 0:
            gg.relay()
            gu.begin_b()
        if tick == 2:
            gg.pass_on()
        if tick == 3:
            gg.last()
            gd.begin_a()
    for tick in range(sum_attn.ticks):
        sum_attn.return_steps(tick)
        if tick == 0:
            gu.relay()
            gd.begin_b()
        if tick == 2:
            gu.pass_on()
    sum_attn.drain()
    save(14, raw_a, raw_a_out)
    tile = rows // 8

    def mid(at, carry):
        near = pl.ds(pl.multiple_of(at * tile, tile), tile)
        raw = raw_a[near, :].astype(F32)
        inv = lax.rsqrt(jnp.mean(raw * raw, axis=1, keepdims=True) + EPS)
        h[near, :] = (x[near, :].astype(F32) + raw * inv * a_gain[...]).astype(BF)
        return carry

    lax.fori_loop(0, 8, mid, 0)
    save(15, h, h_out)
    gg.ready()
    save(4, wg, wg_out)
    n_tile = gate.shape[1] // UNIT

    def gate_tile(at, carry):
        cols = pl.ds(pl.multiple_of(at * UNIT, UNIT), UNIT)
        gate[:, cols] = dot(h[...], wg[:, cols]).astype(BF)
        return carry

    lax.fori_loop(0, n_tile, gate_tile, 0)
    gu.last()
    gd.relay()
    gu.ready()
    save(5, wu, wu_out)

    def up_tile(at, carry):
        cols = pl.ds(pl.multiple_of(at * UNIT, UNIT), UNIT)
        value = dot(h[...], wu[:, cols])
        up[:, cols] = value.astype(BF)
        pre = gate[:, cols].astype(F32)
        act[:, cols] = (pre * jax.nn.sigmoid(pre) * value).astype(BF)
        return carry

    lax.fori_loop(0, n_tile, up_tile, 0)
    save(16, gate, gate_out)
    save(17, up, up_out)
    save(18, act, act_out)
    sum_ffn = RowSum(place, part, took, raw_f, sum_f, place.order)
    for at in range(8):
        if at == 0:
            gd.own_copy().wait()
        elif at == 1:
            gd.arrived(6)
        elif at == 2:
            gd.pass_on()
        elif at == 3:
            gd.arrived(7)
        elif at == 5:
            gd.arrived(8)
        elif at == 6:
            gd.last()
        elif at == 7:
            gd.arrived(9)
        cols = step_of(place.order[at])
        part[:, cols] = dot(act[...], wd[:, cols]).astype(BF)
        sum_ffn.begin(at % 2, at // 2)
        if at in (4, 6):
            sum_ffn.gather_steps((at - 4) // 2)
    save(6, wd, wd_out)
    for tick in range(2, sum_ffn.ticks):
        sum_ffn.gather_steps(tick)
    for tick in range(sum_ffn.ticks):
        sum_ffn.return_steps(tick)
    save(19, raw_f, raw_f_out)
    sum_ffn.drain()
    norm_sum.drain()
    for g in gathers:
        g.drain()
    for copy in started:
        copy.wait()


def forward_call(n_mp, x, weights, cos_tab, sin_tab, seg_col, seg_row, q_gain, k_gain, a_gain):
    rows, width = x.shape
    n_dp = 8
    local = weights[0].shape[1]
    ff = weights[4].shape[1]
    any_spec = pl.BlockSpec(memory_space=pl.ANY)
    vmem = pl.BlockSpec(memory_space=pltpu.VMEM)
    S = jax.ShapeDtypeStruct
    fulls = [(width, local)] * 3 + [(local, width)] + [(width, ff)] * 2 + [(ff, width)]
    acts = [
        ((rows, local), F32), ((rows, local), F32), ((rows, local), BF), ((rows, local), BF),
        ((rows, local), BF), ((rows, local), BF), ((rows, 128), F32), ((rows, width), BF),
        ((rows, width), BF), ((rows, ff), BF), ((rows, ff), BF), ((rows, ff), BF), ((rows, width), BF),
    ]
    V = pltpu.VMEM
    dma = pltpu.SemaphoreType.DMA
    return pl.pallas_call(
        functools.partial(forward_kernel, n_mp),
        out_shape=[S(s, BF) for s in fulls] + [S(s, d) for s, d in acts],
        in_specs=[any_spec] * 8 + [vmem] * 7,
        out_specs=[any_spec] * 20,
        scratch_shapes=[V(s, BF) for s in fulls]
        + [V((rows, width), BF)]
        + [V(s, d) for s, d in acts]
        + [V((rows, width), BF), V((2, 4, rows, width // 8), BF), V((n_mp, 8, rows), F32)]
        + [dma((7, 10)), dma((7, 10)), dma((7,)), dma((4, 2, 4)), dma((4, 2, 4)), dma((2, n_mp)), dma((20,)), dma(())],
        compiler_params=pltpu.CompilerParams(
            collective_id=0, has_side_effects=True, vmem_limit_bytes=67043328,
        ),
    )(x, *weights, cos_tab, sin_tab, seg_col, seg_row, q_gain, k_gain, a_gain)


class Scatter:
    def __init__(self, place, out, give, got, sum_a, sum_b, got_a, got_b, end_a, end_b, done, sems, out_sems, n_units):
        self.place, self.out, self.n_units = place, out, n_units
        self.give, self.got, self.sum_a, self.sum_b = give, got, sum_a, sum_b
        self.got_a, self.got_b, self.end_a, self.end_b, self.done = got_a, got_b, end_a, end_b, done
        self.sems, self.out_sems = sems, out_sems
        self.rows, self.cols = give.shape[2:]
        self.half = self.rows // 2
        self.unit = 0

    def send(self, kind, u):
        p, s = self.place, u % 4
        src, dst, target = {
            0: (self.give.at[u % 2], self.got.at[s], p.sib),
            1: (self.sum_a.at[s, 1 - p.x], self.got_a.at[s], p.xn),
            2: (self.sum_b.at[s, 1 - p.y], self.got_b.at[s], p.yn),
            3: (self.sum_a.at[s, p.x, 1 - p.y], self.end_a.at[s], p.yn),
            4: (self.sum_b.at[s, p.y, 1 - p.x], self.end_b.at[s], p.xn),
        }[kind]
        return remote(src, dst, self.sems.at[0, kind, s], self.sems.at[1, kind, s], {"dp": target})

    def write(self, u):
        return pltpu.make_async_copy(self.done.at[u % 2], self.out.at[u], self.out_sems.at[u % 2])

    def product(self, u, turned, right, col):
        p = self.place
        if u >= 2:
            self.send(0, u - 2).wait_send()

        def other(chip, carry):
            near = pl.ds(pl.multiple_of((2 * chip + 1 - p.c) * self.rows, self.rows), self.rows)
            self.give[u % 2, chip] = dot(turned[near, :], right[:, col]).astype(BF)
            return carry

        lax.fori_loop(0, 4, other, 0)
        self.send(0, u).start()

        def own(chip, carry):
            near = pl.ds(pl.multiple_of((2 * chip + p.c) * self.rows, self.rows), self.rows)
            value = dot(turned[near, :], right[:, col]).astype(BF)
            y_to, x_to = chip // 2, lax.rem(chip, 2)
            self.sum_a[u % 4, x_to, y_to] = value[:self.half]
            self.sum_b[u % 4, y_to, x_to] = value[self.half:]
            return carry

        lax.fori_loop(0, 4, own, 0)

    def across(self, u):
        self.send(0, u).wait_recv()
        s = u % 4

        def add(chip, carry):
            y_to, x_to = chip // 2, lax.rem(chip, 2)
            more = self.got[s, chip].astype(F32)
            self.sum_a[s, x_to, y_to] = (self.sum_a[s, x_to, y_to].astype(F32) + more[:self.half]).astype(BF)
            self.sum_b[s, y_to, x_to] = (self.sum_b[s, y_to, x_to].astype(F32) + more[self.half:]).astype(BF)
            return carry

        lax.fori_loop(0, 4, add, 0)
        self.send(1, u).start()
        self.send(2, u).start()

    def along(self, u):
        p, s = self.place, u % 4
        self.send(1, u).wait_recv()
        for i in range(2):
            self.sum_a[s, p.x, i] = (self.sum_a[s, p.x, i].astype(F32) + self.got_a[s, i].astype(F32)).astype(BF)
        self.send(3, u).start()
        self.send(2, u).wait_recv()
        for i in range(2):
            self.sum_b[s, p.y, i] = (self.sum_b[s, p.y, i].astype(F32) + self.got_b[s, i].astype(F32)).astype(BF)
        self.send(4, u).start()
        self.send(1, u).wait_send()
        self.send(2, u).wait_send()

    def finish(self, u):
        p, s = self.place, u % 4
        if u >= 2:
            self.write(u - 2).wait()
        self.send(3, u).wait_recv()
        self.done[u % 2, :self.half] = self.sum_a[s, p.x, p.y].astype(F32) + self.end_a[s].astype(F32)
        self.send(4, u).wait_recv()
        self.done[u % 2, self.half:] = self.sum_b[s, p.y, p.x].astype(F32) + self.end_b[s].astype(F32)
        self.write(u).start()
        self.send(3, u).wait_send()
        self.send(4, u).wait_send()

    def tick(self, turned=None, right=None, col=None):
        u = self.unit
        self.unit += 1
        if u < self.n_units:
            self.product(u, turned, right, col)
        if 0 <= u - 1 < self.n_units:
            self.across(u - 1)
        if 0 <= u - 2 < self.n_units:
            self.along(u - 2)
        if 0 <= u - 3 < self.n_units:
            self.finish(u - 3)

    def drain(self):
        for u in (self.n_units - 2, self.n_units - 1):
            self.send(0, u).wait_send()
            self.write(u).wait()


def turn_back(grads, cos_tab, sin_tab):
    return grads * cos_tab - pltpu.roll(grads, HD // 2, 1) * sin_tab


def backward_kernel(
    n_mp,
    wq_in, wk_in, wv_in, wo_in, wg_in, wu_in, wd_in,
    qp_in, kp_in, qr_in, kr_in, v_in, o_in, stat_in, raw_a_in, h_in, gate_in, up_in, act_in, raw_f_in,
    x_in, cot_in, mask, cos_ref, sin_ref, seg_col, seg_row, q_gain, k_gain, a_gain, f_gain,
    units_out, raw_h_out, raw_x_out, gains_out,
    wg, wu, wd,
    qp, kp, qr, kr, v, o, stat, h, gate, up, act, d_ffn,
    cot, part, took, raw_h, turned, d_heads, dqn, dkn, dk_sum, dv_sum, sums, gains, gains_got,
    give, got, sum_a, sum_b, got_a, got_b, end_a, end_b, done,
    s_sems, s_out, sum_h, sum_x, small, gain_sems, load_sems, out_sems,
):
    place = Place(n_mp)
    rows, width = cot.shape
    local = qp.shape[1]
    ff = gate.shape[1]
    heads = local // HD
    scale = 1.0 / math.sqrt(HD)
    loads = {}

    def load(name, src, dst):
        copy = pltpu.make_async_copy(src, dst, load_sems.at[len(loads)])
        loads[name] = copy
        copy.start()

    def need(*names):
        for name in names:
            loads[name].wait()

    load("raw_f", raw_f_in, d_ffn)
    load("cot", cot_in, cot)
    load("act", act_in, act)
    load("wd", wd_in, wd)
    load("gate", gate_in, gate)
    load("up", up_in, up)
    load("wg", wg_in, wg)
    load("wu", wu_in, wu)
    load("h", h_in, h)
    for name, src, dst in (
        ("o", o_in, o), ("qr", qr_in, qr), ("kr", kr_in, kr), ("v", v_in, v),
        ("stat", stat_in, stat), ("qp", qp_in, qp), ("kp", kp_in, kp),
    ):
        load(name, src, dst)
    place.barrier()
    tile = rows // 8
    gains[...] = jnp.zeros(gains.shape, F32)

    def row_tile(at):
        return pl.ds(pl.multiple_of(at * tile, tile), tile)

    def back_ffn(at, carry):
        near = row_tile(at)
        raw = d_ffn[near, :].astype(F32)
        dy = mask[near, :] * cot[near, :].astype(F32)
        inv = lax.rsqrt(jnp.mean(raw * raw, axis=1, keepdims=True) + EPS)
        gains[0:1, :] += jnp.sum(dy * raw * inv, axis=0, keepdims=True)
        gained = f_gain[...] * dy
        mean = jnp.mean(gained * raw, axis=1, keepdims=True)
        d_ffn[near, :] = (inv * gained - raw * inv**3 * mean).astype(BF)
        return carry

    need("raw_f", "cot")
    lax.fori_loop(0, 8, back_ffn, 0)

    def flip(src):
        def one(at, carry):
            near = pl.ds(pl.multiple_of(at * UNIT, UNIT), UNIT)
            turned[near, :] = src[:, near].T
            return carry

        lax.fori_loop(0, width // UNIT, one, 0)

    scatter = Scatter(place, units_out, give, got, sum_a, sum_b, got_a, got_b, end_a, end_b, done, s_sems, s_out,
                      (3 * ff + 4 * local) // UNIT)
    flip(d_ffn)
    need("act", "wd", "gate", "up")

    def cols_of(at):
        return slice(at * UNIT, (at + 1) * UNIT)

    def back_act(at, carry):
        cols = pl.ds(pl.multiple_of(at * UNIT, UNIT), UNIT)
        d_act = dot_nt(d_ffn[...], wd[cols, :])
        pre, upper = gate[:, cols].astype(F32), up[:, cols].astype(F32)
        sig = jax.nn.sigmoid(pre)
        up[:, cols] = (d_act * pre * sig).astype(BF)
        gate[:, cols] = (d_act * upper * sig * (1.0 + pre * (1.0 - sig))).astype(BF)
        return carry

    n_ff = ff // UNIT
    for at in range(n_ff // 2):
        scatter.tick(turned, act, cols_of(at))
        lax.fori_loop(2 * at, 2 * at + 2, back_act, 0)
    load("wq", wq_in, wd.at[:, 0:local])
    load("wk", wk_in, wd.at[:, local:2 * local])
    load("wv", wv_in, wd.at[:, 2 * local:3 * local])
    need("wg", "wu")
    sum_back = RowSum(place, part, took, raw_h, sum_h, place.order)
    step = width // 8

    def step_of(block):
        return pl.ds(pl.multiple_of(block * step, step), step)

    for at in range(8):
        spot = step_of(place.order[at])
        part[:, spot] = (dot_nt(gate[...], wg[spot, :]) + dot_nt(up[...], wu[spot, :])).astype(BF)
        sum_back.begin(at % 2, at // 2)
        if at % 2 == 1:
            scatter.tick(turned, act, cols_of(n_ff // 2 + at // 2))
    raw_a = act
    load("raw_a", raw_a_in, raw_a)
    need("h")
    flip(h)
    load("wo", wo_in, wg.at[0:local, :])
    load("x", x_in, wu.at[0:rows, :])
    queue = [(gate, at) for at in range(n_ff)] + [(up, at) for at in range(n_ff)]

    def more():
        right, at = queue.pop(0)
        scatter.tick(turned, right, cols_of(at))

    for tick in range(sum_back.ticks):
        sum_back.gather_steps(tick)
        more()
    for tick in range(sum_back.ticks):
        sum_back.return_steps(tick)
        if tick < sum_back.ticks - 1:
            more()
    sum_back.drain()
    raw_h_copy = pltpu.make_async_copy(raw_h, raw_h_out, out_sems.at[0])
    raw_h_copy.start()
    need("raw_a")
    d_attn = wu.at[rows:2 * rows, :]

    def back_attn(at, carry):
        near = row_tile(at)
        raw = raw_a[near, :].astype(F32)
        dh = mask[near, :] * cot[near, :].astype(F32) + raw_h[near, :].astype(F32)
        inv = lax.rsqrt(jnp.mean(raw * raw, axis=1, keepdims=True) + EPS)
        gains[1:2, :] += jnp.sum(dh * raw * inv, axis=0, keepdims=True)
        gained = a_gain[...] * dh
        mean = jnp.mean(gained * raw, axis=1, keepdims=True)
        d_attn[near, :] = (inv * gained - raw * inv**3 * mean).astype(BF)
        return carry

    lax.fori_loop(0, 8, back_attn, 0)
    need("wo", "o")
    d_heads[...] = dot_nt(d_attn[...], wg[0:local, :]).astype(BF)
    need("qr", "kr", "v", "stat", "qp", "kp")
    more()
    block = rows // 4
    dval = wu.at[2 * rows:3 * rows, 2 * local:3 * local]
    for hd in range(heads):
        cols = slice(hd * HD, (hd + 1) * HD)
        dk_sum[...] = jnp.zeros(dk_sum.shape, F32)
        dv_sum[...] = jnp.zeros(dv_sum.shape, F32)
        for rb in range(4):
            near = slice(rb * block, (rb + 1) * block)
            keys = (rb + 1) * block
            t_at = lax.broadcasted_iota(jnp.int32, (block, keys), 0) + rb * block
            s_at = lax.broadcasted_iota(jnp.int32, (block, keys), 1)
            allowed = (seg_col[near, :] == seg_row[:, 0:keys]) & (s_at <= t_at)
            scores = dot_nt(qr[near, cols], kr[0:keys, cols]) * scale
            probs = jnp.where(allowed, jnp.exp(jnp.where(allowed, scores, -1e30) - stat[near, hd:hd + 1]), 0.0)
            grad = d_heads[near, cols]
            d_prob = dot_nt(grad, v[0:keys, cols])
            delta = jnp.sum(grad.astype(F32) * o[near, cols].astype(F32), axis=1, keepdims=True)
            d_score = (probs * (d_prob - delta)).astype(BF)
            dqn[near, cols] = turn_back(
                dot(d_score, kr[0:keys, cols]) * scale, cos_ref[near, :], sin_ref[near, :])
            dk_sum[0:keys, :] += dot_tn(d_score, qr[near, cols])
            dv_sum[0:keys, :] += dot_tn(probs.astype(BF), grad)
        dkn[:, cols] = turn_back(dk_sum[...] * scale, cos_ref[...], sin_ref[...])
        dval[:, cols] = dv_sum[...].astype(BF)
        if hd % 2 == 1 and queue:
            more()
    inv_q, inv_k = stat[:, heads:heads + 1], stat[:, heads + 1:heads + 2]
    row_sum = SmallSum(place, sums, small)
    sums[0] = jnp.zeros(sums.shape[1:], F32)
    grad_q, grad_k = dqn[...], dkn[...]
    gains[2:3, 0:local] = jnp.sum(grad_q * qp[...] * inv_q, axis=0, keepdims=True)
    gains[3:4, 0:local] = jnp.sum(grad_k * kp[...] * inv_k, axis=0, keepdims=True)
    sums[0, 0:1, :] = as_row(jnp.sum(q_gain[...] * grad_q * qp[...], axis=1, keepdims=True))
    sums[0, 1:2, :] = as_row(jnp.sum(k_gain[...] * grad_k * kp[...], axis=1, keepdims=True))
    row_sum.begin()
    while queue:
        more()
    flip(d_attn)
    scatter.tick(turned, o, cols_of(0))
    totals = row_sum.end()
    mean_q, mean_k = as_col(totals[0:1, :]) / width, as_col(totals[1:2, :]) / width
    dq = wu.at[2 * rows:3 * rows, 0:local]
    dk = wu.at[2 * rows:3 * rows, local:2 * local]
    dq[...] = (inv_q * (q_gain[...] * dqn[...]) - qp[...] * inv_q**3 * mean_q).astype(BF)
    dk[...] = (inv_k * (k_gain[...] * dkn[...]) - kp[...] * inv_k**3 * mean_k).astype(BF)
    need("wq", "wk", "wv", "x")
    raw_x = d_ffn
    sum_in = RowSum(place, part, took, raw_x, sum_x, place.order)
    for at in range(8):
        spot = step_of(place.order[at])
        value = dot_nt(dq[...], wd[spot, 0:local]) + dot_nt(dk[...], wd[spot, local:2 * local])
        part[:, spot] = (value + dot_nt(dval[...], wd[spot, 2 * local:3 * local])).astype(BF)
        sum_in.begin(at % 2, at // 2)
    scatter.tick(turned, o, cols_of(1))
    flip(wu.at[0:rows, :])
    queue = [(right, at) for right in (dq, dk, dval) for at in range(local // UNIT)]
    for tick in range(sum_in.ticks):
        sum_in.gather_steps(tick)
        if queue:
            more()
        else:
            scatter.tick()
    partners = (place.sib, place.xn, place.yn)

    def gain_copy(at):
        return remote(gains.at[pl.ds(8 * at, 8), :], gains_got.at[at], gain_sems.at[0, at], gain_sems.at[1, at],
                      {"dp": partners[at]})

    gain_copy(0).start()
    for tick in range(sum_in.ticks):
        sum_in.return_steps(tick)
        if queue:
            more()
        elif scatter.unit < scatter.n_units + 3:
            scatter.tick()
        if tick < 3:
            gain_copy(tick).wait_recv()
            gains[8 * tick + 8:8 * tick + 16, :] = gains[8 * tick:8 * tick + 8, :] + gains_got[tick]
            if tick < 2:
                gain_copy(tick + 1).start()
    while scatter.unit < scatter.n_units + 3:
        scatter.tick()
    outs = [
        raw_h_copy,
        pltpu.make_async_copy(raw_x, raw_x_out, out_sems.at[1]),
        pltpu.make_async_copy(gains.at[24:32, :], gains_out, out_sems.at[2]),
    ]
    outs[1].start()
    outs[2].start()
    for at in range(3):
        gain_copy(at).wait_send()
    sum_in.drain()
    row_sum.drain()
    scatter.drain()
    for copy in outs:
        copy.wait()


def backward_call(n_mp, saved, x, cot, mask, cos_tab, sin_tab, seg_col, seg_row, q_gain, k_gain, a_gain, f_gain):
    rows, width = x.shape
    local = saved[0].shape[1]
    ff = saved[4].shape[1]
    any_spec = pl.BlockSpec(memory_space=pl.ANY)
    vmem = pl.BlockSpec(memory_space=pltpu.VMEM)
    S = jax.ShapeDtypeStruct
    V = pltpu.VMEM
    dma = pltpu.SemaphoreType.DMA
    n_units = (3 * ff + 4 * local) // UNIT
    high = width // 8
    return pl.pallas_call(
        functools.partial(backward_kernel, n_mp),
        out_shape=[S((n_units, high, UNIT), F32), S((rows, width), BF), S((rows, width), BF), S((8, width), F32)],
        in_specs=[any_spec] * 22 + [vmem] * 9,
        out_specs=[any_spec] * 4,
        scratch_shapes=[
            V((width, ff), BF), V((width, ff), BF), V((ff, width), BF),
            V((rows, local), F32), V((rows, local), F32), V((rows, local), BF), V((rows, local), BF),
            V((rows, local), BF), V((rows, local), BF), V((rows, 128), F32),
            V((rows, width), BF), V((rows, ff), BF), V((rows, ff), BF), V((rows, ff), BF), V((rows, width), BF),
            V((rows, width), BF), V((rows, width), BF), V((2, 4, rows, width // 8), BF), V((rows, width), BF),
            V((width, rows), BF), V((rows, local), BF), V((rows, local), F32), V((rows, local), F32),
            V((rows, HD), F32), V((rows, HD), F32), V((n_mp, 8, rows), F32), V((32, width), F32), V((3, 8, width), F32),
            V((2, 4, high, UNIT), BF), V((4, 4, high, UNIT), BF),
            V((4, 2, 2, high // 2, UNIT), BF), V((4, 2, 2, high // 2, UNIT), BF),
            V((4, 2, high // 2, UNIT), BF), V((4, 2, high // 2, UNIT), BF),
            V((4, high // 2, UNIT), BF), V((4, high // 2, UNIT), BF), V((2, high, UNIT), F32),
            dma((2, 5, 4)), dma((2,)), dma((4, 2, 4)), dma((4, 2, 4)), dma((2, n_mp)), dma((2, 3)), dma((24,)), dma((3,)),
        ],
        compiler_params=pltpu.CompilerParams(
            collective_id=1, has_side_effects=True, vmem_limit_bytes=67043328,
        ),
    )(*saved, x, cot, mask, cos_tab, sin_tab, seg_col, seg_row, q_gain, k_gain, a_gain, f_gain)


def doc_positions(seg_row):
    row_count = seg_row.shape[0]
    row_index = jnp.arange(row_count, dtype=jnp.int32)
    change = jnp.concatenate([jnp.ones((1,), dtype=bool), seg_row[1:] != seg_row[:-1]])
    doc_start = lax.cummax(jnp.where(change, row_index, jnp.zeros_like(row_index)), axis=0)
    return (row_index - doc_start).astype(jnp.float32)


def rotary_tables(positions, head_size):
    half_size = head_size // 2
    inv_freq = THETA ** (-(jnp.arange(half_size, dtype=jnp.float32) * (2.0 / head_size)))
    angles = positions[:, None] * inv_freq[None, :]
    return (jnp.cos(angles)[:, None, :], jnp.sin(angles)[:, None, :])


def rotate(values, cos_tab, sin_tab):
    half_size = values.shape[2] // 2
    first_half = values[:, :, :half_size]
    second_half = values[:, :, half_size:]
    return jnp.concatenate(
        [
            first_half * cos_tab - second_half * sin_tab,
            second_half * cos_tab + first_half * sin_tab,
        ],
        axis=2,
    )


def rotate_back(grads, cos_tab, sin_tab):
    half_size = grads.shape[2] // 2
    first_half = grads[:, :, :half_size]
    second_half = grads[:, :, half_size:]
    return jnp.concatenate(
        [
            first_half * cos_tab + second_half * sin_tab,
            second_half * cos_tab - first_half * sin_tab,
        ],
        axis=2,
    )


def block_mask(seg_row, offset, block_rows):
    row_index = jnp.arange(seg_row.shape[0])
    same = seg_row[offset : offset + block_rows, None] == seg_row[None, :]
    return same & (row_index[:, None] >= row_index[None, :])


def block_scores(q_blk, k_bf, allowed, score_scale):
    scores = (
        jnp.einsum("qhe,khe->hqk", q_blk, k_bf, preferred_element_type=jnp.float32) * score_scale
    )
    return jnp.where(allowed[None], scores, jnp.float32(-1e30))


def attend_forward(q_bf, k_bf, v_bf, seg_row, score_scale):
    row_count = q_bf.shape[0]
    block_rows = min(512, row_count)
    allowed = block_mask(seg_row, 0, block_rows)
    scores = block_scores(q_bf, k_bf, allowed, score_scale)
    row_max = jnp.max(scores, axis=2, keepdims=True)
    lse = row_max + jnp.log(jnp.sum(jnp.exp(scores - row_max), axis=2, keepdims=True))
    probs = jnp.exp(scores - lse).astype(jnp.bfloat16)
    outputs = jnp.einsum("hqk,khe->qhe", probs, v_bf, preferred_element_type=jnp.float32)
    lse_parts = [lse]
    return (outputs.astype(jnp.bfloat16), lse_parts)


def attend_backward(q_bf, k_bf, v_bf, o_bf, do_bf, lse_parts, seg_row, score_scale):
    row_count = q_bf.shape[0]
    block_rows = min(512, row_count)
    dq_parts = []
    dk_acc = jnp.zeros(k_bf.shape, jnp.float32)
    dv_acc = jnp.zeros(v_bf.shape, jnp.float32)
    for part_index, offset in enumerate(range(0, row_count, block_rows)):
        allowed = block_mask(seg_row, offset, block_rows)
        scores = block_scores(q_bf, k_bf, allowed, score_scale)
        probs = jnp.exp(scores - lse_parts[part_index])
        probs_bf = probs.astype(jnp.bfloat16)
        dprob = jnp.einsum("qhe,khe->hqk", do_bf, v_bf, preferred_element_type=jnp.float32)
        delta = jnp.transpose(
            jnp.sum(do_bf.astype(jnp.float32) * o_bf.astype(jnp.float32), axis=2)
        )[:, :, None]
        dscore = (probs * (dprob - delta)).astype(jnp.bfloat16)
        dq_parts.append(
            jnp.einsum("hqk,khe->qhe", dscore, k_bf, preferred_element_type=jnp.float32)
            * score_scale
        )
        dk_acc = (
            jnp.einsum("hqk,qhe->khe", dscore, q_bf, preferred_element_type=jnp.float32)
            * score_scale
        )
        dv_acc = jnp.einsum("hqk,qhe->khe", probs_bf, do_bf, preferred_element_type=jnp.float32)
    return (dq_parts[0], dk_acc, dv_acc.astype(jnp.bfloat16))


def scatter_grad(grad, axis_name, scatter_dimension, tiled):
    total = lax.psum_scatter(
        grad.astype(jnp.bfloat16), axis_name, scatter_dimension=scatter_dimension, tiled=tiled
    )
    return total.astype(jnp.float32)


def sum_parts(part, axis_name):
    own = lax.psum_scatter(
        part.astype(jnp.bfloat16), axis_name, scatter_dimension=0, tiled=True
    )
    return lax.all_gather(own, axis_name, axis=0, tiled=True).astype(jnp.float32)


def norm_back(raw, inv_scale, gained, row_sums, width):
    return inv_scale * gained - raw * inv_scale**3 * (row_sums[:, None] / width)


def on_device(
    hidden_in,
    cotangent,
    segments,
    live_counts,
    w_query,
    w_key,
    w_value,
    w_output,
    w_gate,
    w_up,
    w_down,
    query_gain,
    key_gain,
    attn_gain,
    ffn_gain,
):
    gathered = (
        lax.all_gather(w_query, "dp", axis=0, tiled=True),
        lax.all_gather(w_key, "dp", axis=0, tiled=True),
        lax.all_gather(w_value, "dp", axis=0, tiled=True),
        lax.all_gather(w_output, "dp", axis=1, tiled=True),
        lax.all_gather(w_gate, "dp", axis=0, tiled=True),
        lax.all_gather(w_up, "dp", axis=0, tiled=True),
        lax.all_gather(w_down, "dp", axis=1, tiled=True),
    )
    wq_full, wk_full, wv_full, wo_full, wg_full, wu_full, wd_full = gathered
    seg_row = segments[0]
    live_n = live_counts[0]
    row_count, width = hidden_in.shape
    local_width = wq_full.shape[1]
    heads_here = local_width // HD
    score_scale = 1.0 / math.sqrt(HD)
    live_mask = (jnp.arange(row_count, dtype=jnp.int32) < live_n).astype(jnp.float32)[:, None]
    cos_tab, sin_tab = rotary_tables(doc_positions(seg_row), HD)
    q_proj = jnp.dot(hidden_in, wq_full, preferred_element_type=jnp.float32)
    k_proj = jnp.dot(hidden_in, wk_full, preferred_element_type=jnp.float32)
    v_bf = jnp.dot(hidden_in, wv_full, preferred_element_type=jnp.float32).astype(jnp.bfloat16)
    sq_query, sq_key = lax.psum(
        (jnp.sum(q_proj * q_proj, axis=1), jnp.sum(k_proj * k_proj, axis=1)), "mp"
    )
    inv_q = lax.rsqrt(sq_query[:, None] / width + EPS)
    inv_k = lax.rsqrt(sq_key[:, None] / width + EPS)
    q_rot = rotate(
        (q_proj * inv_q * query_gain).reshape(row_count, heads_here, HD), cos_tab, sin_tab
    ).astype(jnp.bfloat16)
    k_rot = rotate(
        (k_proj * inv_k * key_gain).reshape(row_count, heads_here, HD), cos_tab, sin_tab
    ).astype(jnp.bfloat16)
    v_heads = v_bf.reshape(row_count, heads_here, HD)
    o_bf, lse_parts = attend_forward(q_rot, k_rot, v_heads, seg_row, score_scale)
    o_flat = o_bf.reshape(row_count, local_width)
    attn_raw = sum_parts(jnp.dot(o_flat, wo_full, preferred_element_type=jnp.float32), "mp")
    inv_a = lax.rsqrt(jnp.mean(attn_raw * attn_raw, axis=1, keepdims=True) + EPS)
    h_mid = hidden_in.astype(jnp.float32) + attn_raw * inv_a * attn_gain
    h_bf = h_mid.astype(jnp.bfloat16)
    gate_pre = jnp.dot(h_bf, wg_full, preferred_element_type=jnp.float32)
    up_pre = jnp.dot(h_bf, wu_full, preferred_element_type=jnp.float32)
    act_bf = (jax.nn.silu(gate_pre) * up_pre).astype(jnp.bfloat16)
    ffn_raw = sum_parts(jnp.dot(act_bf, wd_full, preferred_element_type=jnp.float32), "mp")
    inv_f = lax.rsqrt(jnp.mean(ffn_raw * ffn_raw, axis=1, keepdims=True) + EPS)
    hidden_out = (live_mask * (h_mid + ffn_raw * inv_f * ffn_gain)).astype(jnp.bfloat16)
    wq_back, wk_back, wv_back, wo_back, wg_back, wu_back, wd_back = gathered
    dy = live_mask * cotangent.astype(jnp.float32)
    g_ffn_gain = jnp.sum(dy * ffn_raw * inv_f, axis=0)
    gained_f = ffn_gain * dy
    d_ffn = norm_back(ffn_raw, inv_f, gained_f, jnp.sum(gained_f * ffn_raw, axis=1), width).astype(
        jnp.bfloat16
    )
    d_act = jnp.dot(d_ffn, wd_back.T, preferred_element_type=jnp.float32)
    sig = jax.nn.sigmoid(gate_pre)
    d_up = (d_act * gate_pre * sig).astype(jnp.bfloat16)
    d_gate = (d_act * up_pre * sig * (1.0 + gate_pre * (1.0 - sig))).astype(jnp.bfloat16)
    ffn_part = jnp.dot(d_gate, wg_back.T, preferred_element_type=jnp.float32) + jnp.dot(
        d_up, wu_back.T, preferred_element_type=jnp.float32
    )
    dh = dy + sum_parts(ffn_part, "mp")
    g_down = jnp.dot(act_bf.T, d_ffn, preferred_element_type=jnp.float32)
    g_gate = jnp.dot(h_bf.T, d_gate, preferred_element_type=jnp.float32)
    g_up = jnp.dot(h_bf.T, d_up, preferred_element_type=jnp.float32)
    g_attn_gain = jnp.sum(dh * attn_raw * inv_a, axis=0)
    gained_a = attn_gain * dh
    d_attn = norm_back(
        attn_raw, inv_a, gained_a, jnp.sum(gained_a * attn_raw, axis=1), width
    ).astype(jnp.bfloat16)
    d_heads = jnp.dot(d_attn, wo_back.T, preferred_element_type=jnp.float32).astype(jnp.bfloat16)
    g_output = jnp.dot(o_flat.T, d_attn, preferred_element_type=jnp.float32)
    dq_rot, dk_rot, d_val = attend_backward(
        q_rot,
        k_rot,
        v_heads,
        o_bf,
        d_heads.reshape(row_count, heads_here, HD),
        lse_parts,
        seg_row,
        score_scale,
    )
    dq_norm = rotate_back(dq_rot, cos_tab, sin_tab).reshape(row_count, local_width)
    dk_norm = rotate_back(dk_rot, cos_tab, sin_tab).reshape(row_count, local_width)
    g_query_gain = jnp.sum(dq_norm * q_proj * inv_q, axis=0)
    g_key_gain = jnp.sum(dk_norm * k_proj * inv_k, axis=0)
    gained_q = query_gain * dq_norm
    gained_k = key_gain * dk_norm
    sums_query, sums_key = lax.psum(
        (jnp.sum(gained_q * q_proj, axis=1), jnp.sum(gained_k * k_proj, axis=1)), "mp"
    )
    dq_bf = norm_back(q_proj, inv_q, gained_q, sums_query, width).astype(jnp.bfloat16)
    dk_bf = norm_back(k_proj, inv_k, gained_k, sums_key, width).astype(jnp.bfloat16)
    dv_bf = d_val.reshape(row_count, local_width)
    input_part = (
        jnp.dot(dq_bf, wq_back.T, preferred_element_type=jnp.float32)
        + jnp.dot(dk_bf, wk_back.T, preferred_element_type=jnp.float32)
        + jnp.dot(dv_bf, wv_back.T, preferred_element_type=jnp.float32)
    )
    grad_in = dh + sum_parts(input_part, "mp")
    g_query = jnp.dot(hidden_in.T, dq_bf, preferred_element_type=jnp.float32)
    g_key = jnp.dot(hidden_in.T, dk_bf, preferred_element_type=jnp.float32)
    g_value = jnp.dot(hidden_in.T, dv_bf, preferred_element_type=jnp.float32)
    owned = (
        scatter_grad(g_query, "dp", scatter_dimension=0, tiled=True),
        scatter_grad(g_key, "dp", scatter_dimension=0, tiled=True),
        scatter_grad(g_value, "dp", scatter_dimension=0, tiled=True),
        scatter_grad(g_output, "dp", scatter_dimension=1, tiled=True),
        scatter_grad(g_gate, "dp", scatter_dimension=0, tiled=True),
        scatter_grad(g_up, "dp", scatter_dimension=0, tiled=True),
        scatter_grad(g_down, "dp", scatter_dimension=1, tiled=True),
    )
    gain_totals = lax.psum((g_query_gain, g_key_gain, g_attn_gain, g_ffn_gain), "dp")
    return (
        hidden_out,
        grad_in,
        owned[0],
        owned[1],
        owned[2],
        owned[3],
        owned[4],
        owned[5],
        owned[6],
        gain_totals[0],
        gain_totals[1],
        gain_totals[2],
        gain_totals[3],
    )


def with_kernels(n_mp, hidden_in, cotangent, segments, live_counts, *rest):
    weights, (query_gain, key_gain, attn_gain, ffn_gain) = rest[:7], rest[7:]
    seg = segments[0]
    rows = hidden_in.shape[0]
    local, ff = weights[0].shape[1], weights[4].shape[1]
    cos_tab, sin_tab = (tab[:, 0] for tab in rotary_tables(doc_positions(seg), HD))
    cos_tab = jnp.concatenate([cos_tab, cos_tab], axis=1)
    sin_tab = jnp.concatenate([-sin_tab, sin_tab], axis=1)
    mask = (jnp.arange(rows, dtype=jnp.int32) < live_counts[0]).astype(F32)[:, None]
    common = (
        cos_tab, sin_tab, seg[:, None], seg[None, :], query_gain[None], key_gain[None], attn_gain[None]
    )
    saved = forward_call(n_mp, hidden_in, weights, *common)
    units, raw_h, raw_x, gains = backward_call(
        n_mp, saved, hidden_in, cotangent, mask, *common, ffn_gain[None]
    )
    raw_a, raw_f = saved[14].astype(F32), saved[19].astype(F32)
    inv_a = lax.rsqrt(jnp.mean(raw_a * raw_a, axis=1, keepdims=True) + EPS)
    inv_f = lax.rsqrt(jnp.mean(raw_f * raw_f, axis=1, keepdims=True) + EPS)
    h_mid = hidden_in.astype(F32) + raw_a * inv_a * attn_gain
    hidden_out = (mask * (h_mid + raw_f * inv_f * ffn_gain)).astype(BF)
    grad_in = mask * cotangent.astype(F32) + raw_h.astype(F32) + raw_x.astype(F32)
    n_ff, n_local = ff // UNIT, local // UNIT
    high = units.shape[1]

    def side(first, count):
        return jnp.transpose(units[first:first + count], (1, 0, 2)).reshape(high, count * UNIT)

    def down(first, count):
        return jnp.transpose(units[first:first + count], (0, 2, 1)).reshape(count * UNIT, high)

    at = 3 * n_ff
    return (
        hidden_out,
        grad_in,
        side(at + n_local, n_local),
        side(at + 2 * n_local, n_local),
        side(at + 3 * n_local, n_local),
        down(at, n_local),
        side(n_ff, n_ff),
        side(2 * n_ff, n_ff),
        down(0, n_ff),
        gains[2, :local],
        gains[3, :local],
        gains[1],
        gains[0],
    )


def kernels_fit(mesh, hidden_in, segments, w_query, w_gate):
    n_dp, n_mp = mesh.shape["dp"], mesh.shape["mp"]
    rows, width = hidden_in.shape[0] // n_dp, hidden_in.shape[1]
    local, ff = w_query.shape[1] // n_mp, w_gate.shape[1] // n_mp
    even = width % (8 * UNIT) == 0 and local % UNIT == 0 and ff % (2 * UNIT) == 0
    fits = rows == UNIT * 2 and width == 8 * UNIT and local == rows and ff == width
    return n_dp == 8 and n_mp >= 2 and even and fits


def solution(mesh):
    in_specs = (
        P("dp", None),
        P("dp", None),
        P("dp", None),
        P("dp"),
        P("dp", "mp"),
        P("dp", "mp"),
        P("dp", "mp"),
        P("mp", "dp"),
        P("dp", "mp"),
        P("dp", "mp"),
        P("mp", "dp"),
        P("mp"),
        P("mp"),
        P(),
        P(),
    )
    out_specs = (
        P("dp", None),
        P("dp", None),
        P("dp", "mp"),
        P("dp", "mp"),
        P("dp", "mp"),
        P("mp", "dp"),
        P("dp", "mp"),
        P("dp", "mp"),
        P("mp", "dp"),
        P("mp"),
        P("mp"),
        P(),
        P(),
    )

    def step(*args):
        if kernels_fit(mesh, args[0], args[2], args[4], args[8]):
            body = functools.partial(with_kernels, mesh.shape["mp"])
        else:
            body = on_device
        return jax.shard_map(
            body, mesh=mesh, in_specs=in_specs, out_specs=out_specs, check_vma=False
        )(*args)

    return step
```

```python
import functools
import math

import jax
import jax.numpy as jnp
from jax import lax
from jax.experimental import pallas as pl
from jax.experimental.pallas import tpu as pltpu
from jax.sharding import PartitionSpec as P

HD = 128
EPS = 1e-06
THETA = 500000.0
UNIT = 256
BF = jnp.bfloat16
F32 = jnp.float32


def dot(a, b):
    return jnp.dot(a, b, preferred_element_type=F32)


def dot_nt(a, b):
    return lax.dot_general(a, b, (((1,), (1,)), ((), ())), preferred_element_type=F32)


def dot_tn(a, b):
    return lax.dot_general(a, b, (((0,), (0,)), ((), ())), preferred_element_type=F32)


def span(start, size):
    return pl.ds(start if isinstance(start, int) else pl.multiple_of(start, size), size)


def loop(count, body, first=0):
    def step(at, carry):
        body(at)
        return carry

    lax.fori_loop(first, first + count, step, 0)


def remote(src, dst, send, recv, device):
    return pltpu.make_async_remote_copy(
        src_ref=src, dst_ref=dst, send_sem=send, recv_sem=recv,
        device_id=device, device_id_type=pl.DeviceIdType.MESH,
    )


class Place:
    def __init__(self, n_mp):
        self.dp, self.z = lax.axis_index("dp"), lax.axis_index("mp")
        self.n_mp, self.end = n_mp, n_mp - 1
        self.c = lax.rem(self.dp, 2)
        self.x = lax.rem(self.dp // 2, 2)
        self.y = self.dp // 4
        self.sib, self.xn, self.yn, self.dg = (self.block(i) for i in (1, 2, 4, 6))

    def block(self, i):
        i0, i1, i2 = i % 2, (i // 2) % 2, i // 4
        c, x, y = (a + b - 2 * a * b for a, b in ((self.c, i0), (self.x, i1), (self.y, i2)))
        return 4 * y + 2 * x + c

    def barrier(self):
        sem = pltpu.get_barrier_semaphore()
        mesh = pl.DeviceIdType.MESH
        for dp in (self.sib, self.xn, self.yn):
            pl.semaphore_signal(sem, inc=1, device_id={"dp": dp}, device_id_type=mesh)
        for step in range(1, self.n_mp):
            z = lax.rem(self.z + step, self.n_mp)
            pl.semaphore_signal(sem, inc=1, device_id={"mp": z}, device_id_type=mesh)
        pl.semaphore_wait(sem, 3 + self.n_mp - 1)


class Gather:
    def __init__(self, place, src, full, by_rows, send, recv, local):
        self.place, self.src, self.full, self.by_rows = place, src, full, by_rows
        self.sends, self.recvs, self.local = send, recv, local
        self.rows, self.cols = src.shape
        self.half = self.rows // 2

    def spot(self, owner, part=None):
        first, count = (0, self.rows) if part is None else (part * self.half, self.half)
        if self.by_rows:
            start = pl.multiple_of(owner * self.rows + first, self.half)
            return self.full.at[pl.ds(start, count), :]
        return self.full.at[pl.ds(first, count), span(owner * self.cols, self.cols)]

    def copies(self):
        p = self.place
        halves = [self.src.at[pl.ds(part * self.half, self.half), :] for part in range(2)]
        return {
            0: (halves[0], p.dp, 0, p.xn, p.xn),
            1: (halves[1], p.dp, 1, p.xn, p.xn),
            2: (halves[0], p.dp, 0, p.yn, p.yn),
            3: (halves[1], p.dp, 1, p.yn, p.yn),
            4: (self.spot(p.yn, 1), p.yn, 1, p.xn, p.dg),
            5: (self.spot(p.xn, 0), p.xn, 0, p.yn, p.dg),
            6: (self.src, p.dp, None, p.sib, p.sib),
            7: (self.spot(p.xn), p.xn, None, p.sib, p.block(3)),
            8: (self.spot(p.yn), p.yn, None, p.sib, p.block(5)),
            9: (self.spot(p.dg), p.dg, None, p.sib, p.block(7)),
        }

    def copy(self, kind):
        src, owner, part, target, _ = self.copies()[kind]
        return remote(src, self.spot(owner, part), self.sends.at[kind], self.recvs.at[kind], {"dp": target})

    def start(self, *kinds):
        for kind in kinds:
            self.copy(kind).start()

    def arrived(self, *kinds):
        for kind in kinds:
            _, _, part, target, owner = self.copies()[kind]
            spot = self.spot(owner, part)
            remote(spot, spot, self.sends.at[kind], self.recvs.at[kind], {"dp": target}).wait_recv()

    def own_copy(self):
        return pltpu.make_async_copy(self.src, self.spot(self.place.dp), self.local)

    def begin_a(self):
        self.start(0, 3)

    def begin_b(self):
        self.start(1, 2, 6)
        self.own_copy().start()

    def relay(self):
        self.arrived(0)
        self.start(5)
        self.arrived(3)
        self.start(4)

    def pass_on(self):
        self.arrived(1)
        self.start(7)
        self.arrived(2)
        self.start(8)

    def last(self):
        self.arrived(5, 4)
        self.start(9)

    def ready(self):
        self.own_copy().wait()
        self.arrived(6, 7, 8, 9)

    def drain(self):
        for kind in range(10):
            self.copy(kind).wait_send()


class RowSum:
    def __init__(self, place, part, took, total, sems, chunk_at):
        self.place, self.part, self.took, self.total, self.sems = place, part, took, total, sems
        self.chunk_at = chunk_at
        self.count, self.high, self.wide = took.shape[1:]
        self.ticks = self.count + 2 * place.end

    def spot(self, ref, flow, k):
        half, bits = self.chunk_at(2 * k + flow)
        return ref.at[span(half * self.high, self.high), span(self.place.block(bits) * self.wide, self.wide)]

    def at(self, flow):
        return self.place.z + flow * (self.place.end - 2 * self.place.z)

    def forth(self, flow, k):
        return remote(
            self.spot(self.part, flow, k), self.took.at[flow, k],
            self.sems.at[0, flow, k], self.sems.at[1, flow, k], {"mp": self.place.z + 1 - 2 * flow},
        )

    def back(self, flow, k):
        spot = self.spot(self.total, flow, k)
        return remote(spot, spot, self.sems.at[2, flow, k], self.sems.at[3, flow, k], {"mp": self.place.z - 1 + 2 * flow})

    def begin(self, chunk):
        flow, k = chunk % 2, chunk // 2

        @pl.when(self.at(flow) == 0)
        def _():
            self.forth(flow, k).start()

    def add(self, dst, flow, k):
        mine, to = self.spot(self.part, flow, k), self.spot(dst, flow, k)
        step = self.high // 4

        def one(at):
            near = span(at * step, step)
            to[near, :] = (mine[near, :].astype(F32) + self.took[flow, k, near, :].astype(F32)).astype(BF)

        loop(4, one)

    def tick(self, t):
        end = self.place.end
        for flow in range(2):
            at = self.at(flow)
            k = t - at

            @pl.when((at > 0) & (k >= 0) & (k < self.count))
            def _():
                self.forth(flow, k).wait_recv()

                @pl.when(at < end)
                def _():
                    self.add(self.part, flow, k)
                    self.forth(flow, k).start()

                @pl.when(at == end)
                def _():
                    self.add(self.total, flow, k)
                    self.back(flow, k).start()

        for flow in range(2):
            at = self.at(flow)
            k = t - 2 * end + at

            @pl.when((at < end) & (k >= 0) & (k < self.count))
            def _():
                self.back(flow, k).wait_recv()

                @pl.when(at > 0)
                def _():
                    self.back(flow, k).start()

    def drain(self):
        for flow in range(2):
            at = self.at(flow)

            def one(k):
                @pl.when(at < self.place.end)
                def _():
                    self.forth(flow, k).wait_send()

                @pl.when(at > 0)
                def _():
                    self.back(flow, k).wait_send()

            loop(self.count, one)


class SmallSum:
    def __init__(self, place, slots, sems):
        self.place, self.slots, self.sems = place, slots, sems

    def copy(self, step):
        p = self.place
        return remote(
            self.slots.at[0], self.slots.at[step], self.sems.at[0, step], self.sems.at[1, step],
            {"mp": lax.rem(p.z + step, p.n_mp)},
        )

    def begin(self):
        for step in range(1, self.place.n_mp):
            self.copy(step).start()

    def end(self):
        for step in range(1, self.place.n_mp):
            self.copy(step).wait_recv()
        total = self.slots[0]
        for step in range(1, self.place.n_mp):
            total = total + self.slots[step]
        return total

    def drain(self):
        for step in range(1, self.place.n_mp):
            self.copy(step).wait_send()


class Scatter:
    def __init__(self, place, pool, outs, sems, out_sems, count):
        self.place, self.pool, self.outs, self.count = place, pool, outs, count
        self.sems, self.out_sems = sems, out_sems
        self.rows = pool[0].shape[0] // 8
        self.half = self.rows // 2

    def column(self, array, at, start, size):
        return self.pool[array].at[span(start, size), pl.ds(at, UNIT)]

    def give(self, u, chip=None):
        first = (u % 2) * 4 * self.rows
        if chip is None:
            return self.column(0, 0, first, 4 * self.rows)
        return self.column(0, 0, first + chip * self.rows, self.rows)

    def got(self, u, chip=None):
        s = u % 4
        first, size = (s % 2) * 4 * self.rows, 4 * self.rows
        if chip is not None:
            first, size = first + chip * self.rows, self.rows
        at = s // 2 * UNIT
        return self.pool[1].at[span(first, size), pl.ds(at if isinstance(at, int) else pl.multiple_of(at, UNIT), UNIT)]

    def sums(self, which, u, to, then=None):
        first, size = (u % 4) * 2 * self.rows + to * self.rows, self.rows
        if then is not None:
            first, size = first + then * self.half, self.half
        return self.column(2, which * UNIT, first, size)

    def met(self, which, u):
        return self.column(0, UNIT, which * 4 * self.rows + (u % 4) * self.rows, self.rows)

    def ended(self, which, u):
        return self.column(3, which * UNIT, (u % 4) * self.half, self.half)

    def done(self, u):
        return self.column(3, 2 * UNIT, (u % 2) * self.rows, self.rows)

    def send(self, kind, u):
        p, s = self.place, u % 4
        src, dst, target = {
            0: lambda: (self.give(u), self.got(u), p.sib),
            1: lambda: (self.sums(0, u, 1 - p.x), self.met(0, u), p.xn),
            2: lambda: (self.sums(1, u, 1 - p.y), self.met(1, u), p.yn),
            3: lambda: (self.sums(0, u, p.x, 1 - p.y), self.ended(0, u), p.yn),
            4: lambda: (self.sums(1, u, p.y, 1 - p.x), self.ended(1, u), p.xn),
        }[kind]()
        return remote(src, dst, self.sems.at[0, kind, s], self.sems.at[1, kind, s], {"dp": target})

    def write(self, u, flipped):
        flat, first = flipped
        at = (u - first) * UNIT
        if flat:
            target = self.outs[0].at[span(at, UNIT), :]
        else:
            target = self.outs[1].at[:, span(at, UNIT)]
        return pltpu.make_async_copy(self.done(u), target, self.out_sems.at[u % 2])

    def product(self, u, turned, right, at):
        p = self.place
        cols = span(at * UNIT, UNIT)

        def other(chip):
            near = span((2 * chip + 1 - p.c) * self.rows, self.rows)
            self.give(u, chip)[...] = dot(turned[near, :], right[:, cols]).astype(BF)

        loop(4, other)
        self.send(0, u).start()

        def own(chip):
            near = span((2 * chip + p.c) * self.rows, self.rows)
            value = dot(turned[near, :], right[:, cols]).astype(BF)
            y_to, x_to = chip // 2, chip % 2
            self.sums(0, u, x_to, y_to)[...] = value[:self.half]
            self.sums(1, u, y_to, x_to)[...] = value[self.half:]

        loop(4, own)

    def across(self, u):
        self.send(0, u).wait_recv()
        self.send(0, u).wait_send()

        def add(chip):
            y_to, x_to = chip // 2, chip % 2
            more = self.got(u, chip)
            for which, spot in ((0, self.sums(0, u, x_to, y_to)), (1, self.sums(1, u, y_to, x_to))):
                near = slice(which * self.half, (which + 1) * self.half)
                spot[...] = (spot[...].astype(F32) + more[near, :].astype(F32)).astype(BF)

        loop(4, add)
        self.send(1, u).start()
        self.send(2, u).start()

    def along(self, u):
        p = self.place
        for which, mine in ((0, p.x), (1, p.y)):
            self.send(1 + which, u).wait_recv()
            spot, more = self.sums(which, u, mine), self.met(which, u)
            spot[...] = (spot[...].astype(F32) + more[...].astype(F32)).astype(BF)
            self.send(3 + which, u).start()
        for kind in (1, 2):
            self.send(kind, u).wait_send()

    def finish(self, u, flipped):
        p = self.place
        if not isinstance(u, int) or u >= 2:
            pltpu.make_async_copy(self.done(u), self.done(u), self.out_sems.at[u % 2]).wait()
        parts = []
        for which, spot in ((0, self.sums(0, u, p.x, p.y)), (1, self.sums(1, u, p.y, p.x))):
            self.send(3 + which, u).wait_recv()
            parts.append(spot[...].astype(F32) + self.ended(which, u)[...].astype(F32))
        value = jnp.concatenate(parts, axis=0)
        self.done(u)[...] = (value.T if flipped[0] else value).astype(BF)
        self.write(u, flipped).start()
        for kind in (3, 4):
            self.send(kind, u).wait_send()

    def tick(self, u, flipped, turned=None, right=None, at=None):
        has = lambda lag: not isinstance(u, int) or 0 <= u - lag < self.count
        if right is not None:
            self.product(u, turned, right, at)
        if has(1):
            self.across(u - 1)
        if has(2):
            self.along(u - 2)
        if has(3):
            self.finish(u - 3, flipped)

    def drain(self):
        for u in (self.count - 2, self.count - 1):
            pltpu.make_async_copy(self.done(u), self.done(u), self.out_sems.at[u % 2]).wait()


def as_row(col):
    n = col.shape[0]
    r = lax.broadcasted_iota(jnp.int32, (n, n), 0)
    s = lax.broadcasted_iota(jnp.int32, (n, n), 1)
    return jnp.sum(jnp.where(r == s, col, 0.0), axis=0, keepdims=True)


def as_col(row):
    n = row.shape[1]
    r = lax.broadcasted_iota(jnp.int32, (n, n), 0)
    s = lax.broadcasted_iota(jnp.int32, (n, n), 1)
    return jnp.sum(jnp.where(r == s, row, 0.0), axis=1, keepdims=True)


def turn(values, cos_tab, sin_tab):
    return values * cos_tab + pltpu.roll(values, HD // 2, 1) * sin_tab


def turn_back(grads, cos_tab, sin_tab):
    return grads * cos_tab - pltpu.roll(grads, HD // 2, 1) * sin_tab


def halves_in_turn(chunk):
    return chunk // 8, chunk % 8


def pairs_in_turn(chunk):
    return (chunk // 2) % 2, 2 * (chunk // 4) + chunk % 2


def layer_kernel(
    n_mp,
    x_in, cot_in, wq_in, wk_in, wv_in, wo_in, wg_in, wu_in, wd_in,
    seg, live, freq, q_gain, k_gain, a_gain, f_gain,
    wq_out, wk_out, wv_out, wo_out, hidden_out, grad_in_out, flat_out, tall_out, gains_out,
    wq, wk, wv, wo, wg, wu, wd,
    x, qp, kp, qr, kr, v, o, stat, cos_tab, sin_tab, side, raw_a, h, gate, up, act, d_ffn, cot, part, took,
    turned, dk_sum, dv_sum, sums, gains, gains_got,
    g_send, g_recv, g_local, row_sems, small, s_sems, s_out, gain_sems, io_sems,
):
    place = Place(n_mp)
    rows, width = x.shape
    local, ff = qp.shape[1], gate.shape[1]
    heads = local // HD
    scale = 1.0 / math.sqrt(HD)
    half = rows // 2
    n_ff = ff // UNIT
    flying = {}

    def move(name, src, dst):
        copy = pltpu.make_async_copy(src, dst, io_sems.at[len(flying)])
        flying[name] = copy
        copy.start()

    def need(*names):
        for name in names:
            flying[name].wait()

    move("x", x_in, x)
    place.barrier()
    gq, gk, gv, go, gg, gu, gd = [
        Gather(place, src, full, i not in (3, 6), g_send.at[i], g_recv.at[i], g_local.at[i])
        for i, (src, full) in enumerate(
            zip((wq_in, wk_in, wv_in, wo_in, wg_in, wu_in, wd_in), (wq, wk, wv, wo, wg, wu, wd))
        )
    ]
    gq.begin_a()
    gq.begin_b()
    gk.begin_a()
    gk.begin_b()
    move("cot", cot_in, cot)
    ids = seg[...].astype(F32)
    ids_col = as_col(ids)
    before = jnp.sum((ids < ids_col).astype(F32), axis=1, keepdims=True)
    row_at = lax.broadcasted_iota(jnp.int32, (rows, 1), 0)
    side[:, 0:1] = ids_col
    side[:, 1:2] = (row_at < live[...]).astype(F32)
    angles = (row_at.astype(F32) - before) * freq[...]
    cos_tab[...] = jnp.cos(angles)
    lane = lax.broadcasted_iota(jnp.int32, (rows, HD), 1)
    sin_tab[...] = jnp.sin(angles) * jnp.where(lane < HD // 2, -1.0, 1.0)
    gq.relay()
    gv.begin_a()
    gq.pass_on()
    gv.begin_b()
    gk.relay()
    go.begin_a()
    gk.pass_on()
    go.begin_b()
    gq.last()
    need("x")
    gq.ready()
    move("wq", wq, wq_out)
    row_sum = SmallSum(place, sums.at[0], small.at[0])

    def project(full, dst, squares_to=None):
        def one(r):
            near = span(r * half, half)
            value = dot(x[near, :], full[...])
            dst[near, :] = value.astype(BF)
            if squares_to is not None:
                stat[near, squares_to:squares_to + 1] = jnp.sum(value * value, axis=1, keepdims=True)

        loop(2, one)

    sums[0, 0] = jnp.zeros(sums.shape[2:], F32)
    project(wq, qp, heads)
    sums[0, 0, 0:1, :] = as_row(stat[:, heads:heads + 1])
    gv.relay()
    gk.last()
    gk.ready()
    move("wk", wk, wk_out)
    project(wk, kp, heads + 1)
    sums[0, 0, 1:2, :] = as_row(stat[:, heads + 1:heads + 2])
    row_sum.begin()
    gv.pass_on()
    go.relay()
    gg.begin_a()
    go.pass_on()
    gg.begin_b()
    gv.last()
    gv.ready()
    move("wv", wv, wv_out)
    project(wv, v)
    totals = row_sum.end()
    inv_q = lax.rsqrt(as_col(totals[0:1, :]) / width + EPS)
    inv_k = lax.rsqrt(as_col(totals[1:2, :]) / width + EPS)
    stat[:, heads:heads + 1] = inv_q
    stat[:, heads + 1:heads + 2] = inv_k

    def rotate_head(hd):
        cols = span(hd * HD, HD)
        qr[:, cols] = turn(qp[:, cols].astype(F32) * inv_q * q_gain[:, cols], cos_tab[...], sin_tab[...]).astype(BF)
        kr[:, cols] = turn(kp[:, cols].astype(F32) * inv_k * k_gain[:, cols], cos_tab[...], sin_tab[...]).astype(BF)

    loop(heads, rotate_head)
    block = rows // 4
    lane_at = lax.broadcasted_iota(jnp.int32, (block, HD), 1)

    def allowed_at(rb):
        near, keys = slice(rb * block, (rb + 1) * block), (rb + 1) * block
        t_at = lax.broadcasted_iota(jnp.int32, (block, keys), 0) + rb * block
        s_at = lax.broadcasted_iota(jnp.int32, (block, keys), 1)
        return near, keys, (side[near, 0:1] == seg[:, 0:keys].astype(F32)) & (s_at <= t_at)

    def attend(rb):
        near, keys, allowed = allowed_at(rb)

        def one(hd):
            cols = span(hd * HD, HD)
            scores = jnp.where(allowed, dot_nt(qr[near, cols], kr[0:keys, cols]) * scale, -1e30)
            top = jnp.max(scores, axis=1, keepdims=True)
            weights = jnp.exp(scores - top)
            norm = jnp.sum(weights, axis=1, keepdims=True)
            stat[near, :] = jnp.where(lane_at == hd, top + jnp.log(norm), stat[near, :])
            o[near, cols] = dot((weights / norm).astype(BF), v[0:keys, cols]).astype(BF)

        loop(heads, one)

    wide = width // 8

    def columns(bits):
        return span(place.block(bits) * wide, wide)

    sum_attn = RowSum(place, part, took, raw_a, row_sems.at[0], halves_in_turn)

    def project_out(r):
        near = slice(r * half, (r + 1) * half)

        def one(i):
            part[near, columns(i)] = dot(o[near, :], wo[:, columns(i)]).astype(BF)
            sum_attn.begin(r * 8 + i)

        loop(8, one)

    attend(0)
    attend(1)
    go.last()
    go.ready()
    move("wo", wo, wo_out)
    project_out(0)
    gu.begin_a()
    attend(2)
    sum_attn.tick(0)
    attend(3)
    project_out(1)
    sum_attn.tick(1)
    gg.relay()
    gu.begin_b()
    sum_attn.tick(2)
    sum_attn.tick(3)
    gg.pass_on()
    sum_attn.tick(4)
    sum_attn.tick(5)
    gu.relay()
    gd.begin_a()
    sum_attn.tick(6)
    sum_attn.tick(7)
    gg.last()
    gd.begin_b()
    sum_attn.tick(8)
    sum_attn.tick(9)

    def mid(r):
        tile = rows // 8

        def one(at):
            near = span(at * tile, tile)
            raw = raw_a[near, :].astype(F32)
            inv = lax.rsqrt(jnp.mean(raw * raw, axis=1, keepdims=True) + EPS)
            h[near, :] = (x[near, :].astype(F32) + raw * inv * a_gain[...]).astype(BF)

        loop(4, one, 4 * r)

    def gate_half(r):
        near = slice(r * half, (r + 1) * half)

        def one(at):
            cols = span(at * UNIT, UNIT)
            gate[near, cols] = dot(h[near, :], wg[:, cols]).astype(BF)

        loop(n_ff, one)

    def up_half(r):
        near = slice(r * half, (r + 1) * half)

        def one(at):
            cols = span(at * UNIT, UNIT)
            value = dot(h[near, :], wu[:, cols])
            up[near, cols] = value.astype(BF)
            pre = gate[near, cols].astype(F32)
            act[near, cols] = (pre * jax.nn.sigmoid(pre) * value).astype(BF)

        loop(n_ff, one)

    mid(0)
    gg.ready()
    sum_attn.tick(10)
    gate_half(0)
    gu.pass_on()
    sum_attn.tick(11)
    sum_attn.tick(12)
    gu.last()
    sum_attn.tick(13)
    gu.ready()
    up_half(0)
    need("wq", "wk", "wv", "wo", "cot")
    for g in (gq, gk, gv, go):
        g.drain()
    gd.relay()
    sum_attn.drain()
    sum_ffn = RowSum(place, part, took, d_ffn, row_sems.at[1], pairs_in_turn)

    def project_down(pair):
        r, bits = pair % 2, 2 * (pair // 2)
        near = slice(r * half, (r + 1) * half)

        def one(i):
            part[near, columns(bits + i)] = dot(act[near, :], wd[:, columns(bits + i)]).astype(BF)
            sum_ffn.begin(2 * pair + i)

        loop(2, one)

    gd.own_copy().wait()
    gd.arrived(6)
    project_down(0)
    mid(1)
    gate_half(1)
    up_half(1)
    sum_ffn.tick(0)
    project_down(1)
    sum_ffn.tick(1)
    gd.pass_on()
    gd.arrived(7)
    project_down(2)
    sum_ffn.tick(2)
    project_down(3)
    sum_ffn.tick(3)
    gd.arrived(8)
    project_down(4)
    sum_ffn.tick(4)
    gd.last()
    project_down(5)
    sum_ffn.tick(5)
    gd.arrived(9)
    project_down(6)
    sum_ffn.tick(6)
    project_down(7)
    for tick in range(7, sum_ffn.ticks):
        sum_ffn.tick(tick)
    sum_ffn.drain()
    for g in (gg, gu, gd):
        g.drain()

    gains[...] = jnp.zeros(gains.shape, F32)
    tile = rows // 8

    def back_ffn(at):
        near = span(at * tile, tile)
        raw = d_ffn[near, :].astype(F32)
        alive = side[near, 1:2]
        dy = alive * cot[near, :].astype(F32)
        inv = lax.rsqrt(jnp.mean(raw * raw, axis=1, keepdims=True) + EPS)
        normed = raw * inv
        gains[0:1, :] += jnp.sum(dy * normed, axis=0, keepdims=True)
        part[near, :] = (alive * (h[near, :].astype(F32) + normed * f_gain[...])).astype(BF)
        gained = f_gain[...] * dy
        mean = jnp.mean(gained * raw, axis=1, keepdims=True)
        d_ffn[near, :] = (inv * gained - raw * inv**3 * mean).astype(BF)

    loop(8, back_ffn)
    move("hidden_out", part, hidden_out)

    def flip(src):
        def one(at):
            near = span(at * UNIT, UNIT)
            turned[near, :] = src[:, near].T

        loop(width // UNIT, one)

    flip(d_ffn)
    scatter = Scatter(place, (wq, wk, wv, wo), (flat_out, tall_out), s_sems, s_out, (3 * ff + 4 * local) // UNIT)
    flat, tall = (True, 0), (False, n_ff)

    def back_act(r):
        near = slice(r * half, (r + 1) * half)

        def one(at):
            cols = span(at * UNIT, UNIT)
            d_act = dot_nt(d_ffn[near, :], wd[cols, :])
            pre, upper = gate[near, cols].astype(F32), up[near, cols].astype(F32)
            sig = jax.nn.sigmoid(pre)
            up[near, cols] = (d_act * pre * sig).astype(BF)
            gate[near, cols] = (d_act * upper * sig * (1.0 + pre * (1.0 - sig))).astype(BF)

        loop(n_ff, one)

    raw_h = x
    sum_back = RowSum(place, part, took, raw_h, row_sems.at[2], halves_in_turn)

    def back_gate(r, first):
        near = slice(r * half, (r + 1) * half)

        def one(i):
            value = dot_nt(gate[near, :], wg[columns(i), :]) + dot_nt(up[near, :], wu[columns(i), :])
            part[near, columns(i)] = value.astype(BF)
            sum_back.begin(r * 8 + i)

        loop(4, one, first)

    scatter.tick(0, flat, turned, act, 0)
    back_act(0)
    scatter.tick(1, flat, turned, act, 1)
    need("hidden_out")
    back_gate(0, 0)
    back_gate(0, 4)
    scatter.tick(2, flat, turned, act, 2)
    sum_back.tick(0)
    back_act(1)
    sum_back.tick(1)
    scatter.tick(3, flat, turned, act, 3)
    sum_back.tick(2)
    back_gate(1, 0)
    sum_back.tick(3)
    back_gate(1, 4)
    move("wq2", wq_out, wd.at[:, 0:local])
    move("wk2", wk_out, wd.at[:, local:2 * local])
    move("wv2", wv_out, wd.at[:, 2 * local:3 * local])
    move("wo2", wo_out, wg.at[0:local, :])
    move("x2", x_in, wu.at[0:rows, :])

    def with_act(i):
        sum_back.tick(4 + i)
        scatter.tick(4 + i, flat, turned, act, 4 + i)

    with_act(0)
    loop(3, with_act, 1)
    flip(h)
    for i in range(3):
        sum_back.tick(8 + i)
        scatter.tick(8 + i, flat, turned, gate, i)
    for i in range(3, 6):
        sum_back.tick(8 + i)
        scatter.tick(8 + i, tall, turned, gate, i)
    sum_back.drain()
    d_attn = wu.at[rows:2 * rows, :]

    def back_attn(at):
        near = span(at * tile, tile)
        raw = raw_a[near, :].astype(F32)
        dh = side[near, 1:2] * cot[near, :].astype(F32) + raw_h[near, :].astype(F32)
        inv = lax.rsqrt(jnp.mean(raw * raw, axis=1, keepdims=True) + EPS)
        gains[1:2, :] += jnp.sum(dh * raw * inv, axis=0, keepdims=True)
        gained = a_gain[...] * dh
        mean = jnp.mean(gained * raw, axis=1, keepdims=True)
        d_attn[near, :] = (inv * gained - raw * inv**3 * mean).astype(BF)

    loop(8, back_attn)
    need("wo2")
    scatter.tick(14, tall, turned, gate, 6)
    d_heads = wu.at[2 * rows:3 * rows, 3 * local:4 * local]
    d_heads[...] = dot_nt(d_attn[...], wg[0:local, :]).astype(BF)
    scatter.tick(15, tall, turned, gate, 7)
    dq, dk, dv = (wu.at[2 * rows:3 * rows, i * local:(i + 1) * local] for i in range(3))

    def back_head(hd):
        cols = span(hd * HD, HD)
        dk_sum[...] = jnp.zeros(dk_sum.shape, F32)
        dv_sum[...] = jnp.zeros(dv_sum.shape, F32)
        for rb in range(4):
            near, keys, allowed = allowed_at(rb)
            lse = jnp.sum(jnp.where(lane_at == hd, stat[near, :], 0.0), axis=1, keepdims=True)
            scores = jnp.where(allowed, dot_nt(qr[near, cols], kr[0:keys, cols]) * scale, -1e30)
            probs = jnp.where(allowed, jnp.exp(scores - lse), 0.0)
            grad = d_heads[near, cols]
            d_prob = dot_nt(grad, v[0:keys, cols])
            delta = jnp.sum(grad.astype(F32) * o[near, cols].astype(F32), axis=1, keepdims=True)
            d_score = (probs * (d_prob - delta)).astype(BF)
            back = dot(d_score, kr[0:keys, cols]) * scale
            dq[near, cols] = turn_back(back, cos_tab[near, :], sin_tab[near, :]).astype(BF)
            dk_sum[0:keys, :] += dot_tn(d_score, qr[near, cols])
            dv_sum[0:keys, :] += dot_tn(probs.astype(BF), grad)
        dk[:, cols] = turn_back(dk_sum[...] * scale, cos_tab[...], sin_tab[...]).astype(BF)
        dv[:, cols] = dv_sum[...].astype(BF)

    for hd in range(0, heads, 2):
        loop(2, back_head, hd)
        scatter.tick(16 + hd // 2, tall, turned, up, hd // 2)
    row_sum_back = SmallSum(place, sums.at[1], small.at[1])
    sums[1, 0] = jnp.zeros(sums.shape[2:], F32)
    for at, (grad, raw, gain, lane_of) in enumerate(((dq, qp, q_gain, heads), (dk, kp, k_gain, heads + 1))):
        both = grad[...].astype(F32) * raw[...].astype(F32)
        gains[2 + at:3 + at, 0:local] = jnp.sum(both * stat[:, lane_of:lane_of + 1], axis=0, keepdims=True)
        sums[1, 0, at:at + 1, :] = as_row(jnp.sum(gain[...] * both, axis=1, keepdims=True))
    row_sum_back.begin()
    scatter.tick(18, tall, turned, up, 2)
    totals = row_sum_back.end()
    for at, (grad, raw, gain, lane_of) in enumerate(((dq, qp, q_gain, heads), (dk, kp, k_gain, heads + 1))):
        inv = stat[:, lane_of:lane_of + 1]
        mean = as_col(totals[at:at + 1, :]) / width
        gained = gain[...] * grad[...].astype(F32)
        grad[...] = (inv * gained - raw[...].astype(F32) * inv**3 * mean).astype(BF)
    need("wq2", "wk2", "wv2", "x2")
    raw_x = d_ffn
    sum_in = RowSum(place, part, took, raw_x, row_sems.at[3], halves_in_turn)

    def back_in(r):
        near = slice(r * half, (r + 1) * half)

        def one(i):
            spot = columns(i)
            value = dot_nt(dq[near, :], wd[spot, 0:local]) + dot_nt(dk[near, :], wd[spot, local:2 * local])
            part[near, spot] = (value + dot_nt(dv[near, :], wd[spot, 2 * local:3 * local])).astype(BF)
            sum_in.begin(r * 8 + i)

        loop(8, one)

    back_in(0)
    scatter.tick(19, tall, turned, up, 3)
    back_in(1)

    def with_up(i):
        sum_in.tick(i)
        scatter.tick(20 + i, tall, turned, up, 4 + i)

    loop(4, with_up)
    flip(d_attn)
    for i in range(2):
        sum_in.tick(4 + i)
        scatter.tick(24 + i, tall, turned, o, i)
    flip(wu.at[0:rows, :])
    last = [(right, at) for right in (dq, dk, dv) for at in range(local // UNIT)]
    partners = (place.sib, place.xn, place.yn)
    n_units = scatter.count

    def gain_copy(at):
        return remote(
            gains.at[pl.ds(8 * at, 8), :], gains_got.at[at], gain_sems.at[0, at], gain_sems.at[1, at],
            {"dp": partners[at]},
        )

    def kind_of(u):
        first_flat = 3 * n_ff
        if u < n_ff:
            return flat
        if u < first_flat:
            return tall
        if u < first_flat + local // UNIT:
            return (True, 2 * n_ff)
        return (False, n_ff + local // UNIT)

    gain_copy(0).start()
    for i in range(n_units + 3 - 26):
        u = 26 + i
        if 6 + i < sum_in.ticks:
            sum_in.tick(6 + i)
        if last:
            scatter.tick(u, kind_of(u - 3), turned, *last.pop(0))
        else:
            scatter.tick(u, kind_of(u - 3))
        if i < 3:
            gain_copy(i).wait_recv()
            gains[8 * i + 8:8 * i + 16, :] = gains[8 * i:8 * i + 8, :] + gains_got[i]
            if i < 2:
                gain_copy(i + 1).start()
    move("gains", gains.at[24:32, :], gains_out)
    for tick in range(6 + n_units + 3 - 26, sum_in.ticks):
        sum_in.tick(tick)

    def end_tile(at):
        near = span(at * tile, tile)
        dh = side[near, 1:2] * cot[near, :].astype(F32) + raw_h[near, :].astype(F32)
        raw_x[near, :] = (dh + raw_x[near, :].astype(F32)).astype(BF)

    sum_in.drain()
    loop(8, end_tile)
    move("grad_in", raw_x, grad_in_out)
    for at in range(3):
        gain_copy(at).wait_send()
    row_sum.drain()
    row_sum_back.drain()
    scatter.drain()
    need("gains", "grad_in")


def layer_call(n_mp, x, cot, weights, seg, live, freq, q_gain, k_gain, a_gain, f_gain):
    rows, width = x.shape
    local, ff = weights[0].shape[1], weights[4].shape[1]
    high, half = width // 8, rows // 2
    any_spec = pl.BlockSpec(memory_space=pl.ANY)
    vmem = pl.BlockSpec(memory_space=pltpu.VMEM)
    S, V, dma = jax.ShapeDtypeStruct, pltpu.VMEM, pltpu.SemaphoreType.DMA
    fulls = [(width, local)] * 3 + [(local, width)] + [(width, ff)] * 2 + [(ff, width)]
    outs = fulls[:4] + [
        (rows, width), (rows, width), (ff + local, high), (high, 2 * ff + 3 * local),
    ]
    return pl.pallas_call(
        functools.partial(layer_kernel, n_mp),
        out_shape=[S(s, BF) for s in outs] + [S((8, width), F32)],
        in_specs=[any_spec] * 9 + [vmem] * 7,
        out_specs=[any_spec] * 9,
        scratch_shapes=[V(s, BF) for s in fulls]
        + [V((rows, width), BF)]
        + [V((rows, local), BF)] * 6
        + [V((rows, HD), F32)] * 4
        + [V((rows, width), BF)] * 2
        + [V((rows, ff), BF)] * 3
        + [V((rows, width), BF)] * 3
        + [V((2, 8, half, high), BF), V((width, rows), BF), V((rows, HD), F32), V((rows, HD), F32)]
        + [V((2, n_mp, 8, rows), F32), V((32, width), F32), V((3, 8, width), F32)]
        + [dma((7, 10)), dma((7, 10)), dma((7,)), dma((4, 4, 2, 8)), dma((2, 2, n_mp))]
        + [dma((2, 5, 4)), dma((2,)), dma((2, 3)), dma((16,))],
        compiler_params=pltpu.CompilerParams(
            collective_id=0, has_side_effects=True, vmem_limit_bytes=67043328,
        ),
    )(x, cot, *weights, seg, live, freq, q_gain, k_gain, a_gain, f_gain)


def with_kernel(n_mp, hidden_in, cotangent, segments, live_counts, *rest):
    weights, (query_gain, key_gain, attn_gain, ffn_gain) = rest[:7], rest[7:]
    local, ff = weights[0].shape[1], weights[4].shape[1]
    inv_freq = THETA ** (-(jnp.arange(HD // 2, dtype=F32) * (2.0 / HD)))
    freq = jnp.concatenate([inv_freq, inv_freq])[None]
    _, _, _, _, hidden_out, grad_in, flat, tall, gains = layer_call(
        n_mp, hidden_in, cotangent, weights, segments, live_counts[None], freq,
        query_gain[None], key_gain[None], attn_gain[None], ffn_gain[None],
    )

    def piece(first, count):
        return tall[:, first:first + count].astype(F32)

    return (
        hidden_out,
        grad_in.astype(F32),
        piece(2 * ff, local),
        piece(2 * ff + local, local),
        piece(2 * ff + 2 * local, local),
        flat[ff:].astype(F32),
        piece(0, ff),
        piece(ff, ff),
        flat[:ff].astype(F32),
        gains[2, :local],
        gains[3, :local],
        gains[1],
        gains[0],
    )


def doc_positions(seg_row):
    row_count = seg_row.shape[0]
    row_index = jnp.arange(row_count, dtype=jnp.int32)
    change = jnp.concatenate([jnp.ones((1,), dtype=bool), seg_row[1:] != seg_row[:-1]])
    doc_start = lax.cummax(jnp.where(change, row_index, jnp.zeros_like(row_index)), axis=0)
    return (row_index - doc_start).astype(jnp.float32)


def rotary_tables(positions, head_size):
    half_size = head_size // 2
    inv_freq = THETA ** (-(jnp.arange(half_size, dtype=jnp.float32) * (2.0 / head_size)))
    angles = positions[:, None] * inv_freq[None, :]
    return (jnp.cos(angles)[:, None, :], jnp.sin(angles)[:, None, :])


def rotate(values, cos_tab, sin_tab):
    half_size = values.shape[2] // 2
    first_half = values[:, :, :half_size]
    second_half = values[:, :, half_size:]
    return jnp.concatenate(
        [
            first_half * cos_tab - second_half * sin_tab,
            second_half * cos_tab + first_half * sin_tab,
        ],
        axis=2,
    )


def rotate_back(grads, cos_tab, sin_tab):
    half_size = grads.shape[2] // 2
    first_half = grads[:, :, :half_size]
    second_half = grads[:, :, half_size:]
    return jnp.concatenate(
        [
            first_half * cos_tab + second_half * sin_tab,
            second_half * cos_tab - first_half * sin_tab,
        ],
        axis=2,
    )


def block_mask(seg_row, offset, block_rows):
    row_index = jnp.arange(seg_row.shape[0])
    same = seg_row[offset : offset + block_rows, None] == seg_row[None, :]
    return same & (row_index[:, None] >= row_index[None, :])


def block_scores(q_blk, k_bf, allowed, score_scale):
    scores = (
        jnp.einsum("qhe,khe->hqk", q_blk, k_bf, preferred_element_type=jnp.float32) * score_scale
    )
    return jnp.where(allowed[None], scores, jnp.float32(-1e30))


def attend_forward(q_bf, k_bf, v_bf, seg_row, score_scale):
    row_count = q_bf.shape[0]
    block_rows = min(512, row_count)
    allowed = block_mask(seg_row, 0, block_rows)
    scores = block_scores(q_bf, k_bf, allowed, score_scale)
    row_max = jnp.max(scores, axis=2, keepdims=True)
    lse = row_max + jnp.log(jnp.sum(jnp.exp(scores - row_max), axis=2, keepdims=True))
    probs = jnp.exp(scores - lse).astype(jnp.bfloat16)
    outputs = jnp.einsum("hqk,khe->qhe", probs, v_bf, preferred_element_type=jnp.float32)
    lse_parts = [lse]
    return (outputs.astype(jnp.bfloat16), lse_parts)


def attend_backward(q_bf, k_bf, v_bf, o_bf, do_bf, lse_parts, seg_row, score_scale):
    row_count = q_bf.shape[0]
    block_rows = min(512, row_count)
    dq_parts = []
    dk_acc = jnp.zeros(k_bf.shape, jnp.float32)
    dv_acc = jnp.zeros(v_bf.shape, jnp.float32)
    for part_index, offset in enumerate(range(0, row_count, block_rows)):
        allowed = block_mask(seg_row, offset, block_rows)
        scores = block_scores(q_bf, k_bf, allowed, score_scale)
        probs = jnp.exp(scores - lse_parts[part_index])
        probs_bf = probs.astype(jnp.bfloat16)
        dprob = jnp.einsum("qhe,khe->hqk", do_bf, v_bf, preferred_element_type=jnp.float32)
        delta = jnp.transpose(
            jnp.sum(do_bf.astype(jnp.float32) * o_bf.astype(jnp.float32), axis=2)
        )[:, :, None]
        dscore = (probs * (dprob - delta)).astype(jnp.bfloat16)
        dq_parts.append(
            jnp.einsum("hqk,khe->qhe", dscore, k_bf, preferred_element_type=jnp.float32)
            * score_scale
        )
        dk_acc = (
            jnp.einsum("hqk,qhe->khe", dscore, q_bf, preferred_element_type=jnp.float32)
            * score_scale
        )
        dv_acc = jnp.einsum("hqk,qhe->khe", probs_bf, do_bf, preferred_element_type=jnp.float32)
    return (dq_parts[0], dk_acc, dv_acc.astype(jnp.bfloat16))


def scatter_grad(grad, axis_name, scatter_dimension, tiled):
    total = lax.psum_scatter(
        grad.astype(jnp.bfloat16), axis_name, scatter_dimension=scatter_dimension, tiled=tiled
    )
    return total.astype(jnp.float32)


def sum_parts(part, axis_name):
    own = lax.psum_scatter(
        part.astype(jnp.bfloat16), axis_name, scatter_dimension=0, tiled=True
    )
    return lax.all_gather(own, axis_name, axis=0, tiled=True).astype(jnp.float32)


def norm_back(raw, inv_scale, gained, row_sums, width):
    return inv_scale * gained - raw * inv_scale**3 * (row_sums[:, None] / width)


def on_device(
    hidden_in,
    cotangent,
    segments,
    live_counts,
    w_query,
    w_key,
    w_value,
    w_output,
    w_gate,
    w_up,
    w_down,
    query_gain,
    key_gain,
    attn_gain,
    ffn_gain,
):
    gathered = (
        lax.all_gather(w_query, "dp", axis=0, tiled=True),
        lax.all_gather(w_key, "dp", axis=0, tiled=True),
        lax.all_gather(w_value, "dp", axis=0, tiled=True),
        lax.all_gather(w_output, "dp", axis=1, tiled=True),
        lax.all_gather(w_gate, "dp", axis=0, tiled=True),
        lax.all_gather(w_up, "dp", axis=0, tiled=True),
        lax.all_gather(w_down, "dp", axis=1, tiled=True),
    )
    wq_full, wk_full, wv_full, wo_full, wg_full, wu_full, wd_full = gathered
    seg_row = segments[0]
    live_n = live_counts[0]
    row_count, width = hidden_in.shape
    local_width = wq_full.shape[1]
    heads_here = local_width // HD
    score_scale = 1.0 / math.sqrt(HD)
    live_mask = (jnp.arange(row_count, dtype=jnp.int32) < live_n).astype(jnp.float32)[:, None]
    cos_tab, sin_tab = rotary_tables(doc_positions(seg_row), HD)
    q_proj = jnp.dot(hidden_in, wq_full, preferred_element_type=jnp.float32)
    k_proj = jnp.dot(hidden_in, wk_full, preferred_element_type=jnp.float32)
    v_bf = jnp.dot(hidden_in, wv_full, preferred_element_type=jnp.float32).astype(jnp.bfloat16)
    sq_query, sq_key = lax.psum(
        (jnp.sum(q_proj * q_proj, axis=1), jnp.sum(k_proj * k_proj, axis=1)), "mp"
    )
    inv_q = lax.rsqrt(sq_query[:, None] / width + EPS)
    inv_k = lax.rsqrt(sq_key[:, None] / width + EPS)
    q_rot = rotate(
        (q_proj * inv_q * query_gain).reshape(row_count, heads_here, HD), cos_tab, sin_tab
    ).astype(jnp.bfloat16)
    k_rot = rotate(
        (k_proj * inv_k * key_gain).reshape(row_count, heads_here, HD), cos_tab, sin_tab
    ).astype(jnp.bfloat16)
    v_heads = v_bf.reshape(row_count, heads_here, HD)
    o_bf, lse_parts = attend_forward(q_rot, k_rot, v_heads, seg_row, score_scale)
    o_flat = o_bf.reshape(row_count, local_width)
    attn_raw = sum_parts(jnp.dot(o_flat, wo_full, preferred_element_type=jnp.float32), "mp")
    inv_a = lax.rsqrt(jnp.mean(attn_raw * attn_raw, axis=1, keepdims=True) + EPS)
    h_mid = hidden_in.astype(jnp.float32) + attn_raw * inv_a * attn_gain
    h_bf = h_mid.astype(jnp.bfloat16)
    gate_pre = jnp.dot(h_bf, wg_full, preferred_element_type=jnp.float32)
    up_pre = jnp.dot(h_bf, wu_full, preferred_element_type=jnp.float32)
    act_bf = (jax.nn.silu(gate_pre) * up_pre).astype(jnp.bfloat16)
    ffn_raw = sum_parts(jnp.dot(act_bf, wd_full, preferred_element_type=jnp.float32), "mp")
    inv_f = lax.rsqrt(jnp.mean(ffn_raw * ffn_raw, axis=1, keepdims=True) + EPS)
    hidden_out = (live_mask * (h_mid + ffn_raw * inv_f * ffn_gain)).astype(jnp.bfloat16)
    wq_back, wk_back, wv_back, wo_back, wg_back, wu_back, wd_back = gathered
    dy = live_mask * cotangent.astype(jnp.float32)
    g_ffn_gain = jnp.sum(dy * ffn_raw * inv_f, axis=0)
    gained_f = ffn_gain * dy
    d_ffn = norm_back(ffn_raw, inv_f, gained_f, jnp.sum(gained_f * ffn_raw, axis=1), width).astype(
        jnp.bfloat16
    )
    d_act = jnp.dot(d_ffn, wd_back.T, preferred_element_type=jnp.float32)
    sig = jax.nn.sigmoid(gate_pre)
    d_up = (d_act * gate_pre * sig).astype(jnp.bfloat16)
    d_gate = (d_act * up_pre * sig * (1.0 + gate_pre * (1.0 - sig))).astype(jnp.bfloat16)
    ffn_part = jnp.dot(d_gate, wg_back.T, preferred_element_type=jnp.float32) + jnp.dot(
        d_up, wu_back.T, preferred_element_type=jnp.float32
    )
    dh = dy + sum_parts(ffn_part, "mp")
    g_down = jnp.dot(act_bf.T, d_ffn, preferred_element_type=jnp.float32)
    g_gate = jnp.dot(h_bf.T, d_gate, preferred_element_type=jnp.float32)
    g_up = jnp.dot(h_bf.T, d_up, preferred_element_type=jnp.float32)
    g_attn_gain = jnp.sum(dh * attn_raw * inv_a, axis=0)
    gained_a = attn_gain * dh
    d_attn = norm_back(
        attn_raw, inv_a, gained_a, jnp.sum(gained_a * attn_raw, axis=1), width
    ).astype(jnp.bfloat16)
    d_heads = jnp.dot(d_attn, wo_back.T, preferred_element_type=jnp.float32).astype(jnp.bfloat16)
    g_output = jnp.dot(o_flat.T, d_attn, preferred_element_type=jnp.float32)
    dq_rot, dk_rot, d_val = attend_backward(
        q_rot,
        k_rot,
        v_heads,
        o_bf,
        d_heads.reshape(row_count, heads_here, HD),
        lse_parts,
        seg_row,
        score_scale,
    )
    dq_norm = rotate_back(dq_rot, cos_tab, sin_tab).reshape(row_count, local_width)
    dk_norm = rotate_back(dk_rot, cos_tab, sin_tab).reshape(row_count, local_width)
    g_query_gain = jnp.sum(dq_norm * q_proj * inv_q, axis=0)
    g_key_gain = jnp.sum(dk_norm * k_proj * inv_k, axis=0)
    gained_q = query_gain * dq_norm
    gained_k = key_gain * dk_norm
    sums_query, sums_key = lax.psum(
        (jnp.sum(gained_q * q_proj, axis=1), jnp.sum(gained_k * k_proj, axis=1)), "mp"
    )
    dq_bf = norm_back(q_proj, inv_q, gained_q, sums_query, width).astype(jnp.bfloat16)
    dk_bf = norm_back(k_proj, inv_k, gained_k, sums_key, width).astype(jnp.bfloat16)
    dv_bf = d_val.reshape(row_count, local_width)
    input_part = (
        jnp.dot(dq_bf, wq_back.T, preferred_element_type=jnp.float32)
        + jnp.dot(dk_bf, wk_back.T, preferred_element_type=jnp.float32)
        + jnp.dot(dv_bf, wv_back.T, preferred_element_type=jnp.float32)
    )
    grad_in = dh + sum_parts(input_part, "mp")
    g_query = jnp.dot(hidden_in.T, dq_bf, preferred_element_type=jnp.float32)
    g_key = jnp.dot(hidden_in.T, dk_bf, preferred_element_type=jnp.float32)
    g_value = jnp.dot(hidden_in.T, dv_bf, preferred_element_type=jnp.float32)
    owned = (
        scatter_grad(g_query, "dp", scatter_dimension=0, tiled=True),
        scatter_grad(g_key, "dp", scatter_dimension=0, tiled=True),
        scatter_grad(g_value, "dp", scatter_dimension=0, tiled=True),
        scatter_grad(g_output, "dp", scatter_dimension=1, tiled=True),
        scatter_grad(g_gate, "dp", scatter_dimension=0, tiled=True),
        scatter_grad(g_up, "dp", scatter_dimension=0, tiled=True),
        scatter_grad(g_down, "dp", scatter_dimension=1, tiled=True),
    )
    gain_totals = lax.psum((g_query_gain, g_key_gain, g_attn_gain, g_ffn_gain), "dp")
    return (
        hidden_out,
        grad_in,
        owned[0],
        owned[1],
        owned[2],
        owned[3],
        owned[4],
        owned[5],
        owned[6],
        gain_totals[0],
        gain_totals[1],
        gain_totals[2],
        gain_totals[3],
    )


def kernel_fits(mesh, hidden_in, segments, w_query, w_gate):
    n_dp, n_mp = mesh.shape["dp"], mesh.shape["mp"]
    rows, width = hidden_in.shape[0] // n_dp, hidden_in.shape[1]
    local, ff = w_query.shape[1] // n_mp, w_gate.shape[1] // n_mp
    even = width % (8 * UNIT) == 0 and local % UNIT == 0 and ff % (2 * UNIT) == 0
    fits = rows == UNIT * 2 and width == 8 * UNIT and local == rows and ff == width
    return n_dp == 8 and n_mp >= 2 and even and fits


def solution(mesh):
    in_specs = (
        P("dp", None),
        P("dp", None),
        P("dp", None),
        P("dp"),
        P("dp", "mp"),
        P("dp", "mp"),
        P("dp", "mp"),
        P("mp", "dp"),
        P("dp", "mp"),
        P("dp", "mp"),
        P("mp", "dp"),
        P("mp"),
        P("mp"),
        P(),
        P(),
    )
    out_specs = (
        P("dp", None),
        P("dp", None),
        P("dp", "mp"),
        P("dp", "mp"),
        P("dp", "mp"),
        P("mp", "dp"),
        P("dp", "mp"),
        P("dp", "mp"),
        P("mp", "dp"),
        P("mp"),
        P("mp"),
        P(),
        P(),
    )

    def step(*args):
        if kernel_fits(mesh, args[0], args[2], args[4], args[8]):
            body = functools.partial(with_kernel, mesh.shape["mp"])
        else:
            body = on_device
        return jax.shard_map(
            body, mesh=mesh, in_specs=in_specs, out_specs=out_specs, check_vma=False
        )(*args)

    return step
```

```python
import functools
import math

import jax
import jax.numpy as jnp
from jax import lax
from jax.experimental import pallas as pl
from jax.experimental.pallas import tpu as pltpu
from jax.sharding import PartitionSpec as P

HD = 128
EPS = 1e-06
THETA = 500000.0
UNIT = 256
BF = jnp.bfloat16
F32 = jnp.float32


def dot(a, b):
    return jnp.dot(a, b, preferred_element_type=F32)


def dot_nt(a, b):
    return lax.dot_general(a, b, (((1,), (1,)), ((), ())), preferred_element_type=F32)


def dot_tn(a, b):
    return lax.dot_general(a, b, (((0,), (0,)), ((), ())), preferred_element_type=F32)


def span(start, size):
    return pl.ds(start if isinstance(start, int) else pl.multiple_of(start, size), size)


def loop(count, body, first=0):
    def step(at, carry):
        body(at)
        return carry

    lax.fori_loop(first, first + count, step, 0)


def remote(src, dst, send, recv, device):
    return pltpu.make_async_remote_copy(
        src_ref=src, dst_ref=dst, send_sem=send, recv_sem=recv,
        device_id=device, device_id_type=pl.DeviceIdType.MESH,
    )


class Place:
    def __init__(self, n_mp):
        self.dp, self.z = lax.axis_index("dp"), lax.axis_index("mp")
        self.n_mp, self.end = n_mp, n_mp - 1
        self.c = lax.rem(self.dp, 2)
        self.x = lax.rem(self.dp // 2, 2)
        self.y = self.dp // 4
        self.sib, self.xn, self.yn, self.dg = (self.block(i) for i in (1, 2, 4, 6))

    def block(self, i):
        i0, i1, i2 = i % 2, (i // 2) % 2, i // 4
        c, x, y = (a + b - 2 * a * b for a, b in ((self.c, i0), (self.x, i1), (self.y, i2)))
        return 4 * y + 2 * x + c

    def barrier(self):
        sem = pltpu.get_barrier_semaphore()
        mesh = pl.DeviceIdType.MESH
        for dp in (self.sib, self.xn, self.yn):
            pl.semaphore_signal(sem, inc=1, device_id={"dp": dp}, device_id_type=mesh)
        for step in range(1, self.n_mp):
            z = lax.rem(self.z + step, self.n_mp)
            pl.semaphore_signal(sem, inc=1, device_id={"mp": z}, device_id_type=mesh)
        pl.semaphore_wait(sem, 3 + self.n_mp - 1)


class Gather:
    def __init__(self, place, src, full, by_rows, send, recv, local):
        self.place, self.src, self.full, self.by_rows = place, src, full, by_rows
        self.sends, self.recvs, self.local = send, recv, local
        self.rows, self.cols = src.shape
        self.half = self.rows // 2

    def spot(self, owner, part=None):
        size = self.rows if self.by_rows else self.cols
        first, count = (0, size) if part is None else (part * size // 2, size // 2)
        near = pl.ds(pl.multiple_of(owner * size + first, size // 2), count)
        return self.full.at[near, :] if self.by_rows else self.full.at[:, near]

    def mine(self, part):
        size = (self.rows if self.by_rows else self.cols) // 2
        near = pl.ds(part * size, size)
        return self.src.at[near, :] if self.by_rows else self.src.at[:, near]

    def copies(self):
        p = self.place
        table = {
            0: (self.mine(0), p.dp, 0, p.xn, p.xn),
            1: (self.mine(1), p.dp, 1, p.xn, p.xn),
            2: (self.mine(0), p.dp, 0, p.yn, p.yn),
            3: (self.mine(1), p.dp, 1, p.yn, p.yn),
            6: (self.src, p.dp, None, p.sib, p.sib),
        }
        for kind, owner, part, target, arrives in (
            (4, p.yn, 1, p.xn, p.dg), (5, p.xn, 0, p.yn, p.dg),
            (7, p.xn, 0, p.sib, p.block(3)), (10, p.xn, 1, p.sib, p.block(3)),
            (8, p.yn, 1, p.sib, p.block(5)), (11, p.yn, 0, p.sib, p.block(5)),
            (9, p.dg, None, p.sib, p.block(7)),
        ):
            table[kind] = (self.spot(owner, part), owner, part, target, arrives)
        return table

    def copy(self, kind):
        src, owner, part, target, _ = self.copies()[kind]
        return remote(src, self.spot(owner, part), self.sends.at[kind], self.recvs.at[kind], {"dp": target})

    def start(self, *kinds):
        for kind in kinds:
            self.copy(kind).start()

    def arrived(self, *kinds):
        for kind in kinds:
            _, _, part, target, owner = self.copies()[kind]
            spot = self.spot(owner, part)
            remote(spot, spot, self.sends.at[kind], self.recvs.at[kind], {"dp": target}).wait_recv()

    def own_copy(self):
        return pltpu.make_async_copy(self.src, self.spot(self.place.dp), self.local)

    def begin_a(self):
        self.start(0, 3)

    def begin_b(self):
        self.start(1, 2, 6)
        self.own_copy().start()

    def relay(self):
        self.arrived(0)
        self.start(5, 7)
        self.arrived(3)
        self.start(4, 8)

    def pass_on(self):
        self.arrived(1)
        self.start(10)
        self.arrived(2)
        self.start(11)

    def last(self):
        self.arrived(5, 4)
        self.start(9)

    def ready(self):
        self.own_copy().wait()
        self.arrived(6, 7, 8, 9, 10, 11)

    def drain(self):
        for kind in range(12):
            self.copy(kind).wait_send()


class RowSum:
    def __init__(self, place, part, took, total, sems, chunk_at, count):
        self.place, self.part, self.took, self.total, self.sems = place, part, took, total, sems
        self.chunk_at = chunk_at
        self.count = count

    def spot(self, ref, flow, k):
        return ref.at[self.chunk_at(flow, k)]

    def at(self, flow):
        return self.place.z + flow * (self.place.end - 2 * self.place.z)

    def forth(self, flow, k):
        return remote(
            self.spot(self.part, flow, k), self.took(flow, k),
            self.sems.at[0, flow, k], self.sems.at[1, flow, k], {"mp": self.place.z + 1 - 2 * flow},
        )

    def back(self, flow, k):
        spot = self.spot(self.total, flow, k)
        return remote(spot, spot, self.sems.at[2, flow, k], self.sems.at[3, flow, k], {"mp": self.place.z - 1 + 2 * flow})

    def push(self, k):
        if isinstance(k, int) and k >= self.count:
            return

        def one(flow):
            @pl.when((self.at(flow) == 0) & (k < self.count))
            def _():
                self.forth(flow, k).start()

        loop(2, one)

    def add(self, dst, flow, k):
        mine, to, more = self.spot(self.part, flow, k), self.spot(dst, flow, k), self.took(flow, k)
        step = mine.shape[0] // 4

        def one(at):
            near = span(at * step, step)
            to[near, :] = (mine[near, :].astype(F32) + more[near, :].astype(F32)).astype(BF)

        loop(4, one)

    def tick(self, t, half):
        end, count = self.place.end, self.count // 2
        if isinstance(t, int) and t >= count + 2 * end:
            return

        def gather(flow):
            at = self.at(flow)
            k = t - at

            @pl.when((at > 0) & (k >= 0) & (k < count))
            def _():
                chunk = half * count + k
                self.forth(flow, chunk).wait_recv()

                @pl.when(at < end)
                def _():
                    self.add(self.part, flow, chunk)
                    self.forth(flow, chunk).start()

                @pl.when(at == end)
                def _():
                    self.add(self.total, flow, chunk)
                    self.back(flow, chunk).start()

        def bring_back(flow):
            at = self.at(flow)
            k = t - 2 * end + at

            @pl.when((at < end) & (k >= 0) & (k < count))
            def _():
                chunk = half * count + k
                self.back(flow, chunk).wait_recv()

                @pl.when(at > 0)
                def _():
                    self.back(flow, chunk).start()

        if not isinstance(t, int) or t < count + end:
            loop(2, gather)
        if not isinstance(t, int) or t >= end + 1:
            loop(2, bring_back)

    def both(self, t, lag):
        self.tick(t, 0)
        self.tick(t - lag, 1)

    def sent(self, half=None):
        first, count = (0, self.count) if half is None else (half * self.count // 2, self.count // 2)
        for flow in range(2):
            at = self.at(flow)

            def one(k):
                @pl.when(at < self.place.end)
                def _():
                    self.forth(flow, k).wait_send()

                @pl.when(at > 0)
                def _():
                    self.back(flow, k).wait_send()

            loop(count, one, first)


class SmallSum:
    def __init__(self, place, slots, sems):
        self.place, self.slots, self.sems = place, slots, sems

    def copy(self, step):
        p = self.place
        return remote(
            self.slots.at[0], self.slots.at[step], self.sems.at[0, step], self.sems.at[1, step],
            {"mp": lax.rem(p.z + step, p.n_mp)},
        )

    def begin(self):
        for step in range(1, self.place.n_mp):
            self.copy(step).start()

    def end(self):
        for step in range(1, self.place.n_mp):
            self.copy(step).wait_recv()
        total = self.slots[0]
        for step in range(1, self.place.n_mp):
            total = total + self.slots[step]
        return total

    def drain(self):
        for step in range(1, self.place.n_mp):
            self.copy(step).wait_send()


class Scatter:
    def __init__(self, place, pool, outs, sems, out_sems, n_ff, n_local):
        self.place, self.pool, self.outs = place, pool, outs
        self.n_ff, self.n_local, self.early = n_ff, n_local, 3 * n_ff
        self.count = 3 * n_ff + 4 * n_local
        self.sems, self.out_sems = sems, out_sems
        self.rows = pool[0].shape[0] // 8
        self.half = self.rows // 2

    def column(self, array, at, start, size):
        return self.pool[array].at[span(start, size), pl.ds(at, UNIT)]

    def made(self, u, own):
        return self.pool[0].at[span((u % 2) * 4 * self.rows, 4 * self.rows), span(own * UNIT, UNIT)]

    def got(self, u, chip=None):
        s = u % 4
        first, size = (s % 2) * 4 * self.rows, 4 * self.rows
        if chip is not None:
            first, size = first + chip * self.rows, self.rows
        return self.pool[1].at[span(first, size), span(s // 2 * UNIT, UNIT)]

    def sums(self, which, u, to, then=None):
        first, size = (u % 4) * 2 * self.rows + to * self.rows, self.rows
        if then is not None:
            first, size = first + then * self.half, self.half
        return self.column(2, which * UNIT, first, size)

    def met(self, which, u):
        return self.pool[3].at[span((u % 2) * self.rows, self.rows), span((3 + 2 * which + u % 4 // 2) * UNIT, UNIT)]

    def ended(self, which, u):
        return self.column(3, which * UNIT, (u % 4) * self.half, self.half)

    def done(self, u):
        return self.column(3, 2 * UNIT, (u % 2) * self.rows, self.rows)

    def send(self, kind, u):
        p, s = self.place, u % 4
        src, dst, target = {
            0: lambda: (self.made(u, 0), self.got(u), p.sib),
            1: lambda: (self.sums(0, u, 1 - p.x), self.met(0, u), p.xn),
            2: lambda: (self.sums(1, u, 1 - p.y), self.met(1, u), p.yn),
            3: lambda: (self.sums(0, u, p.x, 1 - p.y), self.ended(0, u), p.yn),
            4: lambda: (self.sums(1, u, p.y, 1 - p.x), self.ended(1, u), p.xn),
        }[kind]()
        return remote(src, dst, self.sems.at[0, kind, s], self.sems.at[1, kind, s], {"dp": target})

    def product(self, u, turned, right, at):
        cols = span(at * UNIT, UNIT)

        def one(own):
            near = span(own * 4 * self.rows, 4 * self.rows)
            self.made(u, own)[...] = dot(turned[near, :], right[:, cols]).astype(BF)

            @pl.when(own == 0)
            def _():
                self.send(0, u).start()

        loop(2, one)

    def across(self, u):
        self.send(0, u).wait_recv()
        self.send(0, u).wait_send()
        mine = self.made(u, 1)

        def add(chip):
            y_to, x_to = chip // 2, chip % 2
            more = self.got(u, chip)
            for which, spot in ((0, self.sums(0, u, x_to, y_to)), (1, self.sums(1, u, y_to, x_to))):
                near = slice(which * self.half, (which + 1) * self.half)
                own = mine[span(chip * self.rows + which * self.half, self.half), :]
                spot[...] = (own.astype(F32) + more[near, :].astype(F32)).astype(BF)

        loop(4, add)
        self.send(1, u).start()
        self.send(2, u).start()

    def along(self, u):
        p = self.place
        for which, mine in ((0, p.x), (1, p.y)):
            self.send(1 + which, u).wait_recv()
            spot, more = self.sums(which, u, mine), self.met(which, u)
            spot[...] = (spot[...].astype(F32) + more[...].astype(F32)).astype(BF)
            self.send(3 + which, u).start()
        for kind in (1, 2):
            self.send(kind, u).wait_send()

    def wait_write(self, u):
        pltpu.make_async_copy(self.done(u), self.done(u), self.out_sems.at[u % 2]).wait()

    def finish(self, u):
        p = self.place

        @pl.when(u >= 2)
        def _():
            self.wait_write(u)

        parts = []
        for which, spot in ((0, self.sums(0, u, p.x, p.y)), (1, self.sums(1, u, p.y, p.x))):
            self.send(3 + which, u).wait_recv()
            parts.append(spot[...].astype(F32) + self.ended(which, u)[...].astype(F32))
        value = jnp.concatenate(parts, axis=0)
        late = u // self.early
        flat = (u < self.n_ff) | ((u >= self.early) & (u < self.early + self.n_local))

        @pl.when(flat)
        def _():
            self.done(u)[...] = value.T.astype(BF)
            target = self.outs[0].at[span((u - late * 2 * self.n_ff) * UNIT, UNIT), :]
            pltpu.make_async_copy(self.done(u), target, self.out_sems.at[u % 2]).start()

        @pl.when(jnp.logical_not(flat))
        def _():
            self.done(u)[...] = value.astype(BF)
            target = self.outs[1].at[:, span((u - self.n_ff - late * self.n_local) * UNIT, UNIT)]
            pltpu.make_async_copy(self.done(u), target, self.out_sems.at[u % 2]).start()

        for kind in (3, 4):
            self.send(kind, u).wait_send()

    def tick(self, u, turned, ffs, others):
        @pl.when(u < self.early)
        def _():
            self.product(u, turned, ffs.at[u // self.n_ff], u % self.n_ff)

        @pl.when((u >= self.early) & (u < self.count))
        def _():
            self.product(u, turned, others, u - self.early)

        for lag, stage in ((1, self.across), (2, self.along), (3, self.finish)):
            @pl.when((u >= lag) & (u < self.count + lag))
            def _():
                stage(u - lag)

    def drain(self):
        for u in (self.count - 2, self.count - 1):
            self.wait_write(u)


def as_row(col):
    n = col.shape[0]
    r = lax.broadcasted_iota(jnp.int32, (n, n), 0)
    s = lax.broadcasted_iota(jnp.int32, (n, n), 1)
    return jnp.sum(jnp.where(r == s, col, 0.0), axis=0, keepdims=True)


def as_col(row):
    n = row.shape[1]
    r = lax.broadcasted_iota(jnp.int32, (n, n), 0)
    s = lax.broadcasted_iota(jnp.int32, (n, n), 1)
    return jnp.sum(jnp.where(r == s, row, 0.0), axis=1, keepdims=True)


def turn(values, cos_tab, sin_tab):
    return values * cos_tab + pltpu.roll(values, HD // 2, 1) * sin_tab


def turn_back(grads, cos_tab, sin_tab):
    return grads * cos_tab - pltpu.roll(grads, HD // 2, 1) * sin_tab


def layer_kernel(
    n_mp,
    x_in, cot_in, wq_in, wk_in, wv_in, wo_in, wg_in, wu_in, wd_in,
    seg, live, freq, q_gain, k_gain, a_gain, f_gain,
    wq_out, wk_out, wv_out, wo_out, hidden_out, grad_in_out, flat_out, tall_out, gains_out,
    wq, wk, wv, wo, wg, wu, wd,
    x, qp, kp, qr, kr, v, o, stat, cos_tab, sin_tab, side, raw_a, h, ffs, d_ffn, cot, part, took,
    turned, dk_sum, dv_sum, sums, gains, gains_got,
    g_send, g_recv, g_local, row_sems, small, s_sems, s_out, gain_sems, io_sems,
):
    place = Place(n_mp)
    rows, width = x.shape
    local, ff = qp.shape[1], ffs.shape[2]
    act, gate, up = (ffs.at[i] for i in range(3))
    heads = local // HD
    scale = 1.0 / math.sqrt(HD)
    half = rows // 2
    n_ff, n_local = ff // UNIT, local // UNIT
    flying = {}

    def move(name, src, dst):
        at = len(flying)
        flying[name] = lambda: pltpu.make_async_copy(src, dst, io_sems.at[at])
        flying[name]().start()

    def need(*names):
        for name in names:
            flying[name]().wait()

    move("x", x_in, x)
    place.barrier()
    gq, gk, gv, go, gg, gu, gd = [
        Gather(place, src, full, i not in (3, 6), g_send.at[i], g_recv.at[i], g_local.at[i])
        for i, (src, full) in enumerate(
            zip((wq_in, wk_in, wv_in, wo_in, wg_in, wu_in, wd_in), (wq, wk, wv, wo, wg, wu, wd))
        )
    ]
    gq.begin_a()
    gq.begin_b()
    gk.begin_a()
    gk.begin_b()
    move("cot", cot_in, cot)
    ids = seg[...].astype(F32)
    ids_col = as_col(ids)
    before = jnp.sum((ids < ids_col).astype(F32), axis=1, keepdims=True)
    row_at = lax.broadcasted_iota(jnp.int32, (rows, 1), 0)
    side[:, 0:1] = ids_col
    side[:, 1:2] = (row_at < live[...]).astype(F32)
    angles = (row_at.astype(F32) - before) * freq[...]
    cos_tab[...] = jnp.cos(angles)
    lane = lax.broadcasted_iota(jnp.int32, (rows, HD), 1)
    sin_tab[...] = jnp.sin(angles) * jnp.where(lane < HD // 2, -1.0, 1.0)
    gq.relay()
    gv.begin_a()
    gq.pass_on()
    gv.begin_b()
    gk.relay()
    go.begin_a()
    gk.pass_on()
    gq.last()
    need("x")
    gq.ready()
    move("wq", wq, wq_out)
    row_sum = SmallSum(place, sums.at[0], small.at[0])

    def project(full, dst, squares_to=None):
        def one(r):
            near = span(r * half, half)
            value = dot(x[near, :], full[...])
            dst[near, :] = value.astype(BF)
            if squares_to is not None:
                stat[near, squares_to:squares_to + 1] = jnp.sum(value * value, axis=1, keepdims=True)

        loop(2, one)

    sums[0, 0] = jnp.zeros(sums.shape[2:], F32)
    project(wq, qp, heads)
    sums[0, 0, 0:1, :] = as_row(stat[:, heads:heads + 1])
    gv.relay()
    go.begin_b()
    gv.pass_on()
    gk.last()
    gk.ready()
    move("wk", wk, wk_out)
    project(wk, kp, heads + 1)
    sums[0, 0, 1:2, :] = as_row(stat[:, heads + 1:heads + 2])
    row_sum.begin()
    go.relay()
    gg.begin_a()
    gv.last()
    gv.ready()
    move("wv", wv, wv_out)
    project(wv, v)
    go.pass_on()
    gg.begin_b()
    totals = row_sum.end()
    inv_q = lax.rsqrt(as_col(totals[0:1, :]) / width + EPS)
    inv_k = lax.rsqrt(as_col(totals[1:2, :]) / width + EPS)
    stat[:, heads:heads + 1] = inv_q
    stat[:, heads + 1:heads + 2] = inv_k

    def rotate_head(hd):
        cols = span(hd * HD, HD)
        qr[:, cols] = turn(qp[:, cols].astype(F32) * inv_q * q_gain[:, cols], cos_tab[...], sin_tab[...]).astype(BF)
        kr[:, cols] = turn(kp[:, cols].astype(F32) * inv_k * k_gain[:, cols], cos_tab[...], sin_tab[...]).astype(BF)

    loop(heads, rotate_head)
    go.last()
    block = rows // 4
    lane_at = lax.broadcasted_iota(jnp.int32, (block, HD), 1)

    def allowed_at(rb):
        near, keys = slice(rb * block, (rb + 1) * block), (rb + 1) * block
        t_at = lax.broadcasted_iota(jnp.int32, (block, keys), 0) + rb * block
        s_at = lax.broadcasted_iota(jnp.int32, (block, keys), 1)
        return near, keys, (side[near, 0:1] == seg[:, 0:keys].astype(F32)) & (s_at <= t_at)

    def attend(rb):
        near, keys, allowed = allowed_at(rb)

        def one(hd):
            cols = span(hd * HD, HD)
            scores = jnp.where(allowed, dot_nt(qr[near, cols], kr[0:keys, cols]) * scale, -1e30)
            top = jnp.max(scores, axis=1, keepdims=True)
            weights = jnp.exp(scores - top)
            norm = jnp.sum(weights, axis=1, keepdims=True)
            stat[near, :] = jnp.where(lane_at == hd, top + jnp.log(norm), stat[near, :])
            o[near, cols] = dot((weights / norm).astype(BF), v[0:keys, cols]).astype(BF)

        loop(heads, one)

    wide = width // 8

    def columns(bits):
        return span(place.block(bits) * wide, wide)

    def by_rows(flow, k):
        return span(k // 4 * half, half), columns(2 * (k % 4) + flow)

    def took_slot(flow, k):
        return took.at[flow, k]

    sum_attn = RowSum(place, part, took_slot, raw_a, row_sems.at[0], by_rows, 8)

    def project_out(r):
        near = slice(r * half, (r + 1) * half)

        def one(i):
            part[near, columns(i)] = dot(o[near, :], wo[:, columns(i)]).astype(BF)

        loop(8, one)

    def mid(r):
        tile = rows // 8

        def one(at):
            near = span(at * tile, tile)
            raw = raw_a[near, :].astype(F32)
            inv = lax.rsqrt(jnp.mean(raw * raw, axis=1, keepdims=True) + EPS)
            h[near, :] = (x[near, :].astype(F32) + raw * inv * a_gain[...]).astype(BF)

        loop(4, one, 4 * r)

    def gate_part(r, first, count):
        near = slice(r * half, (r + 1) * half)

        def one(at):
            cols = span(at * UNIT, UNIT)
            gate[near, cols] = dot(h[near, :], wg[:, cols]).astype(BF)

        loop(count, one, first)

    def up_half(r, first, count):
        near = slice(r * half, (r + 1) * half)

        def one(at):
            cols = span(at * UNIT, UNIT)
            value = dot(h[near, :], wu[:, cols])
            up[near, cols] = value.astype(BF)
            pre = gate[near, cols].astype(F32)
            act[near, cols] = (pre * jax.nn.sigmoid(pre) * value).astype(BF)

        loop(count, one, first)

    attend(0)
    attend(1)
    go.ready()
    move("wo", wo, wo_out)
    project_out(0)
    sum_attn.push(0)
    sum_attn.push(1)
    gu.begin_a()
    attend(2)
    sum_attn.tick(1, 0)
    sum_attn.push(2)
    attend(3)
    sum_attn.tick(2, 0)
    sum_attn.push(3)
    project_out(1)
    gg.relay()
    gu.begin_b()
    sum_attn.push(4)
    sum_attn.tick(3, 0)
    gg.pass_on()

    def attn_both(t):
        sum_attn.push(t + 1)
        sum_attn.both(t, 3)

    attn_both(4)
    attn_both(5)
    gu.relay()
    gd.begin_a()
    loop(2, attn_both, 6)
    gg.last()
    gd.begin_b()
    loop(2, attn_both, 8)
    gg.ready()
    mid(0)

    def gate_and_tick(i):
        gate_part(0, i * (n_ff // 2), n_ff // 2)
        sum_attn.tick(7 + i, 1)

    loop(2, gate_and_tick)
    gu.pass_on()
    sum_attn.tick(9, 1)
    mid(1)
    gate_part(1, 0, n_ff)
    gu.last()
    gu.ready()
    up_half(0, 0, n_ff)
    sum_attn.sent()
    sum_ffn = RowSum(place, part, took_slot, d_ffn, row_sems.at[1], by_rows, 8)

    def project_down(k):
        near = span(k // 4 * half, half)

        def one(flow):
            cols = columns(2 * (k % 4) + flow)
            part[near, cols] = dot(act[near, :], wd[:, cols]).astype(BF)

        loop(2, one)
        sum_ffn.push(k)

    gd.own_copy().wait()
    gd.arrived(6)
    project_down(0)
    need("wq", "wk", "wv", "wo")
    for g in (gq, gk, gv, go):
        g.drain()
    up_half(1, 0, n_ff // 2)
    gd.relay()
    sum_ffn.tick(1, 0)
    up_half(1, n_ff // 2, n_ff // 2)
    project_down(4)
    gd.pass_on()
    gd.arrived(7, 8, 10, 11)
    project_down(1)
    sum_ffn.both(2, 1)
    project_down(2)
    project_down(5)
    sum_ffn.both(3, 1)
    project_down(6)
    gd.last()
    gd.arrived(9)
    project_down(3)
    sum_ffn.tick(4, 0)
    project_down(7)
    sum_ffn.tick(3, 1)

    def ffn_both(t):
        sum_ffn.both(t, 1)

    loop(5, ffn_both, 5)
    sum_ffn.sent(0)
    for g in (gg, gu, gd):
        g.drain()
    need("cot")

    gains[...] = jnp.zeros(gains.shape, F32)
    tile = rows // 8

    def back_ffn(at):
        near = span(at * tile, tile)
        raw = d_ffn[near, :].astype(F32)
        alive = side[near, 1:2]
        dy = alive * cot[near, :].astype(F32)
        inv = lax.rsqrt(jnp.mean(raw * raw, axis=1, keepdims=True) + EPS)
        normed = raw * inv
        gains[0:1, :] += jnp.sum(dy * normed, axis=0, keepdims=True)
        value = (alive * (h[near, :].astype(F32) + normed * f_gain[...])).astype(BF)
        for q in range(width // local):
            wv[span(q * rows + at * tile, tile), :] = value[:, q * local:(q + 1) * local]
        gained = f_gain[...] * dy
        mean = jnp.mean(gained * raw, axis=1, keepdims=True)
        d_ffn[near, :] = (inv * gained - raw * inv**3 * mean).astype(BF)

    def flip(src):
        def one(at):
            parity = at % 2
            own = 1 - (parity + place.c - 2 * parity * place.c)
            turned[span((4 * own + at // 2) * wide, wide), :] = src[:, span(at * wide, wide)].T

        loop(8, one)

    scatter = Scatter(place, (wq, wk, wv, wo), (flat_out, tall_out), s_sems, s_out, n_ff, n_local)

    def back_act(r, first, count):
        near = slice(r * half, (r + 1) * half)

        def one(at):
            cols = span(at * UNIT, UNIT)
            d_act = dot_nt(d_ffn[near, :], wd[cols, :])
            pre, upper = gate[near, cols].astype(F32), up[near, cols].astype(F32)
            sig = jax.nn.sigmoid(pre)
            up[near, cols] = (d_act * pre * sig).astype(BF)
            gate[near, cols] = (d_act * upper * sig * (1.0 + pre * (1.0 - sig))).astype(BF)

        loop(count, one, first)

    raw_h = x
    sum_back = RowSum(place, part, took_slot, raw_h, row_sems.at[2], by_rows, 8)

    def back_gate(r, first):
        near = slice(r * half, (r + 1) * half)

        def one(i):
            value = dot_nt(gate[near, :], wg[columns(i), :]) + dot_nt(up[near, :], wu[columns(i), :])
            part[near, columns(i)] = value.astype(BF)

        loop(4, one, first)

    dq, dk, dv = (wu.at[2 * rows:3 * rows, i * local:(i + 1) * local] for i in range(1, 4))
    others = wu.at[2 * rows:3 * rows, :]
    d_heads = wu.at[3 * rows:4 * rows, 0:local]
    loop(4, back_ffn)
    back_act(0, 0, n_ff // 2)
    sum_ffn.tick(9, 1)
    back_act(0, n_ff // 2, n_ff // 2)
    back_gate(0, 0)
    loop(2, sum_back.push)
    sum_ffn.sent(1)
    loop(4, back_ffn, 4)
    for q in range(width // local):
        move(f"hidden{q}", wv.at[q * rows:(q + 1) * rows, :], hidden_out.at[:, q * local:(q + 1) * local])
    flip(d_ffn)
    d_attn = wu.at[rows:2 * rows, :]

    def back_attn(at):
        near = span(at * tile, tile)
        raw = raw_a[near, :].astype(F32)
        dh = side[near, 1:2] * cot[near, :].astype(F32) + raw_h[near, :].astype(F32)
        inv = lax.rsqrt(jnp.mean(raw * raw, axis=1, keepdims=True) + EPS)
        gains[1:2, :] += jnp.sum(dh * raw * inv, axis=0, keepdims=True)
        gained = a_gain[...] * dh
        mean = jnp.mean(gained * raw, axis=1, keepdims=True)
        d_attn[near, :] = (inv * gained - raw * inv**3 * mean).astype(BF)

    def back_out(r):
        near = slice(r * half, (r + 1) * half)
        loop(4, back_attn, 4 * r)
        d_heads[near, :] = dot_nt(d_attn[near, :], wg[0:local, :]).astype(BF)

    def back_head(hd):
        cols = span(hd * HD, HD)
        dk_sum[...] = jnp.zeros(dk_sum.shape, F32)
        dv_sum[...] = jnp.zeros(dv_sum.shape, F32)
        for rb in range(4):
            near, keys, allowed = allowed_at(rb)
            lse = jnp.sum(jnp.where(lane_at == hd, stat[near, :], 0.0), axis=1, keepdims=True)
            scores = jnp.where(allowed, dot_nt(qr[near, cols], kr[0:keys, cols]) * scale, -1e30)
            probs = jnp.where(allowed, jnp.exp(scores - lse), 0.0)
            grad = d_heads[near, cols]
            d_prob = dot_nt(grad, v[0:keys, cols])
            delta = jnp.sum(grad.astype(F32) * o[near, cols].astype(F32), axis=1, keepdims=True)
            d_score = (probs * (d_prob - delta)).astype(BF)
            back = dot(d_score, kr[0:keys, cols]) * scale
            dq[near, cols] = turn_back(back, cos_tab[near, :], sin_tab[near, :]).astype(BF)
            dk_sum[0:keys, :] += dot_tn(d_score, qr[near, cols])
            dv_sum[0:keys, :] += dot_tn(probs.astype(BF), grad)
        dk[:, cols] = turn_back(dk_sum[...] * scale, cos_tab[...], sin_tab[...]).astype(BF)
        dv[:, cols] = dv_sum[...].astype(BF)

    row_sum_back = SmallSum(place, sums.at[1], small.at[1])
    normed = ((dq, qp, q_gain, heads), (dk, kp, k_gain, heads + 1))

    def begin_norms():
        sums[1, 0] = jnp.zeros(sums.shape[2:], F32)
        for at, (grad, raw, gain, lane_of) in enumerate(normed):
            both = grad[...].astype(F32) * raw[...].astype(F32)
            gains[2 + at:3 + at, 0:local] = jnp.sum(both * stat[:, lane_of:lane_of + 1], axis=0, keepdims=True)
            sums[1, 0, at:at + 1, :] = as_row(jnp.sum(gain[...] * both, axis=1, keepdims=True))
        row_sum_back.begin()

    def end_norms():
        totals = row_sum_back.end()
        for at, (grad, raw, gain, lane_of) in enumerate(normed):
            inv = stat[:, lane_of:lane_of + 1]
            mean = as_col(totals[at:at + 1, :]) / width
            gained = gain[...] * grad[...].astype(F32)
            grad[...] = (inv * gained - raw[...].astype(F32) * inv**3 * mean).astype(BF)

    raw_x = d_ffn
    sum_in = RowSum(place, part, took_slot, raw_x, row_sems.at[3], by_rows, 8)

    def back_in(r):
        near = slice(r * half, (r + 1) * half)

        def one(i):
            spot = columns(i)
            value = dot_nt(dq[near, :], wd[spot, 0:local]) + dot_nt(dk[near, :], wd[spot, local:2 * local])
            part[near, spot] = (value + dot_nt(dv[near, :], wd[spot, 2 * local:3 * local])).astype(BF)

        loop(8, one)
        loop(4, sum_in.push, 4 * r)

    def end_tile(at):
        near = span(at * tile, tile)
        dh = side[near, 1:2] * cot[near, :].astype(F32) + raw_h[near, :].astype(F32)
        raw_x[near, :] = (dh + raw_x[near, :].astype(F32)).astype(BF)

    partners = (place.sib, place.xn, place.yn)

    def gain_copy(at):
        return remote(
            gains.at[pl.ds(8 * at, 8), :], gains_got.at[at], gain_sems.at[0, at], gain_sems.at[1, at],
            {"dp": partners[at]},
        )

    def add_gains(at):
        gain_copy(at).wait_recv()
        gains[8 * at + 8:8 * at + 16, :] = gains[8 * at:8 * at + 8, :] + gains_got[at]
        if at < 2:
            gain_copy(at + 1).start()
        else:
            move("gains", gains.at[24:32, :], gains_out)

    def fetch():
        move("wq2", wq_out, wd.at[:, 0:local])
        move("wk2", wk_out, wd.at[:, local:2 * local])
        move("wv2", wv_out, wd.at[:, 2 * local:3 * local])
        move("wo2", wo_out, wg.at[0:local, :])
        move("x2", x_in, wu.at[0:rows, :])

    def after_tick(u):
        if u == 0:
            back_gate(0, 4)
            loop(2, sum_back.push, 2)
        elif u in (1, 2):
            back_act(1, (u - 1) * (n_ff // 2), n_ff // 2)
        elif u == 3:
            back_gate(1, 0)
            loop(2, sum_back.push, 4)
        elif u == 4:
            back_gate(1, 4)
            loop(2, sum_back.push, 6)
            fetch()
        elif u == 13:
            need("wo2")
            back_out(0)
        elif u == 18:
            sum_back.sent()
            back_out(1)
            others[:, 0:local] = o[...]
        elif u == 19:
            loop(heads // 2, back_head)
        elif u == 20:
            loop(heads - heads // 2, back_head, heads // 2)
            begin_norms()
        elif u == 21:
            end_norms()
            need("wq2", "wk2", "wv2", "x2")
            back_in(0)
        elif u == 22:
            sum_in.tick(1, 0)
            back_in(1)
            gain_copy(0).start()
        elif u in (24, 26, 28):
            add_gains((u - 24) // 2)
        elif u == 32:
            sum_in.sent()
            loop(8, end_tile)
            move("grad_in", raw_x, grad_in_out)

    def at_tick(u, act_on):
        @pl.when(u == act_on[0])
        def _():
            act_on[1]()

    def step(u):
        for when, src in ((n_ff, h), (3 * n_ff, d_attn), (3 * n_ff + n_local, wu.at[0:rows, :])):
            at_tick(u, (when, functools.partial(flip, src)))
        at_tick(u, (1, functools.partial(need, *(f"hidden{q}" for q in range(width // local)))))
        scatter.tick(u, turned, ffs, others)

        @pl.when((u >= 1) & (u <= 5))
        def _():
            sum_back.tick(u, 0)

        @pl.when((u >= 6) & (u <= 13))
        def _():
            odd = u % 2
            sum_back.tick((u - 4 + 9 * odd) // 2, 1 - odd)

        @pl.when((u >= 14) & (u <= 18))
        def _():
            sum_back.tick(u - 9, 1)

        @pl.when((u >= 23) & (u <= 32))
        def _():
            sum_in.tick(u - 21, 0)
            sum_in.tick(u - 23, 1)

        for when in (0, 1, 2, 3, 4, 13, 18, 19, 20, 21, 22, 24, 26, 28, 32):
            at_tick(u, (when, functools.partial(after_tick, when)))

    loop(scatter.count + 3, step)
    for at in range(3):
        gain_copy(at).wait_send()
    row_sum.drain()
    row_sum_back.drain()
    scatter.drain()
    need("gains", "grad_in")


def layer_call(n_mp, x, cot, weights, seg, live, freq, q_gain, k_gain, a_gain, f_gain):
    rows, width = x.shape
    local, ff = weights[0].shape[1], weights[4].shape[1]
    high, half = width // 8, rows // 2
    any_spec = pl.BlockSpec(memory_space=pl.ANY)
    vmem = pl.BlockSpec(memory_space=pltpu.VMEM)
    S, V, dma = jax.ShapeDtypeStruct, pltpu.VMEM, pltpu.SemaphoreType.DMA
    fulls = [(width, local)] * 3 + [(local, width)] + [(width, ff)] * 2 + [(ff, width)]
    outs = fulls[:4] + [
        (rows, width), (rows, width), (ff + local, high), (high, 2 * ff + 3 * local),
    ]
    return pl.pallas_call(
        functools.partial(layer_kernel, n_mp),
        out_shape=[S(s, BF) for s in outs] + [S((8, width), F32)],
        in_specs=[any_spec] * 9 + [vmem] * 7,
        out_specs=[any_spec] * 9,
        scratch_shapes=[V(s, BF) for s in fulls]
        + [V((rows, width), BF)]
        + [V((rows, local), BF)] * 6
        + [V((rows, HD), F32)] * 4
        + [V((rows, width), BF)] * 2
        + [V((3, rows, ff), BF)]
        + [V((rows, width), BF)] * 3
        + [V((2, 8, half, high), BF), V((width, rows), BF), V((rows, HD), F32), V((rows, HD), F32)]
        + [V((2, n_mp, 8, rows), F32), V((32, width), F32), V((3, 8, width), F32)]
        + [dma((7, 12)), dma((7, 12)), dma((7,)), dma((4, 4, 2, 8)), dma((2, 2, n_mp))]
        + [dma((2, 5, 4)), dma((2,)), dma((2, 3)), dma((20,))],
        compiler_params=pltpu.CompilerParams(
            collective_id=0, has_side_effects=True, vmem_limit_bytes=67043328,
        ),
    )(x, cot, *weights, seg, live, freq, q_gain, k_gain, a_gain, f_gain)


def with_kernel(n_mp, hidden_in, cotangent, segments, live_counts, *rest):
    weights, (query_gain, key_gain, attn_gain, ffn_gain) = rest[:7], rest[7:]
    local, ff = weights[0].shape[1], weights[4].shape[1]
    inv_freq = THETA ** (-(jnp.arange(HD // 2, dtype=F32) * (2.0 / HD)))
    freq = jnp.concatenate([inv_freq, inv_freq])[None]
    _, _, _, _, hidden_out, grad_in, flat, tall, gains = layer_call(
        n_mp, hidden_in, cotangent, weights, segments, live_counts[None], freq,
        query_gain[None], key_gain[None], attn_gain[None], ffn_gain[None],
    )

    def piece(first, count):
        return tall[:, first:first + count].astype(F32)

    return (
        hidden_out,
        grad_in.astype(F32),
        piece(2 * ff, local),
        piece(2 * ff + local, local),
        piece(2 * ff + 2 * local, local),
        flat[ff:].astype(F32),
        piece(0, ff),
        piece(ff, ff),
        flat[:ff].astype(F32),
        gains[2, :local],
        gains[3, :local],
        gains[1],
        gains[0],
    )


def doc_positions(seg_row):
    row_count = seg_row.shape[0]
    row_index = jnp.arange(row_count, dtype=jnp.int32)
    change = jnp.concatenate([jnp.ones((1,), dtype=bool), seg_row[1:] != seg_row[:-1]])
    doc_start = lax.cummax(jnp.where(change, row_index, jnp.zeros_like(row_index)), axis=0)
    return (row_index - doc_start).astype(jnp.float32)


def rotary_tables(positions, head_size):
    half_size = head_size // 2
    inv_freq = THETA ** (-(jnp.arange(half_size, dtype=jnp.float32) * (2.0 / head_size)))
    angles = positions[:, None] * inv_freq[None, :]
    return (jnp.cos(angles)[:, None, :], jnp.sin(angles)[:, None, :])


def rotate(values, cos_tab, sin_tab):
    half_size = values.shape[2] // 2
    first_half = values[:, :, :half_size]
    second_half = values[:, :, half_size:]
    return jnp.concatenate(
        [
            first_half * cos_tab - second_half * sin_tab,
            second_half * cos_tab + first_half * sin_tab,
        ],
        axis=2,
    )


def rotate_back(grads, cos_tab, sin_tab):
    half_size = grads.shape[2] // 2
    first_half = grads[:, :, :half_size]
    second_half = grads[:, :, half_size:]
    return jnp.concatenate(
        [
            first_half * cos_tab + second_half * sin_tab,
            second_half * cos_tab - first_half * sin_tab,
        ],
        axis=2,
    )


def block_mask(seg_row, offset, block_rows):
    row_index = jnp.arange(seg_row.shape[0])
    same = seg_row[offset : offset + block_rows, None] == seg_row[None, :]
    return same & (row_index[:, None] >= row_index[None, :])


def block_scores(q_blk, k_bf, allowed, score_scale):
    scores = (
        jnp.einsum("qhe,khe->hqk", q_blk, k_bf, preferred_element_type=jnp.float32) * score_scale
    )
    return jnp.where(allowed[None], scores, jnp.float32(-1e30))


def attend_forward(q_bf, k_bf, v_bf, seg_row, score_scale):
    row_count = q_bf.shape[0]
    block_rows = min(512, row_count)
    allowed = block_mask(seg_row, 0, block_rows)
    scores = block_scores(q_bf, k_bf, allowed, score_scale)
    row_max = jnp.max(scores, axis=2, keepdims=True)
    lse = row_max + jnp.log(jnp.sum(jnp.exp(scores - row_max), axis=2, keepdims=True))
    probs = jnp.exp(scores - lse).astype(jnp.bfloat16)
    outputs = jnp.einsum("hqk,khe->qhe", probs, v_bf, preferred_element_type=jnp.float32)
    lse_parts = [lse]
    return (outputs.astype(jnp.bfloat16), lse_parts)


def attend_backward(q_bf, k_bf, v_bf, o_bf, do_bf, lse_parts, seg_row, score_scale):
    row_count = q_bf.shape[0]
    block_rows = min(512, row_count)
    dq_parts = []
    dk_acc = jnp.zeros(k_bf.shape, jnp.float32)
    dv_acc = jnp.zeros(v_bf.shape, jnp.float32)
    for part_index, offset in enumerate(range(0, row_count, block_rows)):
        allowed = block_mask(seg_row, offset, block_rows)
        scores = block_scores(q_bf, k_bf, allowed, score_scale)
        probs = jnp.exp(scores - lse_parts[part_index])
        probs_bf = probs.astype(jnp.bfloat16)
        dprob = jnp.einsum("qhe,khe->hqk", do_bf, v_bf, preferred_element_type=jnp.float32)
        delta = jnp.transpose(
            jnp.sum(do_bf.astype(jnp.float32) * o_bf.astype(jnp.float32), axis=2)
        )[:, :, None]
        dscore = (probs * (dprob - delta)).astype(jnp.bfloat16)
        dq_parts.append(
            jnp.einsum("hqk,khe->qhe", dscore, k_bf, preferred_element_type=jnp.float32)
            * score_scale
        )
        dk_acc = (
            jnp.einsum("hqk,qhe->khe", dscore, q_bf, preferred_element_type=jnp.float32)
            * score_scale
        )
        dv_acc = jnp.einsum("hqk,qhe->khe", probs_bf, do_bf, preferred_element_type=jnp.float32)
    return (dq_parts[0], dk_acc, dv_acc.astype(jnp.bfloat16))


def scatter_grad(grad, axis_name, scatter_dimension, tiled):
    total = lax.psum_scatter(
        grad.astype(jnp.bfloat16), axis_name, scatter_dimension=scatter_dimension, tiled=tiled
    )
    return total.astype(jnp.float32)


def sum_parts(part, axis_name):
    own = lax.psum_scatter(
        part.astype(jnp.bfloat16), axis_name, scatter_dimension=0, tiled=True
    )
    return lax.all_gather(own, axis_name, axis=0, tiled=True).astype(jnp.float32)


def norm_back(raw, inv_scale, gained, row_sums, width):
    return inv_scale * gained - raw * inv_scale**3 * (row_sums[:, None] / width)


def on_device(
    hidden_in,
    cotangent,
    segments,
    live_counts,
    w_query,
    w_key,
    w_value,
    w_output,
    w_gate,
    w_up,
    w_down,
    query_gain,
    key_gain,
    attn_gain,
    ffn_gain,
):
    gathered = (
        lax.all_gather(w_query, "dp", axis=0, tiled=True),
        lax.all_gather(w_key, "dp", axis=0, tiled=True),
        lax.all_gather(w_value, "dp", axis=0, tiled=True),
        lax.all_gather(w_output, "dp", axis=1, tiled=True),
        lax.all_gather(w_gate, "dp", axis=0, tiled=True),
        lax.all_gather(w_up, "dp", axis=0, tiled=True),
        lax.all_gather(w_down, "dp", axis=1, tiled=True),
    )
    wq_full, wk_full, wv_full, wo_full, wg_full, wu_full, wd_full = gathered
    seg_row = segments[0]
    live_n = live_counts[0]
    row_count, width = hidden_in.shape
    local_width = wq_full.shape[1]
    heads_here = local_width // HD
    score_scale = 1.0 / math.sqrt(HD)
    live_mask = (jnp.arange(row_count, dtype=jnp.int32) < live_n).astype(jnp.float32)[:, None]
    cos_tab, sin_tab = rotary_tables(doc_positions(seg_row), HD)
    q_proj = jnp.dot(hidden_in, wq_full, preferred_element_type=jnp.float32)
    k_proj = jnp.dot(hidden_in, wk_full, preferred_element_type=jnp.float32)
    v_bf = jnp.dot(hidden_in, wv_full, preferred_element_type=jnp.float32).astype(jnp.bfloat16)
    sq_query, sq_key = lax.psum(
        (jnp.sum(q_proj * q_proj, axis=1), jnp.sum(k_proj * k_proj, axis=1)), "mp"
    )
    inv_q = lax.rsqrt(sq_query[:, None] / width + EPS)
    inv_k = lax.rsqrt(sq_key[:, None] / width + EPS)
    q_rot = rotate(
        (q_proj * inv_q * query_gain).reshape(row_count, heads_here, HD), cos_tab, sin_tab
    ).astype(jnp.bfloat16)
    k_rot = rotate(
        (k_proj * inv_k * key_gain).reshape(row_count, heads_here, HD), cos_tab, sin_tab
    ).astype(jnp.bfloat16)
    v_heads = v_bf.reshape(row_count, heads_here, HD)
    o_bf, lse_parts = attend_forward(q_rot, k_rot, v_heads, seg_row, score_scale)
    o_flat = o_bf.reshape(row_count, local_width)
    attn_raw = sum_parts(jnp.dot(o_flat, wo_full, preferred_element_type=jnp.float32), "mp")
    inv_a = lax.rsqrt(jnp.mean(attn_raw * attn_raw, axis=1, keepdims=True) + EPS)
    h_mid = hidden_in.astype(jnp.float32) + attn_raw * inv_a * attn_gain
    h_bf = h_mid.astype(jnp.bfloat16)
    gate_pre = jnp.dot(h_bf, wg_full, preferred_element_type=jnp.float32)
    up_pre = jnp.dot(h_bf, wu_full, preferred_element_type=jnp.float32)
    act_bf = (jax.nn.silu(gate_pre) * up_pre).astype(jnp.bfloat16)
    ffn_raw = sum_parts(jnp.dot(act_bf, wd_full, preferred_element_type=jnp.float32), "mp")
    inv_f = lax.rsqrt(jnp.mean(ffn_raw * ffn_raw, axis=1, keepdims=True) + EPS)
    hidden_out = (live_mask * (h_mid + ffn_raw * inv_f * ffn_gain)).astype(jnp.bfloat16)
    wq_back, wk_back, wv_back, wo_back, wg_back, wu_back, wd_back = gathered
    dy = live_mask * cotangent.astype(jnp.float32)
    g_ffn_gain = jnp.sum(dy * ffn_raw * inv_f, axis=0)
    gained_f = ffn_gain * dy
    d_ffn = norm_back(ffn_raw, inv_f, gained_f, jnp.sum(gained_f * ffn_raw, axis=1), width).astype(
        jnp.bfloat16
    )
    d_act = jnp.dot(d_ffn, wd_back.T, preferred_element_type=jnp.float32)
    sig = jax.nn.sigmoid(gate_pre)
    d_up = (d_act * gate_pre * sig).astype(jnp.bfloat16)
    d_gate = (d_act * up_pre * sig * (1.0 + gate_pre * (1.0 - sig))).astype(jnp.bfloat16)
    ffn_part = jnp.dot(d_gate, wg_back.T, preferred_element_type=jnp.float32) + jnp.dot(
        d_up, wu_back.T, preferred_element_type=jnp.float32
    )
    dh = dy + sum_parts(ffn_part, "mp")
    g_down = jnp.dot(act_bf.T, d_ffn, preferred_element_type=jnp.float32)
    g_gate = jnp.dot(h_bf.T, d_gate, preferred_element_type=jnp.float32)
    g_up = jnp.dot(h_bf.T, d_up, preferred_element_type=jnp.float32)
    g_attn_gain = jnp.sum(dh * attn_raw * inv_a, axis=0)
    gained_a = attn_gain * dh
    d_attn = norm_back(
        attn_raw, inv_a, gained_a, jnp.sum(gained_a * attn_raw, axis=1), width
    ).astype(jnp.bfloat16)
    d_heads = jnp.dot(d_attn, wo_back.T, preferred_element_type=jnp.float32).astype(jnp.bfloat16)
    g_output = jnp.dot(o_flat.T, d_attn, preferred_element_type=jnp.float32)
    dq_rot, dk_rot, d_val = attend_backward(
        q_rot,
        k_rot,
        v_heads,
        o_bf,
        d_heads.reshape(row_count, heads_here, HD),
        lse_parts,
        seg_row,
        score_scale,
    )
    dq_norm = rotate_back(dq_rot, cos_tab, sin_tab).reshape(row_count, local_width)
    dk_norm = rotate_back(dk_rot, cos_tab, sin_tab).reshape(row_count, local_width)
    g_query_gain = jnp.sum(dq_norm * q_proj * inv_q, axis=0)
    g_key_gain = jnp.sum(dk_norm * k_proj * inv_k, axis=0)
    gained_q = query_gain * dq_norm
    gained_k = key_gain * dk_norm
    sums_query, sums_key = lax.psum(
        (jnp.sum(gained_q * q_proj, axis=1), jnp.sum(gained_k * k_proj, axis=1)), "mp"
    )
    dq_bf = norm_back(q_proj, inv_q, gained_q, sums_query, width).astype(jnp.bfloat16)
    dk_bf = norm_back(k_proj, inv_k, gained_k, sums_key, width).astype(jnp.bfloat16)
    dv_bf = d_val.reshape(row_count, local_width)
    input_part = (
        jnp.dot(dq_bf, wq_back.T, preferred_element_type=jnp.float32)
        + jnp.dot(dk_bf, wk_back.T, preferred_element_type=jnp.float32)
        + jnp.dot(dv_bf, wv_back.T, preferred_element_type=jnp.float32)
    )
    grad_in = dh + sum_parts(input_part, "mp")
    g_query = jnp.dot(hidden_in.T, dq_bf, preferred_element_type=jnp.float32)
    g_key = jnp.dot(hidden_in.T, dk_bf, preferred_element_type=jnp.float32)
    g_value = jnp.dot(hidden_in.T, dv_bf, preferred_element_type=jnp.float32)
    owned = (
        scatter_grad(g_query, "dp", scatter_dimension=0, tiled=True),
        scatter_grad(g_key, "dp", scatter_dimension=0, tiled=True),
        scatter_grad(g_value, "dp", scatter_dimension=0, tiled=True),
        scatter_grad(g_output, "dp", scatter_dimension=1, tiled=True),
        scatter_grad(g_gate, "dp", scatter_dimension=0, tiled=True),
        scatter_grad(g_up, "dp", scatter_dimension=0, tiled=True),
        scatter_grad(g_down, "dp", scatter_dimension=1, tiled=True),
    )
    gain_totals = lax.psum((g_query_gain, g_key_gain, g_attn_gain, g_ffn_gain), "dp")
    return (
        hidden_out,
        grad_in,
        owned[0],
        owned[1],
        owned[2],
        owned[3],
        owned[4],
        owned[5],
        owned[6],
        gain_totals[0],
        gain_totals[1],
        gain_totals[2],
        gain_totals[3],
    )


def kernel_fits(mesh, hidden_in, segments, w_query, w_gate):
    n_dp, n_mp = mesh.shape["dp"], mesh.shape["mp"]
    rows, width = hidden_in.shape[0] // n_dp, hidden_in.shape[1]
    local, ff = w_query.shape[1] // n_mp, w_gate.shape[1] // n_mp
    even = width % (8 * UNIT) == 0 and local % UNIT == 0 and ff % (2 * UNIT) == 0
    fits = rows == UNIT * 2 and width == 8 * UNIT and local == rows and ff == width
    return n_dp == 8 and n_mp >= 2 and even and fits


def solution(mesh):
    in_specs = (
        P("dp", None),
        P("dp", None),
        P("dp", None),
        P("dp"),
        P("dp", "mp"),
        P("dp", "mp"),
        P("dp", "mp"),
        P("mp", "dp"),
        P("dp", "mp"),
        P("dp", "mp"),
        P("mp", "dp"),
        P("mp"),
        P("mp"),
        P(),
        P(),
    )
    out_specs = (
        P("dp", None),
        P("dp", None),
        P("dp", "mp"),
        P("dp", "mp"),
        P("dp", "mp"),
        P("mp", "dp"),
        P("dp", "mp"),
        P("dp", "mp"),
        P("mp", "dp"),
        P("mp"),
        P("mp"),
        P(),
        P(),
    )

    def step(*args):
        if kernel_fits(mesh, args[0], args[2], args[4], args[8]):
            body = functools.partial(with_kernel, mesh.shape["mp"])
        else:
            body = on_device
        return jax.shard_map(
            body, mesh=mesh, in_specs=in_specs, out_specs=out_specs, check_vma=False
        )(*args)

    return step
```

```python
import functools
import math

import jax
import jax.numpy as jnp
from jax import lax
from jax.experimental import pallas as pl
from jax.experimental.pallas import tpu as pltpu
from jax.sharding import PartitionSpec as P

HD = 128
EPS = 1e-06
THETA = 500000.0
UNIT = 256
BF = jnp.bfloat16
F32 = jnp.float32


def dot(a, b):
    return jnp.dot(a, b, preferred_element_type=F32)


def dot_nt(a, b):
    return lax.dot_general(a, b, (((1,), (1,)), ((), ())), preferred_element_type=F32)


def dot_tn(a, b):
    return lax.dot_general(a, b, (((0,), (0,)), ((), ())), preferred_element_type=F32)


def span(start, size):
    return pl.ds(start if isinstance(start, int) else pl.multiple_of(start, size), size)


def loop(count, body, first=0):
    def step(at, carry):
        body(at)
        return carry

    lax.fori_loop(first, first + count, step, 0)


def remote(src, dst, send, recv, device):
    return pltpu.make_async_remote_copy(
        src_ref=src, dst_ref=dst, send_sem=send, recv_sem=recv,
        device_id=device, device_id_type=pl.DeviceIdType.MESH,
    )


class Place:
    def __init__(self, n_mp):
        self.dp, self.z = lax.axis_index("dp"), lax.axis_index("mp")
        self.n_mp, self.end = n_mp, n_mp - 1
        self.c = lax.rem(self.dp, 2)
        self.x = lax.rem(self.dp // 2, 2)
        self.y = self.dp // 4
        self.sib, self.xn, self.yn, self.dg = (self.block(i) for i in (1, 2, 4, 6))

    def block(self, i):
        i0, i1, i2 = i % 2, (i // 2) % 2, i // 4
        c, x, y = (a + b - 2 * a * b for a, b in ((self.c, i0), (self.x, i1), (self.y, i2)))
        return 4 * y + 2 * x + c

    def barrier(self):
        sem = pltpu.get_barrier_semaphore()
        mesh = pl.DeviceIdType.MESH
        for dp in (self.sib, self.xn, self.yn):
            pl.semaphore_signal(sem, inc=1, device_id={"dp": dp}, device_id_type=mesh)
        for step in range(1, self.n_mp):
            z = lax.rem(self.z + step, self.n_mp)
            pl.semaphore_signal(sem, inc=1, device_id={"mp": z}, device_id_type=mesh)
        pl.semaphore_wait(sem, 3 + self.n_mp - 1)


class Gather:
    def __init__(self, place, src, full, by_rows, send, recv, local):
        self.place, self.src, self.full, self.by_rows = place, src, full, by_rows
        self.sends, self.recvs, self.local = send, recv, local
        self.rows, self.cols = src.shape
        self.half = self.rows // 2

    def spot(self, owner, part=None):
        size = self.rows if self.by_rows else self.cols
        first, count = (0, size) if part is None else (part * size // 2, size // 2)
        near = pl.ds(pl.multiple_of(owner * size + first, size // 2), count)
        return self.full.at[near, :] if self.by_rows else self.full.at[:, near]

    def mine(self, part):
        size = (self.rows if self.by_rows else self.cols) // 2
        near = pl.ds(part * size, size)
        return self.src.at[near, :] if self.by_rows else self.src.at[:, near]

    def copies(self):
        p = self.place
        table = {
            0: (self.mine(0), p.dp, 0, p.xn, p.xn),
            1: (self.mine(1), p.dp, 1, p.xn, p.xn),
            2: (self.mine(0), p.dp, 0, p.yn, p.yn),
            3: (self.mine(1), p.dp, 1, p.yn, p.yn),
            6: (self.src, p.dp, None, p.sib, p.sib),
        }
        for kind, owner, part, target, arrives in (
            (4, p.yn, 1, p.xn, p.dg), (5, p.xn, 0, p.yn, p.dg),
            (7, p.xn, 0, p.sib, p.block(3)), (10, p.xn, 1, p.sib, p.block(3)),
            (8, p.yn, 1, p.sib, p.block(5)), (11, p.yn, 0, p.sib, p.block(5)),
            (9, p.dg, None, p.sib, p.block(7)),
        ):
            table[kind] = (self.spot(owner, part), owner, part, target, arrives)
        return table

    def copy(self, kind):
        src, owner, part, target, _ = self.copies()[kind]
        return remote(src, self.spot(owner, part), self.sends.at[kind], self.recvs.at[kind], {"dp": target})

    def start(self, *kinds):
        for kind in kinds:
            self.copy(kind).start()

    def arrived(self, *kinds):
        for kind in kinds:
            _, _, part, target, owner = self.copies()[kind]
            spot = self.spot(owner, part)
            remote(spot, spot, self.sends.at[kind], self.recvs.at[kind], {"dp": target}).wait_recv()

    def own_copy(self):
        return pltpu.make_async_copy(self.src, self.spot(self.place.dp), self.local)

    def begin_a(self):
        self.start(0, 3)

    def begin_b(self):
        self.start(1, 2, 6)
        self.own_copy().start()

    def relay(self):
        self.arrived(0)
        self.start(5, 7)
        self.arrived(3)
        self.start(4, 8)

    def pass_on(self):
        self.arrived(1)
        self.start(10)
        self.arrived(2)
        self.start(11)

    def last(self):
        self.arrived(5, 4)
        self.start(9)

    def ready(self):
        self.own_copy().wait()
        self.arrived(6, 7, 8, 9, 10, 11)

    def drain(self):
        for kind in range(12):
            self.copy(kind).wait_send()


class RowSum:
    def __init__(self, place, part, took, total, sems, chunk_at, count):
        self.place, self.part, self.took, self.total, self.sems = place, part, took, total, sems
        self.chunk_at = chunk_at
        self.count = count

    def spot(self, ref, flow, k):
        return ref.at[self.chunk_at(flow, k)]

    def at(self, flow):
        return self.place.z + flow * (self.place.end - 2 * self.place.z)

    def forth(self, flow, k):
        return remote(
            self.spot(self.part, flow, k), self.took(flow, k),
            self.sems.at[0, flow, k], self.sems.at[1, flow, k], {"mp": self.place.z + 1 - 2 * flow},
        )

    def back(self, flow, k):
        spot = self.spot(self.total, flow, k)
        return remote(spot, spot, self.sems.at[2, flow, k], self.sems.at[3, flow, k], {"mp": self.place.z - 1 + 2 * flow})

    def push(self, k):
        if isinstance(k, int) and k >= self.count:
            return

        def one(flow):
            @pl.when((self.at(flow) == 0) & (k < self.count))
            def _():
                self.forth(flow, k).start()

        loop(2, one)

    def add(self, dst, flow, k):
        mine, to, more = self.spot(self.part, flow, k), self.spot(dst, flow, k), self.took(flow, k)
        step = mine.shape[0] // 4

        def one(at):
            near = span(at * step, step)
            to[near, :] = (mine[near, :].astype(F32) + more[near, :].astype(F32)).astype(BF)

        loop(4, one)

    def tick(self, t, half):
        end, count = self.place.end, self.count // 2
        if isinstance(t, int) and t >= count + 2 * end:
            return

        def gather(flow):
            at = self.at(flow)
            k = t - at

            @pl.when((at > 0) & (k >= 0) & (k < count))
            def _():
                chunk = half * count + k
                self.forth(flow, chunk).wait_recv()

                @pl.when(at < end)
                def _():
                    self.add(self.part, flow, chunk)
                    self.forth(flow, chunk).start()

                @pl.when(at == end)
                def _():
                    self.add(self.total, flow, chunk)
                    self.back(flow, chunk).start()

        def bring_back(flow):
            at = self.at(flow)
            k = t - 2 * end + at

            @pl.when((at < end) & (k >= 0) & (k < count))
            def _():
                chunk = half * count + k
                self.back(flow, chunk).wait_recv()

                @pl.when(at > 0)
                def _():
                    self.back(flow, chunk).start()

        if not isinstance(t, int) or t < count + end:
            loop(2, gather)
        if not isinstance(t, int) or t >= end + 1:
            loop(2, bring_back)

    def both(self, t, lag):
        self.tick(t, 0)
        self.tick(t - lag, 1)

    def sent(self, half=None):
        first, count = (0, self.count) if half is None else (half * self.count // 2, self.count // 2)
        for flow in range(2):
            at = self.at(flow)

            def one(k):
                @pl.when(at < self.place.end)
                def _():
                    self.forth(flow, k).wait_send()

                @pl.when(at > 0)
                def _():
                    self.back(flow, k).wait_send()

            loop(count, one, first)


class SmallSum:
    def __init__(self, place, slots, sems):
        self.place, self.slots, self.sems = place, slots, sems

    def copy(self, step):
        p = self.place
        return remote(
            self.slots.at[0], self.slots.at[step], self.sems.at[0, step], self.sems.at[1, step],
            {"mp": lax.rem(p.z + step, p.n_mp)},
        )

    def begin(self):
        for step in range(1, self.place.n_mp):
            self.copy(step).start()

    def end(self):
        for step in range(1, self.place.n_mp):
            self.copy(step).wait_recv()
        total = self.slots[0]
        for step in range(1, self.place.n_mp):
            total = total + self.slots[step]
        return total

    def drain(self):
        for step in range(1, self.place.n_mp):
            self.copy(step).wait_send()


class Scatter:
    slots = 6

    def __init__(self, place, tall, broad, outs, sems, out_sems, n_ff, n_local):
        self.place, self.tall, self.broad, self.outs = place, tall, broad, outs
        self.n_ff, self.n_local, self.early = n_ff, n_local, 3 * n_ff
        self.count = 3 * n_ff + 4 * n_local
        self.sems, self.out_sems = sems, out_sems
        self.rows = broad.shape[1] // 8
        self.half = self.rows // 2

    def made(self, u, own):
        return self.tall.at[span((u % 2) * 4 * self.rows, 4 * self.rows), span(own * UNIT, UNIT)]

    def got(self, u, chip=None):
        s = u % 4
        first, size = (8 + s % 2 * 4) * self.rows, 4 * self.rows
        if chip is not None:
            first, size = first + chip * self.rows, self.rows
        return self.tall.at[span(first, size), span(s // 2 * UNIT, UNIT)]

    def sums(self, which, u, to, then=None):
        first, size = (16 + u % self.slots * 2 + to) * self.rows, self.rows
        if then is not None:
            first, size = first + then * self.half, self.half
        return self.tall.at[span(first, size), pl.ds(which * UNIT, UNIT)]

    def ended(self, which, u):
        first = (16 + 2 * self.slots) * self.rows + u % self.slots * self.half
        return self.tall.at[span(first, self.half), pl.ds(which * UNIT, UNIT)]

    def met(self, which, u):
        s = u % self.slots
        return self.broad.at[span(s % 2 * self.rows, self.rows), span((s // 2 * 2 + which) * UNIT, UNIT)]

    def done(self, u):
        return self.broad.at[span((u % 2) * self.rows, self.rows), span(self.slots * UNIT, UNIT)]

    def send(self, kind, u):
        p, s = self.place, u % self.slots
        src, dst, target = {
            0: lambda: (self.made(u, 0), self.got(u), p.sib),
            1: lambda: (self.sums(0, u, 1 - p.x), self.met(0, u), p.xn),
            2: lambda: (self.sums(1, u, 1 - p.y), self.met(1, u), p.yn),
            3: lambda: (self.sums(0, u, p.x, 1 - p.y), self.ended(0, u), p.yn),
            4: lambda: (self.sums(1, u, p.y, 1 - p.x), self.ended(1, u), p.xn),
        }[kind]()
        return remote(src, dst, self.sems.at[0, kind, s], self.sems.at[1, kind, s], {"dp": target})

    def product(self, u, turned, right, at):
        cols = span(at * UNIT, UNIT)

        def one(own):
            near = span(own * 4 * self.rows, 4 * self.rows)
            self.made(u, own)[...] = dot(turned[near, :], right[:, cols]).astype(BF)

            @pl.when(own == 0)
            def _():
                self.send(0, u).start()

        loop(2, one)

    def across(self, u):
        self.send(0, u).wait_recv()
        self.send(0, u).wait_send()
        mine = self.made(u, 1)

        def add(chip):
            y_to, x_to = chip // 2, chip % 2
            more = self.got(u, chip)
            for which, spot in ((0, self.sums(0, u, x_to, y_to)), (1, self.sums(1, u, y_to, x_to))):
                near = slice(which * self.half, (which + 1) * self.half)
                own = mine[span(chip * self.rows + which * self.half, self.half), :]
                spot[...] = (own.astype(F32) + more[near, :].astype(F32)).astype(BF)

        loop(4, add)
        self.send(1, u).start()
        self.send(2, u).start()

    def along(self, u):
        p = self.place
        for which, mine in ((0, p.x), (1, p.y)):
            self.send(1 + which, u).wait_recv()
            spot, more = self.sums(which, u, mine), self.met(which, u)
            spot[...] = (spot[...].astype(F32) + more[...].astype(F32)).astype(BF)
            self.send(3 + which, u).start()
        for kind in (1, 2):
            self.send(kind, u).wait_send()

    def wait_write(self, u):
        pltpu.make_async_copy(self.done(u), self.done(u), self.out_sems.at[u % 2]).wait()

    def finish(self, u):
        p = self.place

        @pl.when(u >= 2)
        def _():
            self.wait_write(u)

        parts = []
        for which, spot in ((0, self.sums(0, u, p.x, p.y)), (1, self.sums(1, u, p.y, p.x))):
            self.send(3 + which, u).wait_recv()
            parts.append(spot[...].astype(F32) + self.ended(which, u)[...].astype(F32))
        value = jnp.concatenate(parts, axis=0)

        def put(first, out, flat):
            self.done(u)[...] = (value.T if flat else value).astype(BF)
            near = span((u - first) * UNIT, UNIT)
            target = out.at[near, :] if flat else out.at[:, near]
            pltpu.make_async_copy(self.done(u), target, self.out_sems.at[u % 2]).start()

        first = 0
        for at, out in enumerate(self.outs):
            count = (self.n_ff, self.n_ff, self.n_ff, self.n_local, 3 * self.n_local)[at]
            pl.when((u >= first) & (u < first + count))(functools.partial(put, first, out, at in (0, 3)))
            first += count

        for kind in (3, 4):
            self.send(kind, u).wait_send()

    def tick(self, u, turned, ffs, others):
        @pl.when(u < self.early)
        def _():
            self.product(u, turned, ffs.at[u // self.n_ff], u % self.n_ff)

        @pl.when((u >= self.early) & (u < self.count))
        def _():
            self.product(u, turned, others, u - self.early)

        for lag, stage in ((1, self.across), (3, self.along), (5, self.finish)):
            @pl.when((u >= lag) & (u < self.count + lag))
            def _():
                stage(u - lag)

    def drain(self):
        for u in (self.count - 2, self.count - 1):
            self.wait_write(u)


def as_row(col):
    n = col.shape[0]
    r = lax.broadcasted_iota(jnp.int32, (n, n), 0)
    s = lax.broadcasted_iota(jnp.int32, (n, n), 1)
    return jnp.sum(jnp.where(r == s, col, 0.0), axis=0, keepdims=True)


def as_col(row):
    n = row.shape[1]
    r = lax.broadcasted_iota(jnp.int32, (n, n), 0)
    s = lax.broadcasted_iota(jnp.int32, (n, n), 1)
    return jnp.sum(jnp.where(r == s, row, 0.0), axis=1, keepdims=True)


def turn(values, cos_tab, sin_tab):
    return values * cos_tab + pltpu.roll(values, HD // 2, 1) * sin_tab


def turn_back(grads, cos_tab, sin_tab):
    return grads * cos_tab - pltpu.roll(grads, HD // 2, 1) * sin_tab


def layer_kernel(
    n_mp,
    x_in, cot_in, wq_in, wk_in, wv_in, wo_in, wg_in, wu_in, wd_in,
    seg, live, freq, q_gain, k_gain, a_gain, f_gain,
    wq_out, wk_out, wv_out, wo_out, hidden_out, grad_in_out, gd_out, gg_out, gu_out, go_out, gqkv_out, *rest,
):
    gain_outs = rest[:4]
    (
        tall, wo, wg, wu, wd,
        x, qp, kp, qr, kr, v, o, stat, cos_tab, sin_tab, side, raw_a, h, ffs, d_ffn, cot, part, took,
        turned, dk_sum, dv_sum, sums, gains, gains_got,
        g_send, g_recv, g_local, row_sems, small, s_sems, s_out, gain_sems, io_sems,
    ) = rest[4:]
    place = Place(n_mp)
    rows, width = x.shape
    wq, wk, wv = (tall.at[i * width:(i + 1) * width, :] for i in range(3))
    local, ff = qp.shape[1], ffs.shape[2]
    act, gate, up = (ffs.at[i] for i in range(3))
    heads = local // HD
    scale = 1.0 / math.sqrt(HD)
    half = rows // 2
    n_ff, n_local = ff // UNIT, local // UNIT
    flying = {}

    def move(name, src, dst):
        at = len(flying)
        flying[name] = lambda: pltpu.make_async_copy(src, dst, io_sems.at[at])
        flying[name]().start()

    def need(*names):
        for name in names:
            flying[name]().wait()

    move("x", x_in, x)
    place.barrier()
    gq, gk, gv, go, gg, gu, gd = [
        Gather(place, src, full, i not in (3, 6), g_send.at[i], g_recv.at[i], g_local.at[i])
        for i, (src, full) in enumerate(
            zip((wq_in, wk_in, wv_in, wo_in, wg_in, wu_in, wd_in), (wq, wk, wv, wo, wg, wu, wd))
        )
    ]
    gq.begin_a()
    gq.begin_b()
    gk.begin_a()
    gk.begin_b()
    move("cot", cot_in, cot)
    ids = seg[...].astype(F32)
    ids_col = as_col(ids)
    before = jnp.sum((ids < ids_col).astype(F32), axis=1, keepdims=True)
    row_at = lax.broadcasted_iota(jnp.int32, (rows, 1), 0)
    side[:, 0:1] = ids_col
    side[:, 1:2] = (row_at < live[...]).astype(F32)
    angles = (row_at.astype(F32) - before) * freq[...]
    cos_tab[...] = jnp.cos(angles)
    lane = lax.broadcasted_iota(jnp.int32, (rows, HD), 1)
    sin_tab[...] = jnp.sin(angles) * jnp.where(lane < HD // 2, -1.0, 1.0)
    gq.relay()
    gv.begin_a()
    gq.pass_on()
    gv.begin_b()
    gk.relay()
    go.begin_a()
    gk.pass_on()
    gq.last()
    need("x")
    gq.ready()
    move("wq", wq, wq_out)
    row_sum = SmallSum(place, sums.at[0], small.at[0])

    def project(full, dst, squares_to=None):
        def one(r):
            near = span(r * half, half)
            value = dot(x[near, :], full[...])
            dst[near, :] = value.astype(BF)
            if squares_to is not None:
                stat[near, squares_to:squares_to + 1] = jnp.sum(value * value, axis=1, keepdims=True)

        loop(2, one)

    sums[0, 0] = jnp.zeros(sums.shape[2:], F32)
    project(wq, qp, heads)
    sums[0, 0, 0:1, :] = as_row(stat[:, heads:heads + 1])
    gv.relay()
    go.begin_b()
    gv.pass_on()
    gk.last()
    gk.ready()
    move("wk", wk, wk_out)
    project(wk, kp, heads + 1)
    sums[0, 0, 1:2, :] = as_row(stat[:, heads + 1:heads + 2])
    row_sum.begin()
    go.relay()
    gg.begin_a()
    gv.last()
    gv.ready()
    move("wv", wv, wv_out)
    project(wv, v)
    go.pass_on()
    gg.begin_b()
    totals = row_sum.end()
    inv_q = lax.rsqrt(as_col(totals[0:1, :]) / width + EPS)
    inv_k = lax.rsqrt(as_col(totals[1:2, :]) / width + EPS)
    stat[:, heads:heads + 1] = inv_q
    stat[:, heads + 1:heads + 2] = inv_k

    def rotate_head(hd):
        cols = span(hd * HD, HD)
        qr[:, cols] = turn(qp[:, cols].astype(F32) * inv_q * q_gain[:, cols], cos_tab[...], sin_tab[...]).astype(BF)
        kr[:, cols] = turn(kp[:, cols].astype(F32) * inv_k * k_gain[:, cols], cos_tab[...], sin_tab[...]).astype(BF)

    loop(heads, rotate_head)
    go.last()
    block = rows // 4
    lane_at = lax.broadcasted_iota(jnp.int32, (block, HD), 1)

    def allowed_at(rb):
        near, keys = slice(rb * block, (rb + 1) * block), (rb + 1) * block
        t_at = lax.broadcasted_iota(jnp.int32, (block, keys), 0) + rb * block
        s_at = lax.broadcasted_iota(jnp.int32, (block, keys), 1)
        return near, keys, (side[near, 0:1] == seg[:, 0:keys].astype(F32)) & (s_at <= t_at)

    def attend(rb):
        near, keys, allowed = allowed_at(rb)

        def one(hd):
            cols = span(hd * HD, HD)
            scores = jnp.where(allowed, dot_nt(qr[near, cols], kr[0:keys, cols]) * scale, -1e30)
            top = jnp.max(scores, axis=1, keepdims=True)
            weights = jnp.exp(scores - top)
            norm = jnp.sum(weights, axis=1, keepdims=True)
            stat[near, :] = jnp.where(lane_at == hd, top + jnp.log(norm), stat[near, :])
            o[near, cols] = dot((weights / norm).astype(BF), v[0:keys, cols]).astype(BF)

        loop(heads, one)

    wide = width // 8

    def columns(bits):
        return span(place.block(bits) * wide, wide)

    def by_rows(flow, k):
        return span(k // 4 * half, half), columns(2 * (k % 4) + flow)

    def took_slot(flow, k):
        return took.at[flow, k]

    sum_attn = RowSum(place, part, took_slot, raw_a, row_sems.at[0], by_rows, 8)

    def project_out(r):
        near = slice(r * half, (r + 1) * half)

        def one(i):
            part[near, columns(i)] = dot(o[near, :], wo[:, columns(i)]).astype(BF)

        loop(8, one)

    def mid(r):
        tile = rows // 8

        def one(at):
            near = span(at * tile, tile)
            raw = raw_a[near, :].astype(F32)
            inv = lax.rsqrt(jnp.mean(raw * raw, axis=1, keepdims=True) + EPS)
            h[near, :] = (x[near, :].astype(F32) + raw * inv * a_gain[...]).astype(BF)

        loop(4, one, 4 * r)

    def gate_part(r, first, count):
        near = slice(r * half, (r + 1) * half)

        def one(at):
            cols = span(at * UNIT, UNIT)
            gate[near, cols] = dot(h[near, :], wg[:, cols]).astype(BF)

        loop(count, one, first)

    def up_half(r, first, count):
        near = slice(r * half, (r + 1) * half)

        def one(at):
            cols = span(at * UNIT, UNIT)
            value = dot(h[near, :], wu[:, cols])
            up[near, cols] = value.astype(BF)
            pre = gate[near, cols].astype(F32)
            act[near, cols] = (pre * jax.nn.sigmoid(pre) * value).astype(BF)

        loop(count, one, first)

    attend(0)
    attend(1)
    go.ready()
    move("wo", wo, wo_out)
    project_out(0)
    sum_attn.push(0)
    sum_attn.push(1)
    gu.begin_a()
    attend(2)
    sum_attn.tick(1, 0)
    sum_attn.push(2)
    attend(3)
    sum_attn.tick(2, 0)
    sum_attn.push(3)
    project_out(1)
    gg.relay()
    gu.begin_b()
    sum_attn.push(4)
    sum_attn.tick(3, 0)
    gg.pass_on()

    def attn_both(t):
        sum_attn.push(t + 1)
        sum_attn.both(t, 3)

    attn_both(4)
    attn_both(5)
    gu.relay()
    gd.begin_a()
    loop(2, attn_both, 6)
    gg.last()
    gd.begin_b()
    loop(2, attn_both, 8)
    gg.ready()
    mid(0)

    def gate_and_tick(i):
        gate_part(0, i * (n_ff // 2), n_ff // 2)
        sum_attn.tick(7 + i, 1)

    loop(2, gate_and_tick)
    gu.pass_on()
    sum_attn.tick(9, 1)
    mid(1)
    gate_part(1, 0, n_ff)
    gu.last()
    gu.ready()
    up_half(0, 0, n_ff)
    sum_attn.sent()
    sum_ffn = RowSum(place, part, took_slot, d_ffn, row_sems.at[1], by_rows, 8)

    def project_down(k):
        near = span(k // 4 * half, half)

        def one(flow):
            cols = columns(2 * (k % 4) + flow)
            part[near, cols] = dot(act[near, :], wd[:, cols]).astype(BF)

        loop(2, one)
        sum_ffn.push(k)

    gd.own_copy().wait()
    gd.arrived(6)
    project_down(0)
    need("wq", "wk", "wv", "wo")
    for g in (gq, gk, gv, go):
        g.drain()
    up_half(1, 0, n_ff // 2)
    gd.relay()
    sum_ffn.tick(1, 0)
    up_half(1, n_ff // 2, n_ff // 2)
    project_down(4)
    gd.pass_on()
    gd.arrived(7, 8, 10, 11)
    project_down(1)
    sum_ffn.both(2, 1)
    project_down(2)
    project_down(5)
    sum_ffn.both(3, 1)
    project_down(6)
    gd.last()
    gd.arrived(9)
    project_down(3)
    sum_ffn.tick(4, 0)
    project_down(7)
    sum_ffn.tick(3, 1)

    def ffn_both(t):
        sum_ffn.both(t, 1)

    loop(5, ffn_both, 5)
    sum_ffn.sent(0)
    for g in (gg, gu, gd):
        g.drain()
    need("cot")

    gains[...] = jnp.zeros(gains.shape, F32)
    tile = rows // 8

    def back_ffn(at):
        near = span(at * tile, tile)
        raw = d_ffn[near, :].astype(F32)
        alive = side[near, 1:2]
        dy = alive * cot[near, :].astype(F32)
        inv = lax.rsqrt(jnp.mean(raw * raw, axis=1, keepdims=True) + EPS)
        normed = raw * inv
        gains[0:1, :] += jnp.sum(dy * normed, axis=0, keepdims=True)
        value = (alive * (h[near, :].astype(F32) + normed * f_gain[...])).astype(BF)
        for q in range(width // local):
            wv[span(q * rows + at * tile, tile), :] = value[:, q * local:(q + 1) * local]
        gained = f_gain[...] * dy
        mean = jnp.mean(gained * raw, axis=1, keepdims=True)
        d_ffn[near, :] = (inv * gained - raw * inv**3 * mean).astype(BF)

    def flip(src):
        def one(at):
            parity = at % 2
            own = 1 - (parity + place.c - 2 * parity * place.c)
            turned[span((4 * own + at // 2) * wide, wide), :] = src[:, span(at * wide, wide)].T

        loop(8, one)

    grads_out = (gd_out, gg_out, gu_out, go_out, gqkv_out)
    scatter = Scatter(place, tall, wo, grads_out, s_sems, s_out, n_ff, n_local)

    def back_act(r, first, count):
        near = slice(r * half, (r + 1) * half)

        def one(at):
            cols = span(at * UNIT, UNIT)
            d_act = dot_nt(d_ffn[near, :], wd[cols, :])
            pre, upper = gate[near, cols].astype(F32), up[near, cols].astype(F32)
            sig = jax.nn.sigmoid(pre)
            up[near, cols] = (d_act * pre * sig).astype(BF)
            gate[near, cols] = (d_act * upper * sig * (1.0 + pre * (1.0 - sig))).astype(BF)

        loop(count, one, first)

    raw_h = x
    sum_back = RowSum(place, part, took_slot, raw_h, row_sems.at[2], by_rows, 8)

    def back_gate(r, first):
        near = slice(r * half, (r + 1) * half)

        def one(i):
            value = dot_nt(gate[near, :], wg[columns(i), :]) + dot_nt(up[near, :], wu[columns(i), :])
            part[near, columns(i)] = value.astype(BF)

        loop(4, one, first)
        loop(2, sum_back.push, 4 * r + first // 2)

    dq, dk, dv = (wu.at[2 * rows:3 * rows, i * local:(i + 1) * local] for i in range(1, 4))
    others = wu.at[2 * rows:3 * rows, :]
    d_heads = wu.at[3 * rows:4 * rows, 0:local]
    loop(4, back_ffn)
    back_act(0, 0, n_ff // 2)
    sum_ffn.tick(9, 1)
    back_act(0, n_ff // 2, n_ff // 2)
    back_gate(0, 0)
    sum_ffn.sent(1)
    loop(4, back_ffn, 4)
    for q in range(width // local):
        move(f"hidden{q}", wv.at[q * rows:(q + 1) * rows, :], hidden_out.at[:, q * local:(q + 1) * local])
    flip(d_ffn)
    d_attn = wu.at[rows:2 * rows, :]

    def back_attn(at):
        near = span(at * tile, tile)
        raw = raw_a[near, :].astype(F32)
        dh = side[near, 1:2] * cot[near, :].astype(F32) + raw_h[near, :].astype(F32)
        inv = lax.rsqrt(jnp.mean(raw * raw, axis=1, keepdims=True) + EPS)
        gains[1:2, :] += jnp.sum(dh * raw * inv, axis=0, keepdims=True)
        gained = a_gain[...] * dh
        mean = jnp.mean(gained * raw, axis=1, keepdims=True)
        d_attn[near, :] = (inv * gained - raw * inv**3 * mean).astype(BF)

    def back_out(r):
        near = slice(r * half, (r + 1) * half)
        loop(4, back_attn, 4 * r)
        d_heads[near, :] = dot_nt(d_attn[near, :], wg[0:local, :]).astype(BF)

    def back_head(hd):
        cols = span(hd * HD, HD)
        dk_sum[...] = jnp.zeros(dk_sum.shape, F32)
        dv_sum[...] = jnp.zeros(dv_sum.shape, F32)
        for rb in range(4):
            near, keys, allowed = allowed_at(rb)
            lse = jnp.sum(jnp.where(lane_at == hd, stat[near, :], 0.0), axis=1, keepdims=True)
            scores = jnp.where(allowed, dot_nt(qr[near, cols], kr[0:keys, cols]) * scale, -1e30)
            probs = jnp.where(allowed, jnp.exp(scores - lse), 0.0)
            grad = d_heads[near, cols]
            d_prob = dot_nt(grad, v[0:keys, cols])
            delta = jnp.sum(grad.astype(F32) * o[near, cols].astype(F32), axis=1, keepdims=True)
            d_score = (probs * (d_prob - delta)).astype(BF)
            back = dot(d_score, kr[0:keys, cols]) * scale
            dq[near, cols] = turn_back(back, cos_tab[near, :], sin_tab[near, :]).astype(BF)
            dk_sum[0:keys, :] += dot_tn(d_score, qr[near, cols])
            dv_sum[0:keys, :] += dot_tn(probs.astype(BF), grad)
        dk[:, cols] = turn_back(dk_sum[...] * scale, cos_tab[...], sin_tab[...]).astype(BF)
        dv[:, cols] = dv_sum[...].astype(BF)

    row_sum_back = SmallSum(place, sums.at[1], small.at[1])
    normed = ((dq, qp, q_gain, heads), (dk, kp, k_gain, heads + 1))

    def begin_norms():
        sums[1, 0] = jnp.zeros(sums.shape[2:], F32)
        for at, (grad, raw, gain, lane_of) in enumerate(normed):
            both = grad[...].astype(F32) * raw[...].astype(F32)
            gains[2 + at:3 + at, 0:local] = jnp.sum(both * stat[:, lane_of:lane_of + 1], axis=0, keepdims=True)
            sums[1, 0, at:at + 1, :] = as_row(jnp.sum(gain[...] * both, axis=1, keepdims=True))
        row_sum_back.begin()

    def end_norms():
        totals = row_sum_back.end()
        for at, (grad, raw, gain, lane_of) in enumerate(normed):
            inv = stat[:, lane_of:lane_of + 1]
            mean = as_col(totals[at:at + 1, :]) / width
            gained = gain[...] * grad[...].astype(F32)
            grad[...] = (inv * gained - raw[...].astype(F32) * inv**3 * mean).astype(BF)

    raw_x = d_ffn
    sum_in = RowSum(place, part, took_slot, raw_x, row_sems.at[3], by_rows, 8)

    def back_in(r):
        near = slice(r * half, (r + 1) * half)

        def one(i):
            spot = columns(i)
            value = dot_nt(dq[near, :], wd[spot, 0:local]) + dot_nt(dk[near, :], wd[spot, local:2 * local])
            part[near, spot] = (value + dot_nt(dv[near, :], wd[spot, 2 * local:3 * local])).astype(BF)

        loop(8, one)
        loop(4, sum_in.push, 4 * r)

    def end_tile(at):
        near = span(at * tile, tile)
        dh = side[near, 1:2] * cot[near, :].astype(F32) + raw_h[near, :].astype(F32)
        cot[near, :] = (dh + raw_x[near, :].astype(F32)).astype(BF)

    def end_half(r):
        loop(4, end_tile, 4 * r)
        near = slice(r * half, (r + 1) * half)
        move(f"grad_in{r}", cot.at[near, :], grad_in_out.at[near, :])

    partners = (place.sib, place.xn, place.yn)

    def gain_copy(at):
        return remote(
            gains.at[pl.ds(8 * at, 8), :], gains_got.at[at], gain_sems.at[0, at], gain_sems.at[1, at],
            {"dp": partners[at]},
        )

    def add_gains(at):
        gain_copy(at).wait_recv()
        gains[8 * at + 8:8 * at + 16, :] = gains[8 * at:8 * at + 8, :] + gains_got[at]
        if at < 2:
            gain_copy(at + 1).start()
        else:
            for i, out in enumerate(gain_outs):
                move(f"gain{i}", gains.at[24 + i:25 + i, 0:out.shape[1]], out)

    def fetch():
        move("wq2", wq_out, wd.at[:, 0:local])
        move("wk2", wk_out, wd.at[:, local:2 * local])
        move("wv2", wv_out, wd.at[:, 2 * local:3 * local])
        move("wo2", wo_out, wg.at[0:local, :])
        move("x2", x_in, wu.at[0:rows, :])

    def at_step(s):
        if s == 0:
            back_gate(0, 4)
        elif s in (1, 2):
            back_act(1, (s - 1) * (n_ff // 2), n_ff // 2)
        elif s in (3, 4):
            back_gate(1, 4 * (s - 3))
            if s == 4:
                fetch()
        elif s == 12:
            need("wo2")
            back_out(0)
        elif s == 13:
            sum_back.sent()
            back_out(1)
            others[:, 0:local] = o[...]
        elif s == 14:
            loop(heads // 2, back_head)
        elif s == 15:
            loop(heads - heads // 2, back_head, heads // 2)
            begin_norms()
        elif s == 17:
            end_norms()
            need("wq2", "wk2", "wv2", "x2")
        elif s in (18, 19):
            back_in(s - 18)
        elif s == 20:
            gain_copy(0).start()
        elif s in (22, 24, 26):
            add_gains((s - 22) // 2)
        elif s in (28, 29):
            end_half(s - 28)

    def at_tick(u, act_on):
        @pl.when(u == act_on[0])
        def _():
            act_on[1]()

    doubles = (4, 7, 21, 22, 25, 26)

    def one_tick(u):
        for when, src in ((n_ff, h), (3 * n_ff, d_attn), (3 * n_ff + n_local, wu.at[0:rows, :])):
            at_tick(u, (when, functools.partial(flip, src)))
        at_tick(u, (1, functools.partial(need, *(f"hidden{q}" for q in range(width // local)))))
        scatter.tick(u, turned, ffs, others)

    def step(s):
        before = sum((s > at).astype(jnp.int32) for at in doubles)
        here = sum((s == at).astype(jnp.int32) for at in doubles)
        loop(1 + here, one_tick, s + before)

        at_tick(s, (19, functools.partial(at_step, 19)))

        for row_sum_, half_, t, first, last in (
            (sum_back, 0, s, 1, 5), (sum_back, 1, s - 3, 4, 12), (sum_in, 0, s - 18, 19, 27), (sum_in, 1, s - 20, 21, 29),
        ):
            @pl.when((s >= first) & (s <= last))
            def _():
                row_sum_.tick(t, half_)

        @pl.when((s >= 6) & (s <= 12) & (s % 2 == 0))
        def _():
            sum_back.tick((s + 6) // 2, 0)

        for when in (0, 1, 2, 3, 4, 12, 13, 14, 15, 17, 18, 20, 22, 24, 26, 28, 29):
            at_tick(s, (when, functools.partial(at_step, when)))

    loop(scatter.count + 5 - len(doubles), step)
    for at in range(3):
        gain_copy(at).wait_send()
    sum_in.sent()
    row_sum.drain()
    row_sum_back.drain()
    scatter.drain()
    need("gain0", "gain1", "gain2", "gain3", "grad_in0", "grad_in1")


def layer_call(n_mp, x, cot, weights, seg, live, freq, q_gain, k_gain, a_gain, f_gain):
    rows, width = x.shape
    local, ff = weights[0].shape[1], weights[4].shape[1]
    high, half = width // 8, rows // 2
    any_spec = pl.BlockSpec(memory_space=pl.ANY)
    vmem = pl.BlockSpec(memory_space=pltpu.VMEM)
    S, V, dma = jax.ShapeDtypeStruct, pltpu.VMEM, pltpu.SemaphoreType.DMA
    fulls = [(width, local)] * 3 + [(local, width)] + [(width, ff)] * 2 + [(ff, width)]
    outs = fulls[:4] + [
        (rows, width), (rows, width), (ff, high), (high, ff), (high, ff), (local, high), (high, 3 * local),
    ]
    return pl.pallas_call(
        functools.partial(layer_kernel, n_mp),
        out_shape=[S(s, BF) for s in outs] + [S((1, n), F32) for n in (width, width, local, local)],
        in_specs=[any_spec] * 9 + [vmem] * 7,
        out_specs=[any_spec] * 15,
        scratch_shapes=[V(((16 + 5 * Scatter.slots // 2) * high, local), BF)]
        + [V(s, BF) for s in fulls[3:]]
        + [V((rows, width), BF)]
        + [V((rows, local), BF)] * 6
        + [V((rows, HD), F32)] * 4
        + [V((rows, width), BF)] * 2
        + [V((3, rows, ff), BF)]
        + [V((rows, width), BF)] * 3
        + [V((2, 8, half, high), BF), V((width, rows), BF), V((rows, HD), F32), V((rows, HD), F32)]
        + [V((2, n_mp, 8, rows), F32), V((32, width), F32), V((3, 8, width), F32)]
        + [dma((7, 12)), dma((7, 12)), dma((7,)), dma((4, 4, 2, 8)), dma((2, 2, n_mp))]
        + [dma((2, 5, Scatter.slots)), dma((2,)), dma((2, 3)), dma((24,))],
        compiler_params=pltpu.CompilerParams(
            collective_id=0, has_side_effects=True, vmem_limit_bytes=67043328,
        ),
    )(x, cot, *weights, seg, live, freq, q_gain, k_gain, a_gain, f_gain)


def with_kernel(n_mp, hidden_in, cotangent, segments, live_counts, *rest):
    weights, (query_gain, key_gain, attn_gain, ffn_gain) = rest[:7], rest[7:]
    local = weights[0].shape[1]
    inv_freq = THETA ** (-(jnp.arange(HD // 2, dtype=F32) * (2.0 / HD)))
    freq = jnp.concatenate([inv_freq, inv_freq])[None]
    hidden_out, grad_in, g_down, g_gate, g_up, g_output, g_qkv, d_f, d_a, d_q, d_k = layer_call(
        n_mp, hidden_in, cotangent, weights, segments, live_counts[None], freq,
        query_gain[None], key_gain[None], attn_gain[None], ffn_gain[None],
    )[4:]

    return (
        hidden_out,
        grad_in.astype(F32),
        g_qkv[:, :local].astype(F32),
        g_qkv[:, local:2 * local].astype(F32),
        g_qkv[:, 2 * local:].astype(F32),
        g_output.astype(F32),
        g_gate.astype(F32),
        g_up.astype(F32),
        g_down.astype(F32),
        d_q[0],
        d_k[0],
        d_a[0],
        d_f[0],
    )


def doc_positions(seg_row):
    row_count = seg_row.shape[0]
    row_index = jnp.arange(row_count, dtype=jnp.int32)
    change = jnp.concatenate([jnp.ones((1,), dtype=bool), seg_row[1:] != seg_row[:-1]])
    doc_start = lax.cummax(jnp.where(change, row_index, jnp.zeros_like(row_index)), axis=0)
    return (row_index - doc_start).astype(jnp.float32)


def rotary_tables(positions, head_size):
    half_size = head_size // 2
    inv_freq = THETA ** (-(jnp.arange(half_size, dtype=jnp.float32) * (2.0 / head_size)))
    angles = positions[:, None] * inv_freq[None, :]
    return (jnp.cos(angles)[:, None, :], jnp.sin(angles)[:, None, :])


def rotate(values, cos_tab, sin_tab):
    half_size = values.shape[2] // 2
    first_half = values[:, :, :half_size]
    second_half = values[:, :, half_size:]
    return jnp.concatenate(
        [
            first_half * cos_tab - second_half * sin_tab,
            second_half * cos_tab + first_half * sin_tab,
        ],
        axis=2,
    )


def rotate_back(grads, cos_tab, sin_tab):
    half_size = grads.shape[2] // 2
    first_half = grads[:, :, :half_size]
    second_half = grads[:, :, half_size:]
    return jnp.concatenate(
        [
            first_half * cos_tab + second_half * sin_tab,
            second_half * cos_tab - first_half * sin_tab,
        ],
        axis=2,
    )


def block_mask(seg_row, offset, block_rows):
    row_index = jnp.arange(seg_row.shape[0])
    same = seg_row[offset : offset + block_rows, None] == seg_row[None, :]
    return same & (row_index[:, None] >= row_index[None, :])


def block_scores(q_blk, k_bf, allowed, score_scale):
    scores = (
        jnp.einsum("qhe,khe->hqk", q_blk, k_bf, preferred_element_type=jnp.float32) * score_scale
    )
    return jnp.where(allowed[None], scores, jnp.float32(-1e30))


def attend_forward(q_bf, k_bf, v_bf, seg_row, score_scale):
    row_count = q_bf.shape[0]
    block_rows = min(512, row_count)
    allowed = block_mask(seg_row, 0, block_rows)
    scores = block_scores(q_bf, k_bf, allowed, score_scale)
    row_max = jnp.max(scores, axis=2, keepdims=True)
    lse = row_max + jnp.log(jnp.sum(jnp.exp(scores - row_max), axis=2, keepdims=True))
    probs = jnp.exp(scores - lse).astype(jnp.bfloat16)
    outputs = jnp.einsum("hqk,khe->qhe", probs, v_bf, preferred_element_type=jnp.float32)
    lse_parts = [lse]
    return (outputs.astype(jnp.bfloat16), lse_parts)


def attend_backward(q_bf, k_bf, v_bf, o_bf, do_bf, lse_parts, seg_row, score_scale):
    row_count = q_bf.shape[0]
    block_rows = min(512, row_count)
    dq_parts = []
    dk_acc = jnp.zeros(k_bf.shape, jnp.float32)
    dv_acc = jnp.zeros(v_bf.shape, jnp.float32)
    for part_index, offset in enumerate(range(0, row_count, block_rows)):
        allowed = block_mask(seg_row, offset, block_rows)
        scores = block_scores(q_bf, k_bf, allowed, score_scale)
        probs = jnp.exp(scores - lse_parts[part_index])
        probs_bf = probs.astype(jnp.bfloat16)
        dprob = jnp.einsum("qhe,khe->hqk", do_bf, v_bf, preferred_element_type=jnp.float32)
        delta = jnp.transpose(
            jnp.sum(do_bf.astype(jnp.float32) * o_bf.astype(jnp.float32), axis=2)
        )[:, :, None]
        dscore = (probs * (dprob - delta)).astype(jnp.bfloat16)
        dq_parts.append(
            jnp.einsum("hqk,khe->qhe", dscore, k_bf, preferred_element_type=jnp.float32)
            * score_scale
        )
        dk_acc = (
            jnp.einsum("hqk,qhe->khe", dscore, q_bf, preferred_element_type=jnp.float32)
            * score_scale
        )
        dv_acc = jnp.einsum("hqk,qhe->khe", probs_bf, do_bf, preferred_element_type=jnp.float32)
    return (dq_parts[0], dk_acc, dv_acc.astype(jnp.bfloat16))


def scatter_grad(grad, axis_name, scatter_dimension, tiled):
    total = lax.psum_scatter(
        grad.astype(jnp.bfloat16), axis_name, scatter_dimension=scatter_dimension, tiled=tiled
    )
    return total.astype(jnp.float32)


def sum_parts(part, axis_name):
    own = lax.psum_scatter(
        part.astype(jnp.bfloat16), axis_name, scatter_dimension=0, tiled=True
    )
    return lax.all_gather(own, axis_name, axis=0, tiled=True).astype(jnp.float32)


def norm_back(raw, inv_scale, gained, row_sums, width):
    return inv_scale * gained - raw * inv_scale**3 * (row_sums[:, None] / width)


def on_device(
    hidden_in,
    cotangent,
    segments,
    live_counts,
    w_query,
    w_key,
    w_value,
    w_output,
    w_gate,
    w_up,
    w_down,
    query_gain,
    key_gain,
    attn_gain,
    ffn_gain,
):
    gathered = (
        lax.all_gather(w_query, "dp", axis=0, tiled=True),
        lax.all_gather(w_key, "dp", axis=0, tiled=True),
        lax.all_gather(w_value, "dp", axis=0, tiled=True),
        lax.all_gather(w_output, "dp", axis=1, tiled=True),
        lax.all_gather(w_gate, "dp", axis=0, tiled=True),
        lax.all_gather(w_up, "dp", axis=0, tiled=True),
        lax.all_gather(w_down, "dp", axis=1, tiled=True),
    )
    wq_full, wk_full, wv_full, wo_full, wg_full, wu_full, wd_full = gathered
    seg_row = segments[0]
    live_n = live_counts[0]
    row_count, width = hidden_in.shape
    local_width = wq_full.shape[1]
    heads_here = local_width // HD
    score_scale = 1.0 / math.sqrt(HD)
    live_mask = (jnp.arange(row_count, dtype=jnp.int32) < live_n).astype(jnp.float32)[:, None]
    cos_tab, sin_tab = rotary_tables(doc_positions(seg_row), HD)
    q_proj = jnp.dot(hidden_in, wq_full, preferred_element_type=jnp.float32)
    k_proj = jnp.dot(hidden_in, wk_full, preferred_element_type=jnp.float32)
    v_bf = jnp.dot(hidden_in, wv_full, preferred_element_type=jnp.float32).astype(jnp.bfloat16)
    sq_query, sq_key = lax.psum(
        (jnp.sum(q_proj * q_proj, axis=1), jnp.sum(k_proj * k_proj, axis=1)), "mp"
    )
    inv_q = lax.rsqrt(sq_query[:, None] / width + EPS)
    inv_k = lax.rsqrt(sq_key[:, None] / width + EPS)
    q_rot = rotate(
        (q_proj * inv_q * query_gain).reshape(row_count, heads_here, HD), cos_tab, sin_tab
    ).astype(jnp.bfloat16)
    k_rot = rotate(
        (k_proj * inv_k * key_gain).reshape(row_count, heads_here, HD), cos_tab, sin_tab
    ).astype(jnp.bfloat16)
    v_heads = v_bf.reshape(row_count, heads_here, HD)
    o_bf, lse_parts = attend_forward(q_rot, k_rot, v_heads, seg_row, score_scale)
    o_flat = o_bf.reshape(row_count, local_width)
    attn_raw = sum_parts(jnp.dot(o_flat, wo_full, preferred_element_type=jnp.float32), "mp")
    inv_a = lax.rsqrt(jnp.mean(attn_raw * attn_raw, axis=1, keepdims=True) + EPS)
    h_mid = hidden_in.astype(jnp.float32) + attn_raw * inv_a * attn_gain
    h_bf = h_mid.astype(jnp.bfloat16)
    gate_pre = jnp.dot(h_bf, wg_full, preferred_element_type=jnp.float32)
    up_pre = jnp.dot(h_bf, wu_full, preferred_element_type=jnp.float32)
    act_bf = (jax.nn.silu(gate_pre) * up_pre).astype(jnp.bfloat16)
    ffn_raw = sum_parts(jnp.dot(act_bf, wd_full, preferred_element_type=jnp.float32), "mp")
    inv_f = lax.rsqrt(jnp.mean(ffn_raw * ffn_raw, axis=1, keepdims=True) + EPS)
    hidden_out = (live_mask * (h_mid + ffn_raw * inv_f * ffn_gain)).astype(jnp.bfloat16)
    wq_back, wk_back, wv_back, wo_back, wg_back, wu_back, wd_back = gathered
    dy = live_mask * cotangent.astype(jnp.float32)
    g_ffn_gain = jnp.sum(dy * ffn_raw * inv_f, axis=0)
    gained_f = ffn_gain * dy
    d_ffn = norm_back(ffn_raw, inv_f, gained_f, jnp.sum(gained_f * ffn_raw, axis=1), width).astype(
        jnp.bfloat16
    )
    d_act = jnp.dot(d_ffn, wd_back.T, preferred_element_type=jnp.float32)
    sig = jax.nn.sigmoid(gate_pre)
    d_up = (d_act * gate_pre * sig).astype(jnp.bfloat16)
    d_gate = (d_act * up_pre * sig * (1.0 + gate_pre * (1.0 - sig))).astype(jnp.bfloat16)
    ffn_part = jnp.dot(d_gate, wg_back.T, preferred_element_type=jnp.float32) + jnp.dot(
        d_up, wu_back.T, preferred_element_type=jnp.float32
    )
    dh = dy + sum_parts(ffn_part, "mp")
    g_down = jnp.dot(act_bf.T, d_ffn, preferred_element_type=jnp.float32)
    g_gate = jnp.dot(h_bf.T, d_gate, preferred_element_type=jnp.float32)
    g_up = jnp.dot(h_bf.T, d_up, preferred_element_type=jnp.float32)
    g_attn_gain = jnp.sum(dh * attn_raw * inv_a, axis=0)
    gained_a = attn_gain * dh
    d_attn = norm_back(
        attn_raw, inv_a, gained_a, jnp.sum(gained_a * attn_raw, axis=1), width
    ).astype(jnp.bfloat16)
    d_heads = jnp.dot(d_attn, wo_back.T, preferred_element_type=jnp.float32).astype(jnp.bfloat16)
    g_output = jnp.dot(o_flat.T, d_attn, preferred_element_type=jnp.float32)
    dq_rot, dk_rot, d_val = attend_backward(
        q_rot,
        k_rot,
        v_heads,
        o_bf,
        d_heads.reshape(row_count, heads_here, HD),
        lse_parts,
        seg_row,
        score_scale,
    )
    dq_norm = rotate_back(dq_rot, cos_tab, sin_tab).reshape(row_count, local_width)
    dk_norm = rotate_back(dk_rot, cos_tab, sin_tab).reshape(row_count, local_width)
    g_query_gain = jnp.sum(dq_norm * q_proj * inv_q, axis=0)
    g_key_gain = jnp.sum(dk_norm * k_proj * inv_k, axis=0)
    gained_q = query_gain * dq_norm
    gained_k = key_gain * dk_norm
    sums_query, sums_key = lax.psum(
        (jnp.sum(gained_q * q_proj, axis=1), jnp.sum(gained_k * k_proj, axis=1)), "mp"
    )
    dq_bf = norm_back(q_proj, inv_q, gained_q, sums_query, width).astype(jnp.bfloat16)
    dk_bf = norm_back(k_proj, inv_k, gained_k, sums_key, width).astype(jnp.bfloat16)
    dv_bf = d_val.reshape(row_count, local_width)
    input_part = (
        jnp.dot(dq_bf, wq_back.T, preferred_element_type=jnp.float32)
        + jnp.dot(dk_bf, wk_back.T, preferred_element_type=jnp.float32)
        + jnp.dot(dv_bf, wv_back.T, preferred_element_type=jnp.float32)
    )
    grad_in = dh + sum_parts(input_part, "mp")
    g_query = jnp.dot(hidden_in.T, dq_bf, preferred_element_type=jnp.float32)
    g_key = jnp.dot(hidden_in.T, dk_bf, preferred_element_type=jnp.float32)
    g_value = jnp.dot(hidden_in.T, dv_bf, preferred_element_type=jnp.float32)
    owned = (
        scatter_grad(g_query, "dp", scatter_dimension=0, tiled=True),
        scatter_grad(g_key, "dp", scatter_dimension=0, tiled=True),
        scatter_grad(g_value, "dp", scatter_dimension=0, tiled=True),
        scatter_grad(g_output, "dp", scatter_dimension=1, tiled=True),
        scatter_grad(g_gate, "dp", scatter_dimension=0, tiled=True),
        scatter_grad(g_up, "dp", scatter_dimension=0, tiled=True),
        scatter_grad(g_down, "dp", scatter_dimension=1, tiled=True),
    )
    gain_totals = lax.psum((g_query_gain, g_key_gain, g_attn_gain, g_ffn_gain), "dp")
    return (
        hidden_out,
        grad_in,
        owned[0],
        owned[1],
        owned[2],
        owned[3],
        owned[4],
        owned[5],
        owned[6],
        gain_totals[0],
        gain_totals[1],
        gain_totals[2],
        gain_totals[3],
    )


def kernel_fits(mesh, hidden_in, segments, w_query, w_gate):
    n_dp, n_mp = mesh.shape["dp"], mesh.shape["mp"]
    rows, width = hidden_in.shape[0] // n_dp, hidden_in.shape[1]
    local, ff = w_query.shape[1] // n_mp, w_gate.shape[1] // n_mp
    even = width % (8 * UNIT) == 0 and local % UNIT == 0 and ff % (2 * UNIT) == 0
    fits = rows == UNIT * 2 and width == 8 * UNIT and local == rows and ff == width
    return n_dp == 8 and n_mp >= 2 and even and fits


def solution(mesh):
    in_specs = (
        P("dp", None),
        P("dp", None),
        P("dp", None),
        P("dp"),
        P("dp", "mp"),
        P("dp", "mp"),
        P("dp", "mp"),
        P("mp", "dp"),
        P("dp", "mp"),
        P("dp", "mp"),
        P("mp", "dp"),
        P("mp"),
        P("mp"),
        P(),
        P(),
    )
    out_specs = (
        P("dp", None),
        P("dp", None),
        P("dp", "mp"),
        P("dp", "mp"),
        P("dp", "mp"),
        P("mp", "dp"),
        P("dp", "mp"),
        P("dp", "mp"),
        P("mp", "dp"),
        P("mp"),
        P("mp"),
        P(),
        P(),
    )

    def step(*args):
        if kernel_fits(mesh, args[0], args[2], args[4], args[8]):
            body = functools.partial(with_kernel, mesh.shape["mp"])
        else:
            body = on_device
        return jax.shard_map(
            body, mesh=mesh, in_specs=in_specs, out_specs=out_specs, check_vma=False
        )(*args)

    return step
```

```python
import functools
import math

import jax
import jax.numpy as jnp
from jax import lax
from jax.experimental import pallas as pl
from jax.experimental.pallas import tpu as pltpu
from jax.sharding import PartitionSpec as P

HD = 128
EPS = 1e-06
THETA = 500000.0
UNIT = 256
BF = jnp.bfloat16
F32 = jnp.float32


def dot(a, b):
    return jnp.dot(a, b, preferred_element_type=F32)


def dot_nt(a, b):
    return lax.dot_general(a, b, (((1,), (1,)), ((), ())), preferred_element_type=F32)


def dot_tn(a, b):
    return lax.dot_general(a, b, (((0,), (0,)), ((), ())), preferred_element_type=F32)


def span(start, size):
    return pl.ds(start if isinstance(start, int) else pl.multiple_of(start, size), size)


def loop(count, body, first=0):
    def step(at, carry):
        body(at)
        return carry

    lax.fori_loop(first, first + count, step, 0)


def remote(src, dst, send, recv, device):
    return pltpu.make_async_remote_copy(
        src_ref=src, dst_ref=dst, send_sem=send, recv_sem=recv,
        device_id=device, device_id_type=pl.DeviceIdType.MESH,
    )


class Place:
    def __init__(self, n_mp):
        self.dp, self.z = lax.axis_index("dp"), lax.axis_index("mp")
        self.n_mp, self.end = n_mp, n_mp - 1
        self.c = lax.rem(self.dp, 2)
        self.x = lax.rem(self.dp // 2, 2)
        self.y = self.dp // 4
        self.sib, self.xn, self.yn, self.dg = (self.block(i) for i in (1, 2, 4, 6))

    def block(self, i):
        i0, i1, i2 = i % 2, (i // 2) % 2, i // 4
        c, x, y = (a + b - 2 * a * b for a, b in ((self.c, i0), (self.x, i1), (self.y, i2)))
        return 4 * y + 2 * x + c

    def barrier(self):
        sem = pltpu.get_barrier_semaphore()
        mesh = pl.DeviceIdType.MESH
        for dp in (self.sib, self.xn, self.yn):
            pl.semaphore_signal(sem, inc=1, device_id={"dp": dp}, device_id_type=mesh)
        for step in range(1, self.n_mp):
            z = lax.rem(self.z + step, self.n_mp)
            pl.semaphore_signal(sem, inc=1, device_id={"mp": z}, device_id_type=mesh)
        pl.semaphore_wait(sem, 3 + self.n_mp - 1)


class Gather:
    def __init__(self, place, src, full, by_rows, send, recv, local):
        self.place, self.src, self.full, self.by_rows = place, src, full, by_rows
        self.sends, self.recvs, self.local = send, recv, local
        self.rows, self.cols = src.shape
        self.half = self.rows // 2

    def spot(self, owner, part=None):
        size = self.rows if self.by_rows else self.cols
        first, count = (0, size) if part is None else (part * size // 2, size // 2)
        near = pl.ds(pl.multiple_of(owner * size + first, size // 2), count)
        return self.full.at[near, :] if self.by_rows else self.full.at[:, near]

    def mine(self, part):
        size = (self.rows if self.by_rows else self.cols) // 2
        near = pl.ds(part * size, size)
        return self.src.at[near, :] if self.by_rows else self.src.at[:, near]

    def copies(self):
        p = self.place
        table = {
            0: (self.mine(0), p.dp, 0, p.xn, p.xn),
            1: (self.mine(1), p.dp, 1, p.xn, p.xn),
            2: (self.mine(0), p.dp, 0, p.yn, p.yn),
            3: (self.mine(1), p.dp, 1, p.yn, p.yn),
            6: (self.src, p.dp, None, p.sib, p.sib),
        }
        for kind, owner, part, target, arrives in (
            (4, p.yn, 1, p.xn, p.dg), (5, p.xn, 0, p.yn, p.dg),
            (7, p.xn, 0, p.sib, p.block(3)), (10, p.xn, 1, p.sib, p.block(3)),
            (8, p.yn, 1, p.sib, p.block(5)), (11, p.yn, 0, p.sib, p.block(5)),
            (9, p.dg, None, p.sib, p.block(7)),
        ):
            table[kind] = (self.spot(owner, part), owner, part, target, arrives)
        return table

    def copy(self, kind):
        src, owner, part, target, _ = self.copies()[kind]
        return remote(src, self.spot(owner, part), self.sends.at[kind], self.recvs.at[kind], {"dp": target})

    def start(self, *kinds):
        for kind in kinds:
            self.copy(kind).start()

    def arrived(self, *kinds):
        for kind in kinds:
            _, _, part, target, owner = self.copies()[kind]
            spot = self.spot(owner, part)
            remote(spot, spot, self.sends.at[kind], self.recvs.at[kind], {"dp": target}).wait_recv()

    def own_copy(self):
        return pltpu.make_async_copy(self.src, self.spot(self.place.dp), self.local)

    def begin_a(self):
        self.start(0, 3)

    def begin_b(self):
        self.start(1, 2, 6)
        self.own_copy().start()

    def relay(self):
        self.arrived(0)
        self.start(5, 7)
        self.arrived(3)
        self.start(4, 8)

    def pass_on(self):
        self.arrived(1)
        self.start(10)
        self.arrived(2)
        self.start(11)

    def last(self):
        self.arrived(5, 4)
        self.start(9)

    def ready(self):
        self.own_copy().wait()
        self.arrived(6, 7, 8, 9, 10, 11)

    def drain(self):
        for kind in range(12):
            self.copy(kind).wait_send()


class RowSum:
    def __init__(self, place, part, took, total, sems, chunk_at, count):
        self.place, self.part, self.took, self.total, self.sems = place, part, took, total, sems
        self.chunk_at = chunk_at
        self.count = count

    def spot(self, ref, flow, k):
        return ref.at[self.chunk_at(flow, k)]

    def at(self, flow):
        return self.place.z + flow * (self.place.end - 2 * self.place.z)

    def forth(self, flow, k):
        return remote(
            self.spot(self.part, flow, k), self.took(flow, k),
            self.sems.at[0, flow, k], self.sems.at[1, flow, k], {"mp": self.place.z + 1 - 2 * flow},
        )

    def back(self, flow, k):
        spot = self.spot(self.total, flow, k)
        return remote(spot, spot, self.sems.at[2, flow, k], self.sems.at[3, flow, k], {"mp": self.place.z - 1 + 2 * flow})

    def push(self, k):
        if isinstance(k, int) and k >= self.count:
            return

        def one(flow):
            @pl.when((self.at(flow) == 0) & (k < self.count))
            def _():
                self.forth(flow, k).start()

        loop(2, one)

    def add(self, dst, flow, k):
        mine, to, more = self.spot(self.part, flow, k), self.spot(dst, flow, k), self.took(flow, k)
        step = mine.shape[0] // 4

        def one(at):
            near = span(at * step, step)
            to[near, :] = (mine[near, :].astype(F32) + more[near, :].astype(F32)).astype(BF)

        loop(4, one)

    def tick(self, t, half):
        end, count = self.place.end, self.count // 2
        if isinstance(t, int) and t >= count + 2 * end:
            return

        def gather(flow):
            at = self.at(flow)
            k = t - at

            @pl.when((at > 0) & (k >= 0) & (k < count))
            def _():
                chunk = half * count + k
                self.forth(flow, chunk).wait_recv()

                @pl.when(at < end)
                def _():
                    self.add(self.part, flow, chunk)
                    self.forth(flow, chunk).start()

                @pl.when(at == end)
                def _():
                    self.add(self.total, flow, chunk)
                    self.back(flow, chunk).start()

        def bring_back(flow):
            at = self.at(flow)
            k = t - 2 * end + at

            @pl.when((at < end) & (k >= 0) & (k < count))
            def _():
                chunk = half * count + k
                self.back(flow, chunk).wait_recv()

                @pl.when(at > 0)
                def _():
                    self.back(flow, chunk).start()

        if not isinstance(t, int) or t < count + end:
            loop(2, gather)
        if not isinstance(t, int) or t >= end + 1:
            loop(2, bring_back)

    def both(self, t, lag):
        self.tick(t, 0)
        self.tick(t - lag, 1)

    def sent(self, half=None):
        first, count = (0, self.count) if half is None else (half * self.count // 2, self.count // 2)
        for flow in range(2):
            at = self.at(flow)

            def one(k):
                @pl.when(at < self.place.end)
                def _():
                    self.forth(flow, k).wait_send()

                @pl.when(at > 0)
                def _():
                    self.back(flow, k).wait_send()

            loop(count, one, first)


class SmallSum:
    def __init__(self, place, slots, sems):
        self.place, self.slots, self.sems = place, slots, sems

    def copy(self, step):
        p = self.place
        return remote(
            self.slots.at[0], self.slots.at[step], self.sems.at[0, step], self.sems.at[1, step],
            {"mp": lax.rem(p.z + step, p.n_mp)},
        )

    def begin(self):
        for step in range(1, self.place.n_mp):
            self.copy(step).start()

    def end(self):
        for step in range(1, self.place.n_mp):
            self.copy(step).wait_recv()
        total = self.slots[0]
        for step in range(1, self.place.n_mp):
            total = total + self.slots[step]
        return total

    def drain(self):
        for step in range(1, self.place.n_mp):
            self.copy(step).wait_send()


class Scatter:
    slots = 6

    def __init__(self, place, tall, broad, outs, sems, out_sems, n_ff, n_local):
        self.place, self.tall, self.broad, self.outs = place, tall, broad, outs
        self.n_ff, self.n_local, self.early = n_ff, n_local, 3 * n_ff
        self.count = 3 * n_ff + 4 * n_local
        self.sems, self.out_sems = sems, out_sems
        self.rows = broad.shape[1] // 8
        self.half = self.rows // 2

    def made(self, u, own):
        return self.tall.at[span((u % 2) * 4 * self.rows, 4 * self.rows), span(own * UNIT, UNIT)]

    def got(self, u, chip=None):
        s = u % 4
        first, size = (8 + s % 2 * 4) * self.rows, 4 * self.rows
        if chip is not None:
            first, size = first + chip * self.rows, self.rows
        return self.tall.at[span(first, size), span(s // 2 * UNIT, UNIT)]

    def sums(self, which, u, to, then=None):
        first, size = (16 + u % self.slots * 2 + to) * self.rows, self.rows
        if then is not None:
            first, size = first + then * self.half, self.half
        return self.tall.at[span(first, size), pl.ds(which * UNIT, UNIT)]

    def ended(self, which, u):
        first = (16 + 2 * self.slots) * self.rows + u % self.slots * self.half
        return self.tall.at[span(first, self.half), pl.ds(which * UNIT, UNIT)]

    def met(self, which, u):
        s = u % self.slots
        return self.broad.at[span(s % 2 * self.rows, self.rows), span((s // 2 * 2 + which) * UNIT, UNIT)]

    def done(self, u):
        return self.broad.at[span((u % 2) * self.rows, self.rows), span(self.slots * UNIT, UNIT)]

    def send(self, kind, u):
        p, s = self.place, u % self.slots
        src, dst, target = {
            0: lambda: (self.made(u, 0), self.got(u), p.sib),
            1: lambda: (self.sums(0, u, 1 - p.x), self.met(0, u), p.xn),
            2: lambda: (self.sums(1, u, 1 - p.y), self.met(1, u), p.yn),
            3: lambda: (self.sums(0, u, p.x, 1 - p.y), self.ended(0, u), p.yn),
            4: lambda: (self.sums(1, u, p.y, 1 - p.x), self.ended(1, u), p.xn),
        }[kind]()
        return remote(src, dst, self.sems.at[0, kind, s], self.sems.at[1, kind, s], {"dp": target})

    def product(self, u, turned, right, at):
        cols = span(at * UNIT, UNIT)

        def one(own):
            near = span(own * 4 * self.rows, 4 * self.rows)
            self.made(u, own)[...] = dot(turned[near, :], right[:, cols]).astype(BF)

            @pl.when(own == 0)
            def _():
                self.send(0, u).start()

        loop(2, one)

    def across(self, u):
        self.send(0, u).wait_recv()
        self.send(0, u).wait_send()
        mine = self.made(u, 1)

        def add(chip):
            y_to, x_to = chip // 2, chip % 2
            more = self.got(u, chip)
            for which, spot in ((0, self.sums(0, u, x_to, y_to)), (1, self.sums(1, u, y_to, x_to))):
                near = slice(which * self.half, (which + 1) * self.half)
                own = mine[span(chip * self.rows + which * self.half, self.half), :]
                spot[...] = (own.astype(F32) + more[near, :].astype(F32)).astype(BF)

        loop(4, add)
        self.send(1, u).start()
        self.send(2, u).start()

    def along(self, u):
        p = self.place
        for which, mine in ((0, p.x), (1, p.y)):
            self.send(1 + which, u).wait_recv()
            spot, more = self.sums(which, u, mine), self.met(which, u)
            spot[...] = (spot[...].astype(F32) + more[...].astype(F32)).astype(BF)
            self.send(3 + which, u).start()
        for kind in (1, 2):
            self.send(kind, u).wait_send()

    def wait_write(self, u):
        pltpu.make_async_copy(self.done(u), self.done(u), self.out_sems.at[u % 2]).wait()

    def finish(self, u):
        p = self.place

        @pl.when(u >= 2)
        def _():
            self.wait_write(u)

        parts = []
        for which, spot in ((0, self.sums(0, u, p.x, p.y)), (1, self.sums(1, u, p.y, p.x))):
            self.send(3 + which, u).wait_recv()
            parts.append(spot[...].astype(F32) + self.ended(which, u)[...].astype(F32))
        value = jnp.concatenate(parts, axis=0)

        def put(first, out, flat):
            self.done(u)[...] = (value.T if flat else value).astype(BF)
            near = span((u - first) * UNIT, UNIT)
            target = out.at[near, :] if flat else out.at[:, near]
            pltpu.make_async_copy(self.done(u), target, self.out_sems.at[u % 2]).start()

        first = 0
        for at, out in enumerate(self.outs):
            count = (self.n_ff, self.n_ff, self.n_ff, self.n_local, 3 * self.n_local)[at]
            pl.when((u >= first) & (u < first + count))(functools.partial(put, first, out, at in (0, 3)))
            first += count

        for kind in (3, 4):
            self.send(kind, u).wait_send()

    def tick(self, u, turned, ffs, others):
        @pl.when(u < self.early)
        def _():
            self.product(u, turned, ffs.at[u // self.n_ff], u % self.n_ff)

        @pl.when((u >= self.early) & (u < self.count))
        def _():
            self.product(u, turned, others, u - self.early)

        for lag, stage in ((1, self.across), (3, self.along), (5, self.finish)):
            @pl.when((u >= lag) & (u < self.count + lag))
            def _():
                stage(u - lag)

    def drain(self):
        for u in (self.count - 2, self.count - 1):
            self.wait_write(u)


def as_row(col):
    n = col.shape[0]
    r = lax.broadcasted_iota(jnp.int32, (n, n), 0)
    s = lax.broadcasted_iota(jnp.int32, (n, n), 1)
    return jnp.sum(jnp.where(r == s, col, 0.0), axis=0, keepdims=True)


def as_col(row):
    n = row.shape[1]
    r = lax.broadcasted_iota(jnp.int32, (n, n), 0)
    s = lax.broadcasted_iota(jnp.int32, (n, n), 1)
    return jnp.sum(jnp.where(r == s, row, 0.0), axis=1, keepdims=True)


def turn(values, cos_tab, sin_tab):
    return values * cos_tab + pltpu.roll(values, HD // 2, 1) * sin_tab


def turn_back(grads, cos_tab, sin_tab):
    return grads * cos_tab - pltpu.roll(grads, HD // 2, 1) * sin_tab


def layer_kernel(
    n_mp,
    x_in, cot_in, wq_in, wk_in, wv_in, wo_in, wg_in, wu_in, wd_in,
    seg, live, freq, q_gain, k_gain, a_gain, f_gain,
    wq_out, wk_out, wv_out, wo_out, hidden_out, grad_in_out, gd_out, gg_out, gu_out, go_out, gqkv_out, *rest,
):
    gain_outs = rest[:4]
    (
        tall, wo, wg, wu, wd,
        x, qp, kp, qr, kr, v, o, stat, cos_tab, sin_tab, side, raw_a, h, ffs, d_ffn, cot, part, took,
        turned, dk_sum, dv_sum, sums, gains, gains_got,
        g_send, g_recv, g_local, row_sems, small, s_sems, s_out, gain_sems, io_sems,
    ) = rest[4:]
    place = Place(n_mp)
    rows, width = x.shape
    wq, wk, wv = (tall.at[i * width:(i + 1) * width, :] for i in range(3))
    local, ff = qp.shape[1], ffs.shape[2]
    act, gate, up = (ffs.at[i] for i in range(3))
    heads = local // HD
    scale = 1.0 / math.sqrt(HD)
    half = rows // 2
    n_ff, n_local = ff // UNIT, local // UNIT
    flying = {}

    def move(name, src, dst):
        at = len(flying)
        flying[name] = lambda: pltpu.make_async_copy(src, dst, io_sems.at[at])
        flying[name]().start()

    def need(*names):
        for name in names:
            flying[name]().wait()

    move("x", x_in, x)
    place.barrier()
    gq, gk, gv, go, gg, gu, gd = [
        Gather(place, src, full, i not in (3, 6), g_send.at[i], g_recv.at[i], g_local.at[i])
        for i, (src, full) in enumerate(
            zip((wq_in, wk_in, wv_in, wo_in, wg_in, wu_in, wd_in), (wq, wk, wv, wo, wg, wu, wd))
        )
    ]
    gq.begin_a()
    gq.begin_b()
    gk.begin_a()
    gk.begin_b()
    move("cot", cot_in, cot)
    ids = seg[...].astype(F32)
    ids_col = as_col(ids)
    before = jnp.sum((ids < ids_col).astype(F32), axis=1, keepdims=True)
    row_at = lax.broadcasted_iota(jnp.int32, (rows, 1), 0)
    side[:, 0:1] = ids_col
    side[:, 1:2] = (row_at < live[...]).astype(F32)
    angles = (row_at.astype(F32) - before) * freq[...]
    cos_tab[...] = jnp.cos(angles)
    lane = lax.broadcasted_iota(jnp.int32, (rows, HD), 1)
    sin_tab[...] = jnp.sin(angles) * jnp.where(lane < HD // 2, -1.0, 1.0)
    gq.relay()
    gv.begin_a()
    gq.pass_on()
    gv.begin_b()
    gk.relay()
    go.begin_a()
    gk.pass_on()
    gq.last()
    need("x")
    gq.ready()
    move("wq", wq, wq_out)
    row_sum = SmallSum(place, sums.at[0], small.at[0])

    def project(full, dst, squares_to=None):
        def one(r):
            near = span(r * half, half)
            value = dot(x[near, :], full[...])
            dst[near, :] = value.astype(BF)
            if squares_to is not None:
                stat[near, squares_to:squares_to + 1] = jnp.sum(value * value, axis=1, keepdims=True)

        loop(2, one)

    sums[0, 0] = jnp.zeros(sums.shape[2:], F32)
    project(wq, qp, heads)
    sums[0, 0, 0:1, :] = as_row(stat[:, heads:heads + 1])
    gv.relay()
    go.begin_b()
    gv.pass_on()
    gk.last()
    gk.ready()
    move("wk", wk, wk_out)
    project(wk, kp, heads + 1)
    sums[0, 0, 1:2, :] = as_row(stat[:, heads + 1:heads + 2])
    row_sum.begin()
    go.relay()
    gg.begin_a()
    gv.last()
    gv.ready()
    move("wv", wv, wv_out)
    project(wv, v)
    go.pass_on()
    gg.begin_b()
    totals = row_sum.end()
    inv_q = lax.rsqrt(as_col(totals[0:1, :]) / width + EPS)
    inv_k = lax.rsqrt(as_col(totals[1:2, :]) / width + EPS)
    stat[:, heads:heads + 1] = inv_q
    stat[:, heads + 1:heads + 2] = inv_k

    def rotate_head(hd):
        cols = span(hd * HD, HD)
        qr[:, cols] = turn(qp[:, cols].astype(F32) * inv_q * q_gain[:, cols], cos_tab[...], sin_tab[...]).astype(BF)
        kr[:, cols] = turn(kp[:, cols].astype(F32) * inv_k * k_gain[:, cols], cos_tab[...], sin_tab[...]).astype(BF)

    loop(heads, rotate_head)
    go.last()
    block = rows // 4
    lane_at = lax.broadcasted_iota(jnp.int32, (block, HD), 1)

    def allowed_at(rb):
        near, keys = slice(rb * block, (rb + 1) * block), (rb + 1) * block
        t_at = lax.broadcasted_iota(jnp.int32, (block, keys), 0) + rb * block
        s_at = lax.broadcasted_iota(jnp.int32, (block, keys), 1)
        return near, keys, (side[near, 0:1] == seg[:, 0:keys].astype(F32)) & (s_at <= t_at)

    def attend(rb):
        near, keys, allowed = allowed_at(rb)

        def one(hd):
            cols = span(hd * HD, HD)
            scores = jnp.where(allowed, dot_nt(qr[near, cols], kr[0:keys, cols]) * scale, -1e30)
            top = jnp.max(scores, axis=1, keepdims=True)
            weights = jnp.exp(scores - top)
            norm = jnp.sum(weights, axis=1, keepdims=True)
            stat[near, :] = jnp.where(lane_at == hd, top + jnp.log(norm), stat[near, :])
            o[near, cols] = dot((weights / norm).astype(BF), v[0:keys, cols]).astype(BF)

        loop(heads, one)

    wide = width // 8

    def columns(bits):
        return span(place.block(bits) * wide, wide)

    def by_rows(flow, k):
        return span(k // 4 * half, half), columns(2 * (k % 4) + flow)

    def took_slot(flow, k):
        return took.at[flow, k]

    sum_attn = RowSum(place, part, took_slot, raw_a, row_sems.at[0], by_rows, 8)

    def project_out(r):
        near = slice(r * half, (r + 1) * half)

        def one(i):
            part[near, columns(i)] = dot(o[near, :], wo[:, columns(i)]).astype(BF)

        loop(8, one)

    def mid(r):
        tile = rows // 8

        def one(at):
            near = span(at * tile, tile)
            raw = raw_a[near, :].astype(F32)
            inv = lax.rsqrt(jnp.mean(raw * raw, axis=1, keepdims=True) + EPS)
            h[near, :] = (x[near, :].astype(F32) + raw * inv * a_gain[...]).astype(BF)

        loop(4, one, 4 * r)

    def gate_part(r, first, count):
        near = slice(r * half, (r + 1) * half)

        def one(at):
            cols = span(at * UNIT, UNIT)
            gate[near, cols] = dot(h[near, :], wg[:, cols]).astype(BF)

        loop(count, one, first)

    def up_half(r, first, count):
        near = slice(r * half, (r + 1) * half)

        def one(at):
            cols = span(at * UNIT, UNIT)
            value = dot(h[near, :], wu[:, cols])
            up[near, cols] = value.astype(BF)
            pre = gate[near, cols].astype(F32)
            act[near, cols] = (pre * jax.nn.sigmoid(pre) * value).astype(BF)

        loop(count, one, first)

    attend(0)
    attend(1)
    go.ready()
    move("wo", wo, wo_out)
    project_out(0)
    sum_attn.push(0)
    sum_attn.push(1)
    gu.begin_a()
    attend(2)
    sum_attn.tick(1, 0)
    sum_attn.push(2)
    attend(3)
    sum_attn.tick(2, 0)
    sum_attn.push(3)
    project_out(1)
    gg.relay()
    gu.begin_b()
    sum_attn.push(4)
    sum_attn.tick(3, 0)
    gg.pass_on()

    def attn_both(t):
        sum_attn.push(t + 1)
        sum_attn.both(t, 3)

    attn_both(4)
    attn_both(5)
    gu.relay()
    gd.begin_a()
    loop(2, attn_both, 6)
    gg.last()
    gd.begin_b()
    loop(2, attn_both, 8)
    gg.ready()
    mid(0)

    def gate_and_tick(i):
        gate_part(0, i * (n_ff // 2), n_ff // 2)
        sum_attn.tick(7 + i, 1)

    loop(2, gate_and_tick)
    gu.pass_on()
    sum_attn.tick(9, 1)
    mid(1)
    gate_part(1, 0, n_ff)
    gu.last()
    gu.ready()
    up_half(0, 0, n_ff)
    sum_attn.sent()
    sum_ffn = RowSum(place, part, took_slot, d_ffn, row_sems.at[1], by_rows, 8)

    def project_down(k):
        near = span(k // 4 * half, half)

        def one(flow):
            cols = columns(2 * (k % 4) + flow)
            part[near, cols] = dot(act[near, :], wd[:, cols]).astype(BF)

        loop(2, one)
        sum_ffn.push(k)

    gd.own_copy().wait()
    gd.arrived(6)
    project_down(0)
    need("wq", "wk", "wv", "wo")
    for g in (gq, gk, gv, go):
        g.drain()
    up_half(1, 0, n_ff // 2)
    gd.relay()
    sum_ffn.tick(1, 0)
    up_half(1, n_ff // 2, n_ff // 2)
    project_down(4)
    gd.pass_on()
    gd.arrived(7, 8, 10, 11)
    project_down(1)
    sum_ffn.both(2, 1)
    project_down(2)
    project_down(5)
    sum_ffn.both(3, 1)
    project_down(6)
    gd.last()
    gd.arrived(9)
    project_down(3)
    sum_ffn.tick(4, 0)
    project_down(7)
    sum_ffn.tick(3, 1)

    def ffn_both(t):
        sum_ffn.both(t, 1)

    loop(5, ffn_both, 5)
    sum_ffn.sent(0)
    for g in (gg, gu, gd):
        g.drain()
    need("cot")

    gains[...] = jnp.zeros(gains.shape, F32)
    tile = rows // 8

    def back_ffn(at):
        near = span(at * tile, tile)
        raw = d_ffn[near, :].astype(F32)
        alive = side[near, 1:2]
        dy = alive * cot[near, :].astype(F32)
        inv = lax.rsqrt(jnp.mean(raw * raw, axis=1, keepdims=True) + EPS)
        normed = raw * inv
        gains[0:1, :] += jnp.sum(dy * normed, axis=0, keepdims=True)
        value = (alive * (h[near, :].astype(F32) + normed * f_gain[...])).astype(BF)
        for q in range(width // local):
            wv[span(q * rows + at * tile, tile), :] = value[:, q * local:(q + 1) * local]
        gained = f_gain[...] * dy
        mean = jnp.mean(gained * raw, axis=1, keepdims=True)
        d_ffn[near, :] = (inv * gained - raw * inv**3 * mean).astype(BF)

    def flip(src):
        def one(at):
            parity = at % 2
            own = 1 - (parity + place.c - 2 * parity * place.c)
            turned[span((4 * own + at // 2) * wide, wide), :] = src[:, span(at * wide, wide)].T

        loop(8, one)

    grads_out = (gd_out, gg_out, gu_out, go_out, gqkv_out)
    scatter = Scatter(place, tall, wo, grads_out, s_sems, s_out, n_ff, n_local)

    def back_act(r, first, count):
        near = slice(r * half, (r + 1) * half)

        def one(at):
            cols = span(at * UNIT, UNIT)
            d_act = dot_nt(d_ffn[near, :], wd[cols, :])
            pre, upper = gate[near, cols].astype(F32), up[near, cols].astype(F32)
            sig = jax.nn.sigmoid(pre)
            up[near, cols] = (d_act * pre * sig).astype(BF)
            gate[near, cols] = (d_act * upper * sig * (1.0 + pre * (1.0 - sig))).astype(BF)

        loop(count, one, first)

    raw_h = x
    sum_back = RowSum(place, part, took_slot, raw_h, row_sems.at[2], by_rows, 8)

    def back_gate(r, first):
        near = slice(r * half, (r + 1) * half)

        def one(i):
            value = dot_nt(gate[near, :], wg[columns(i), :]) + dot_nt(up[near, :], wu[columns(i), :])
            part[near, columns(i)] = value.astype(BF)

        loop(4, one, first)
        loop(2, sum_back.push, 4 * r + first // 2)

    dq, dk, dv = (wu.at[2 * rows:3 * rows, i * local:(i + 1) * local] for i in range(1, 4))
    others = wu.at[2 * rows:3 * rows, :]
    d_heads = wu.at[3 * rows:4 * rows, 0:local]
    loop(4, back_ffn)
    back_act(0, 0, n_ff // 2)
    sum_ffn.tick(9, 1)
    back_act(0, n_ff // 2, n_ff // 2)
    back_gate(0, 0)
    sum_ffn.sent(1)
    loop(4, back_ffn, 4)
    for q in range(width // local):
        move(f"hidden{q}", wv.at[q * rows:(q + 1) * rows, :], hidden_out.at[:, q * local:(q + 1) * local])
    flip(d_ffn)
    d_attn = wu.at[rows:2 * rows, :]

    def back_attn(at):
        near = span(at * tile, tile)
        raw = raw_a[near, :].astype(F32)
        dh = side[near, 1:2] * cot[near, :].astype(F32) + raw_h[near, :].astype(F32)
        inv = lax.rsqrt(jnp.mean(raw * raw, axis=1, keepdims=True) + EPS)
        gains[1:2, :] += jnp.sum(dh * raw * inv, axis=0, keepdims=True)
        gained = a_gain[...] * dh
        mean = jnp.mean(gained * raw, axis=1, keepdims=True)
        d_attn[near, :] = (inv * gained - raw * inv**3 * mean).astype(BF)

    def back_out(r):
        near = slice(r * half, (r + 1) * half)
        loop(4, back_attn, 4 * r)
        d_heads[near, :] = dot_nt(d_attn[near, :], wg[0:local, :]).astype(BF)

    def back_head(hd):
        cols = span(hd * HD, HD)
        dk_sum[...] = jnp.zeros(dk_sum.shape, F32)
        dv_sum[...] = jnp.zeros(dv_sum.shape, F32)
        for rb in range(4):
            near, keys, allowed = allowed_at(rb)
            lse = jnp.sum(jnp.where(lane_at == hd, stat[near, :], 0.0), axis=1, keepdims=True)
            scores = jnp.where(allowed, dot_nt(qr[near, cols], kr[0:keys, cols]) * scale, -1e30)
            probs = jnp.where(allowed, jnp.exp(scores - lse), 0.0)
            grad = d_heads[near, cols]
            d_prob = dot_nt(grad, v[0:keys, cols])
            delta = jnp.sum(grad.astype(F32) * o[near, cols].astype(F32), axis=1, keepdims=True)
            d_score = (probs * (d_prob - delta)).astype(BF)
            back = dot(d_score, kr[0:keys, cols]) * scale
            dq[near, cols] = turn_back(back, cos_tab[near, :], sin_tab[near, :]).astype(BF)
            dk_sum[0:keys, :] += dot_tn(d_score, qr[near, cols])
            dv_sum[0:keys, :] += dot_tn(probs.astype(BF), grad)
        dk[:, cols] = turn_back(dk_sum[...] * scale, cos_tab[...], sin_tab[...]).astype(BF)
        dv[:, cols] = dv_sum[...].astype(BF)

    row_sum_back = SmallSum(place, sums.at[1], small.at[1])
    normed = ((dq, qp, q_gain, heads), (dk, kp, k_gain, heads + 1))

    def begin_norms():
        sums[1, 0] = jnp.zeros(sums.shape[2:], F32)
        for at, (grad, raw, gain, lane_of) in enumerate(normed):
            both = grad[...].astype(F32) * raw[...].astype(F32)
            gains[2 + at:3 + at, 0:local] = jnp.sum(both * stat[:, lane_of:lane_of + 1], axis=0, keepdims=True)
            sums[1, 0, at:at + 1, :] = as_row(jnp.sum(gain[...] * both, axis=1, keepdims=True))
        row_sum_back.begin()

    def end_norms():
        totals = row_sum_back.end()
        for at, (grad, raw, gain, lane_of) in enumerate(normed):
            inv = stat[:, lane_of:lane_of + 1]
            mean = as_col(totals[at:at + 1, :]) / width
            gained = gain[...] * grad[...].astype(F32)
            grad[...] = (inv * gained - raw[...].astype(F32) * inv**3 * mean).astype(BF)

    raw_x = d_ffn
    sum_in = RowSum(place, part, took_slot, raw_x, row_sems.at[3], by_rows, 8)

    def back_in(r):
        near = slice(r * half, (r + 1) * half)

        def one(i):
            spot = columns(i)
            value = dot_nt(dq[near, :], wd[spot, 0:local]) + dot_nt(dk[near, :], wd[spot, local:2 * local])
            part[near, spot] = (value + dot_nt(dv[near, :], wd[spot, 2 * local:3 * local])).astype(BF)

        loop(8, one)
        loop(4, sum_in.push, 4 * r)

    def end_tile(at):
        near = span(at * tile, tile)
        dh = side[near, 1:2] * cot[near, :].astype(F32) + raw_h[near, :].astype(F32)
        cot[near, :] = (dh + raw_x[near, :].astype(F32)).astype(BF)

    def end_half(r):
        loop(4, end_tile, 4 * r)
        near = slice(r * half, (r + 1) * half)
        move(f"grad_in{r}", cot.at[near, :], grad_in_out.at[near, :])

    partners = (place.sib, place.xn, place.yn)

    def gain_copy(at):
        return remote(
            gains.at[pl.ds(8 * at, 8), :], gains_got.at[at], gain_sems.at[0, at], gain_sems.at[1, at],
            {"dp": partners[at]},
        )

    def add_gains(at):
        gain_copy(at).wait_recv()
        gains[8 * at + 8:8 * at + 16, :] = gains[8 * at:8 * at + 8, :] + gains_got[at]
        if at < 2:
            gain_copy(at + 1).start()
        else:
            for i, out in enumerate(gain_outs):
                move(f"gain{i}", gains.at[24 + i:25 + i, 0:out.shape[1]], out)

    def fetch():
        move("wq2", wq_out, wd.at[:, 0:local])
        move("wk2", wk_out, wd.at[:, local:2 * local])
        move("wv2", wv_out, wd.at[:, 2 * local:3 * local])
        move("wo2", wo_out, wg.at[0:local, :])
        move("x2", x_in, wu.at[0:rows, :])

    def at_step(s):
        if s == 0:
            back_gate(0, 4)
        elif s in (1, 2):
            back_act(1, (s - 1) * (n_ff // 2), n_ff // 2)
        elif s in (3, 4):
            back_gate(1, 4 * (s - 3))
            if s == 4:
                fetch()
        elif s == 12:
            need("wo2")
            back_out(0)
        elif s == 13:
            sum_back.sent()
            back_out(1)
            others[:, 0:local] = o[...]
        elif s == 14:
            loop(heads // 2, back_head)
        elif s == 15:
            loop(heads - heads // 2, back_head, heads // 2)
            begin_norms()
        elif s == 17:
            end_norms()
            need("wq2", "wk2", "wv2", "x2")
        elif s in (18, 19):
            back_in(s - 18)
        elif s == 20:
            gain_copy(0).start()
        elif s in (22, 24, 26):
            add_gains((s - 22) // 2)
        elif s in (28, 29):
            end_half(s - 28)

    def at_tick(u, act_on):
        @pl.when(u == act_on[0])
        def _():
            act_on[1]()

    doubles = (4, 7, 20, 22, 23, 25)

    def one_tick(u):
        for when, src in ((n_ff, h), (3 * n_ff, d_attn), (3 * n_ff + n_local, wu.at[0:rows, :])):
            at_tick(u, (when, functools.partial(flip, src)))
        at_tick(u, (1, functools.partial(need, *(f"hidden{q}" for q in range(width // local)))))
        scatter.tick(u, turned, ffs, others)

    def step(s):
        before = sum((s > at).astype(jnp.int32) for at in doubles)
        here = sum((s == at).astype(jnp.int32) for at in doubles)
        loop(1 + here, one_tick, s + before)

        at_tick(s, (19, functools.partial(at_step, 19)))

        for row_sum_, half_, t, first, last in (
            (sum_back, 0, s, 1, 5), (sum_back, 1, s - 3, 4, 12), (sum_in, 0, s - 18, 19, 27), (sum_in, 1, s - 20, 21, 29),
        ):
            @pl.when((s >= first) & (s <= last))
            def _():
                row_sum_.tick(t, half_)

        @pl.when((s >= 6) & (s <= 12) & (s % 2 == 0))
        def _():
            sum_back.tick((s + 6) // 2, 0)

        for when in (0, 1, 2, 3, 4, 12, 13, 14, 15, 17, 18, 20, 22, 24, 26, 28, 29):
            at_tick(s, (when, functools.partial(at_step, when)))

    loop(scatter.count + 5 - len(doubles), step)
    for at in range(3):
        gain_copy(at).wait_send()
    sum_in.sent()
    row_sum.drain()
    row_sum_back.drain()
    scatter.drain()
    need("gain0", "gain1", "gain2", "gain3", "grad_in0", "grad_in1")


def layer_call(n_mp, x, cot, weights, seg, live, freq, q_gain, k_gain, a_gain, f_gain):
    rows, width = x.shape
    local, ff = weights[0].shape[1], weights[4].shape[1]
    high, half = width // 8, rows // 2
    any_spec = pl.BlockSpec(memory_space=pl.ANY)
    vmem = pl.BlockSpec(memory_space=pltpu.VMEM)
    S, V, dma = jax.ShapeDtypeStruct, pltpu.VMEM, pltpu.SemaphoreType.DMA
    fulls = [(width, local)] * 3 + [(local, width)] + [(width, ff)] * 2 + [(ff, width)]
    outs = fulls[:4] + [
        (rows, width), (rows, width), (ff, high), (high, ff), (high, ff), (local, high), (high, 3 * local),
    ]
    return pl.pallas_call(
        functools.partial(layer_kernel, n_mp),
        out_shape=[S(s, BF) for s in outs] + [S((1, n), F32) for n in (width, width, local, local)],
        in_specs=[any_spec] * 9 + [vmem] * 7,
        out_specs=[any_spec] * 15,
        scratch_shapes=[V(((16 + 5 * Scatter.slots // 2) * high, local), BF)]
        + [V(s, BF) for s in fulls[3:]]
        + [V((rows, width), BF)]
        + [V((rows, local), BF)] * 6
        + [V((rows, HD), F32)] * 4
        + [V((rows, width), BF)] * 2
        + [V((3, rows, ff), BF)]
        + [V((rows, width), BF)] * 3
        + [V((2, 8, half, high), BF), V((width, rows), BF), V((rows, HD), F32), V((rows, HD), F32)]
        + [V((2, n_mp, 8, rows), F32), V((32, width), F32), V((3, 8, width), F32)]
        + [dma((7, 12)), dma((7, 12)), dma((7,)), dma((4, 4, 2, 8)), dma((2, 2, n_mp))]
        + [dma((2, 5, Scatter.slots)), dma((2,)), dma((2, 3)), dma((24,))],
        compiler_params=pltpu.CompilerParams(
            collective_id=0, has_side_effects=True, vmem_limit_bytes=67043328,
        ),
    )(x, cot, *weights, seg, live, freq, q_gain, k_gain, a_gain, f_gain)


def with_kernel(n_mp, hidden_in, cotangent, segments, live_counts, *rest):
    weights, (query_gain, key_gain, attn_gain, ffn_gain) = rest[:7], rest[7:]
    local = weights[0].shape[1]
    inv_freq = THETA ** (-(jnp.arange(HD // 2, dtype=F32) * (2.0 / HD)))
    freq = jnp.concatenate([inv_freq, inv_freq])[None]
    hidden_out, grad_in, g_down, g_gate, g_up, g_output, g_qkv, d_f, d_a, d_q, d_k = layer_call(
        n_mp, hidden_in, cotangent, weights, segments, live_counts[None], freq,
        query_gain[None], key_gain[None], attn_gain[None], ffn_gain[None],
    )[4:]

    return (
        hidden_out,
        grad_in.astype(F32),
        g_qkv[:, :local].astype(F32),
        g_qkv[:, local:2 * local].astype(F32),
        g_qkv[:, 2 * local:].astype(F32),
        g_output.astype(F32),
        g_gate.astype(F32),
        g_up.astype(F32),
        g_down.astype(F32),
        d_q[0],
        d_k[0],
        d_a[0],
        d_f[0],
    )


def doc_positions(seg_row):
    row_count = seg_row.shape[0]
    row_index = jnp.arange(row_count, dtype=jnp.int32)
    change = jnp.concatenate([jnp.ones((1,), dtype=bool), seg_row[1:] != seg_row[:-1]])
    doc_start = lax.cummax(jnp.where(change, row_index, jnp.zeros_like(row_index)), axis=0)
    return (row_index - doc_start).astype(jnp.float32)


def rotary_tables(positions, head_size):
    half_size = head_size // 2
    inv_freq = THETA ** (-(jnp.arange(half_size, dtype=jnp.float32) * (2.0 / head_size)))
    angles = positions[:, None] * inv_freq[None, :]
    return (jnp.cos(angles)[:, None, :], jnp.sin(angles)[:, None, :])


def rotate(values, cos_tab, sin_tab):
    half_size = values.shape[2] // 2
    first_half = values[:, :, :half_size]
    second_half = values[:, :, half_size:]
    return jnp.concatenate(
        [
            first_half * cos_tab - second_half * sin_tab,
            second_half * cos_tab + first_half * sin_tab,
        ],
        axis=2,
    )


def rotate_back(grads, cos_tab, sin_tab):
    half_size = grads.shape[2] // 2
    first_half = grads[:, :, :half_size]
    second_half = grads[:, :, half_size:]
    return jnp.concatenate(
        [
            first_half * cos_tab + second_half * sin_tab,
            second_half * cos_tab - first_half * sin_tab,
        ],
        axis=2,
    )


def block_mask(seg_row, offset, block_rows):
    row_index = jnp.arange(seg_row.shape[0])
    same = seg_row[offset : offset + block_rows, None] == seg_row[None, :]
    return same & (row_index[:, None] >= row_index[None, :])


def block_scores(q_blk, k_bf, allowed, score_scale):
    scores = (
        jnp.einsum("qhe,khe->hqk", q_blk, k_bf, preferred_element_type=jnp.float32) * score_scale
    )
    return jnp.where(allowed[None], scores, jnp.float32(-1e30))


def attend_forward(q_bf, k_bf, v_bf, seg_row, score_scale):
    row_count = q_bf.shape[0]
    block_rows = min(512, row_count)
    allowed = block_mask(seg_row, 0, block_rows)
    scores = block_scores(q_bf, k_bf, allowed, score_scale)
    row_max = jnp.max(scores, axis=2, keepdims=True)
    lse = row_max + jnp.log(jnp.sum(jnp.exp(scores - row_max), axis=2, keepdims=True))
    probs = jnp.exp(scores - lse).astype(jnp.bfloat16)
    outputs = jnp.einsum("hqk,khe->qhe", probs, v_bf, preferred_element_type=jnp.float32)
    lse_parts = [lse]
    return (outputs.astype(jnp.bfloat16), lse_parts)


def attend_backward(q_bf, k_bf, v_bf, o_bf, do_bf, lse_parts, seg_row, score_scale):
    row_count = q_bf.shape[0]
    block_rows = min(512, row_count)
    dq_parts = []
    dk_acc = jnp.zeros(k_bf.shape, jnp.float32)
    dv_acc = jnp.zeros(v_bf.shape, jnp.float32)
    for part_index, offset in enumerate(range(0, row_count, block_rows)):
        allowed = block_mask(seg_row, offset, block_rows)
        scores = block_scores(q_bf, k_bf, allowed, score_scale)
        probs = jnp.exp(scores - lse_parts[part_index])
        probs_bf = probs.astype(jnp.bfloat16)
        dprob = jnp.einsum("qhe,khe->hqk", do_bf, v_bf, preferred_element_type=jnp.float32)
        delta = jnp.transpose(
            jnp.sum(do_bf.astype(jnp.float32) * o_bf.astype(jnp.float32), axis=2)
        )[:, :, None]
        dscore = (probs * (dprob - delta)).astype(jnp.bfloat16)
        dq_parts.append(
            jnp.einsum("hqk,khe->qhe", dscore, k_bf, preferred_element_type=jnp.float32)
            * score_scale
        )
        dk_acc = (
            jnp.einsum("hqk,qhe->khe", dscore, q_bf, preferred_element_type=jnp.float32)
            * score_scale
        )
        dv_acc = jnp.einsum("hqk,qhe->khe", probs_bf, do_bf, preferred_element_type=jnp.float32)
    return (dq_parts[0], dk_acc, dv_acc.astype(jnp.bfloat16))


def scatter_grad(grad, axis_name, scatter_dimension, tiled):
    total = lax.psum_scatter(
        grad.astype(jnp.bfloat16), axis_name, scatter_dimension=scatter_dimension, tiled=tiled
    )
    return total.astype(jnp.float32)


def sum_parts(part, axis_name):
    own = lax.psum_scatter(
        part.astype(jnp.bfloat16), axis_name, scatter_dimension=0, tiled=True
    )
    return lax.all_gather(own, axis_name, axis=0, tiled=True).astype(jnp.float32)


def norm_back(raw, inv_scale, gained, row_sums, width):
    return inv_scale * gained - raw * inv_scale**3 * (row_sums[:, None] / width)


def on_device(
    hidden_in,
    cotangent,
    segments,
    live_counts,
    w_query,
    w_key,
    w_value,
    w_output,
    w_gate,
    w_up,
    w_down,
    query_gain,
    key_gain,
    attn_gain,
    ffn_gain,
):
    gathered = (
        lax.all_gather(w_query, "dp", axis=0, tiled=True),
        lax.all_gather(w_key, "dp", axis=0, tiled=True),
        lax.all_gather(w_value, "dp", axis=0, tiled=True),
        lax.all_gather(w_output, "dp", axis=1, tiled=True),
        lax.all_gather(w_gate, "dp", axis=0, tiled=True),
        lax.all_gather(w_up, "dp", axis=0, tiled=True),
        lax.all_gather(w_down, "dp", axis=1, tiled=True),
    )
    wq_full, wk_full, wv_full, wo_full, wg_full, wu_full, wd_full = gathered
    seg_row = segments[0]
    live_n = live_counts[0]
    row_count, width = hidden_in.shape
    local_width = wq_full.shape[1]
    heads_here = local_width // HD
    score_scale = 1.0 / math.sqrt(HD)
    live_mask = (jnp.arange(row_count, dtype=jnp.int32) < live_n).astype(jnp.float32)[:, None]
    cos_tab, sin_tab = rotary_tables(doc_positions(seg_row), HD)
    q_proj = jnp.dot(hidden_in, wq_full, preferred_element_type=jnp.float32)
    k_proj = jnp.dot(hidden_in, wk_full, preferred_element_type=jnp.float32)
    v_bf = jnp.dot(hidden_in, wv_full, preferred_element_type=jnp.float32).astype(jnp.bfloat16)
    sq_query, sq_key = lax.psum(
        (jnp.sum(q_proj * q_proj, axis=1), jnp.sum(k_proj * k_proj, axis=1)), "mp"
    )
    inv_q = lax.rsqrt(sq_query[:, None] / width + EPS)
    inv_k = lax.rsqrt(sq_key[:, None] / width + EPS)
    q_rot = rotate(
        (q_proj * inv_q * query_gain).reshape(row_count, heads_here, HD), cos_tab, sin_tab
    ).astype(jnp.bfloat16)
    k_rot = rotate(
        (k_proj * inv_k * key_gain).reshape(row_count, heads_here, HD), cos_tab, sin_tab
    ).astype(jnp.bfloat16)
    v_heads = v_bf.reshape(row_count, heads_here, HD)
    o_bf, lse_parts = attend_forward(q_rot, k_rot, v_heads, seg_row, score_scale)
    o_flat = o_bf.reshape(row_count, local_width)
    attn_raw = sum_parts(jnp.dot(o_flat, wo_full, preferred_element_type=jnp.float32), "mp")
    inv_a = lax.rsqrt(jnp.mean(attn_raw * attn_raw, axis=1, keepdims=True) + EPS)
    h_mid = hidden_in.astype(jnp.float32) + attn_raw * inv_a * attn_gain
    h_bf = h_mid.astype(jnp.bfloat16)
    gate_pre = jnp.dot(h_bf, wg_full, preferred_element_type=jnp.float32)
    up_pre = jnp.dot(h_bf, wu_full, preferred_element_type=jnp.float32)
    act_bf = (jax.nn.silu(gate_pre) * up_pre).astype(jnp.bfloat16)
    ffn_raw = sum_parts(jnp.dot(act_bf, wd_full, preferred_element_type=jnp.float32), "mp")
    inv_f = lax.rsqrt(jnp.mean(ffn_raw * ffn_raw, axis=1, keepdims=True) + EPS)
    hidden_out = (live_mask * (h_mid + ffn_raw * inv_f * ffn_gain)).astype(jnp.bfloat16)
    wq_back, wk_back, wv_back, wo_back, wg_back, wu_back, wd_back = gathered
    dy = live_mask * cotangent.astype(jnp.float32)
    g_ffn_gain = jnp.sum(dy * ffn_raw * inv_f, axis=0)
    gained_f = ffn_gain * dy
    d_ffn = norm_back(ffn_raw, inv_f, gained_f, jnp.sum(gained_f * ffn_raw, axis=1), width).astype(
        jnp.bfloat16
    )
    d_act = jnp.dot(d_ffn, wd_back.T, preferred_element_type=jnp.float32)
    sig = jax.nn.sigmoid(gate_pre)
    d_up = (d_act * gate_pre * sig).astype(jnp.bfloat16)
    d_gate = (d_act * up_pre * sig * (1.0 + gate_pre * (1.0 - sig))).astype(jnp.bfloat16)
    ffn_part = jnp.dot(d_gate, wg_back.T, preferred_element_type=jnp.float32) + jnp.dot(
        d_up, wu_back.T, preferred_element_type=jnp.float32
    )
    dh = dy + sum_parts(ffn_part, "mp")
    g_down = jnp.dot(act_bf.T, d_ffn, preferred_element_type=jnp.float32)
    g_gate = jnp.dot(h_bf.T, d_gate, preferred_element_type=jnp.float32)
    g_up = jnp.dot(h_bf.T, d_up, preferred_element_type=jnp.float32)
    g_attn_gain = jnp.sum(dh * attn_raw * inv_a, axis=0)
    gained_a = attn_gain * dh
    d_attn = norm_back(
        attn_raw, inv_a, gained_a, jnp.sum(gained_a * attn_raw, axis=1), width
    ).astype(jnp.bfloat16)
    d_heads = jnp.dot(d_attn, wo_back.T, preferred_element_type=jnp.float32).astype(jnp.bfloat16)
    g_output = jnp.dot(o_flat.T, d_attn, preferred_element_type=jnp.float32)
    dq_rot, dk_rot, d_val = attend_backward(
        q_rot,
        k_rot,
        v_heads,
        o_bf,
        d_heads.reshape(row_count, heads_here, HD),
        lse_parts,
        seg_row,
        score_scale,
    )
    dq_norm = rotate_back(dq_rot, cos_tab, sin_tab).reshape(row_count, local_width)
    dk_norm = rotate_back(dk_rot, cos_tab, sin_tab).reshape(row_count, local_width)
    g_query_gain = jnp.sum(dq_norm * q_proj * inv_q, axis=0)
    g_key_gain = jnp.sum(dk_norm * k_proj * inv_k, axis=0)
    gained_q = query_gain * dq_norm
    gained_k = key_gain * dk_norm
    sums_query, sums_key = lax.psum(
        (jnp.sum(gained_q * q_proj, axis=1), jnp.sum(gained_k * k_proj, axis=1)), "mp"
    )
    dq_bf = norm_back(q_proj, inv_q, gained_q, sums_query, width).astype(jnp.bfloat16)
    dk_bf = norm_back(k_proj, inv_k, gained_k, sums_key, width).astype(jnp.bfloat16)
    dv_bf = d_val.reshape(row_count, local_width)
    input_part = (
        jnp.dot(dq_bf, wq_back.T, preferred_element_type=jnp.float32)
        + jnp.dot(dk_bf, wk_back.T, preferred_element_type=jnp.float32)
        + jnp.dot(dv_bf, wv_back.T, preferred_element_type=jnp.float32)
    )
    grad_in = dh + sum_parts(input_part, "mp")
    g_query = jnp.dot(hidden_in.T, dq_bf, preferred_element_type=jnp.float32)
    g_key = jnp.dot(hidden_in.T, dk_bf, preferred_element_type=jnp.float32)
    g_value = jnp.dot(hidden_in.T, dv_bf, preferred_element_type=jnp.float32)
    owned = (
        scatter_grad(g_query, "dp", scatter_dimension=0, tiled=True),
        scatter_grad(g_key, "dp", scatter_dimension=0, tiled=True),
        scatter_grad(g_value, "dp", scatter_dimension=0, tiled=True),
        scatter_grad(g_output, "dp", scatter_dimension=1, tiled=True),
        scatter_grad(g_gate, "dp", scatter_dimension=0, tiled=True),
        scatter_grad(g_up, "dp", scatter_dimension=0, tiled=True),
        scatter_grad(g_down, "dp", scatter_dimension=1, tiled=True),
    )
    gain_totals = lax.psum((g_query_gain, g_key_gain, g_attn_gain, g_ffn_gain), "dp")
    return (
        hidden_out,
        grad_in,
        owned[0],
        owned[1],
        owned[2],
        owned[3],
        owned[4],
        owned[5],
        owned[6],
        gain_totals[0],
        gain_totals[1],
        gain_totals[2],
        gain_totals[3],
    )


def kernel_fits(mesh, hidden_in, segments, w_query, w_gate):
    n_dp, n_mp = mesh.shape["dp"], mesh.shape["mp"]
    rows, width = hidden_in.shape[0] // n_dp, hidden_in.shape[1]
    local, ff = w_query.shape[1] // n_mp, w_gate.shape[1] // n_mp
    even = width % (8 * UNIT) == 0 and local % UNIT == 0 and ff % (2 * UNIT) == 0
    fits = rows == UNIT * 2 and width == 8 * UNIT and local == rows and ff == width
    return n_dp == 8 and n_mp >= 2 and even and fits


def solution(mesh):
    in_specs = (
        P("dp", None),
        P("dp", None),
        P("dp", None),
        P("dp"),
        P("dp", "mp"),
        P("dp", "mp"),
        P("dp", "mp"),
        P("mp", "dp"),
        P("dp", "mp"),
        P("dp", "mp"),
        P("mp", "dp"),
        P("mp"),
        P("mp"),
        P(),
        P(),
    )
    out_specs = (
        P("dp", None),
        P("dp", None),
        P("dp", "mp"),
        P("dp", "mp"),
        P("dp", "mp"),
        P("mp", "dp"),
        P("dp", "mp"),
        P("dp", "mp"),
        P("mp", "dp"),
        P("mp"),
        P("mp"),
        P(),
        P(),
    )

    def step(*args):
        if kernel_fits(mesh, args[0], args[2], args[4], args[8]):
            body = functools.partial(with_kernel, mesh.shape["mp"])
        else:
            body = on_device
        return jax.shard_map(
            body, mesh=mesh, in_specs=in_specs, out_specs=out_specs, check_vma=False
        )(*args)

    return step
```
